32 devices in a mesh: stream: 4 (over y, x), span: 8 (over z, core).
Axes of the slice: x: 2, y: 2, z: 4, core: 2. Of those that a mesh axis runs over, the one named last changes fastest.
Arguments:
- fine_pops: float32 [27, 24, 48, 128], P(None, 'stream', 'span'), may hold values from 0.5 to 2
- coarse_pops: float32 [27, 12, 24, 64], P(None, 'stream', 'span'), may hold values from 0.5 to 2
- obstacle: int32 [24, 48, 128], P('stream', 'span'), may hold values from 0 to 1, as said below
- block_level: int32 [4, 8], replicated, may hold values 0 or 1
- relax_rates: float32 [27], replicated, may hold values from 0.5 to 1.9
Outputs:
- fine_next: float32 [27, 24, 48, 128], P(None, 'stream', 'span')
- coarse_next: float32 [27, 12, 24, 64], P(None, 'stream', 'span')
The draws below stay inside these ranges and needn't reach their ends.
Inputs may be any that keep to these rules, and one draw needn't show every extreme that they name: `block_level`: 1 marks a refined block, whose fine cells are active; 0 a coarse block. `obstacle`: 1 marks a building cell. No building cell has a first index x with x % 6 below 2 or at least 4, nor a second index y with y % 6 below 2 or at least 4; a building cell stands on the ground or on another building cell.
All inputs are finite; a program needn't handle non-finite values.
Results may differ from the reference program's by a relative error of at most 0.0003.
Values sent between devices are 32-bit elements; how exact they have to be, the bound alone decides.
No kernel may reach another device: no remote copies, remote signals or barrier semaphores. Data moves between devices by JAX's collectives and lax.ppermute only.
A program may use at most 64 MiB of HBM per device.

```python
import math
import jax
import jax.numpy as jnp
from jax import lax

BX = 6
BY = 6
BZ = 128
NX = 24
NY = 48
N_STREAM = 4
N_SPAN = 8


def draw_obstacle(key, part):
    heights = jax.random.randint(key, (NX, NY), -(BZ // 4), BZ // 2)
    heights = jnp.maximum(heights, 0)
    place_x = jnp.arange(NX) % BX
    place_y = jnp.arange(NY) % BY
    inner_x = (place_x >= 2) & (place_x < BX - 2)
    inner_y = (place_y >= 2) & (place_y < BY - 2)
    heights = jnp.where(inner_x[:, None] & inner_y[None, :], heights, 0)
    levels = jnp.arange(BZ)
    return (levels[None, None, :] < heights[:, :, None]).astype(jnp.int32)


def touch_ends(array, rng, smallest, high):
    dims = array.shape
    spot = [jax.random.randint(jax.random.fold_in(rng, axis), (), 0, dims[axis]) for axis in range(len(dims))]
    array = array.at[tuple(spot)].set(smallest)
    longest = dims.index(max(dims))
    spot[longest] = (spot[longest] + 1) % dims[longest]
    return array.at[tuple(spot)].set(high)


def block_levels(stream_key, extent, shards, smallest, top_value):
    factor_of, own = 1.0, jax.random.fold_in(stream_key, 6)
    for axis_at, blocks in shards:
        draws = jnp.exp(jax.random.uniform(jax.random.fold_in(own, axis_at), (blocks,), jnp.float32, smallest / len(shards), top_value / len(shards)))
        factor_of = factor_of * jnp.repeat(draws, extent[axis_at] // blocks).reshape([-1 if axis == axis_at else 1 for axis in range(len(extent))])
    return factor_of


def setup_inputs(seed: int = 0) -> dict:
    key_of = jax.random.split(jax.random.key(seed), 6)
    fine_pops = jnp.clip(jnp.exp(math.log(2.0) - 1.3862944 * jax.random.uniform(key_of[0], (27, NX, NY, BZ), jnp.float32) ** block_levels(key_of[0], (27, NX, NY, BZ), ((1, 4), (2, 8)), -0.2, 0.2)), 0.5, 2.0)
    coarse_pops = jnp.clip(jnp.exp(math.log(2.0) - 1.3862944 * jax.random.uniform(key_of[1], (27, NX // 2, NY // 2, BZ // 2), jnp.float32) ** block_levels(key_of[1], (27, NX // 2, NY // 2, BZ // 2), ((1, 4), (2, 8)), -0.2, 0.2)), 0.5, 2.0)
    obstacle = draw_obstacle(jax.random.fold_in(key_of[5], 71), 0)
    block_level = touch_ends((jax.random.randint(key_of[3], (N_STREAM, N_SPAN), 0, 2) < 1).astype(jnp.int32), jax.random.fold_in(key_of[3], 1), 0, 1)
    relax_rates = jnp.clip(jax.random.uniform(key_of[4], (27,), jnp.float32, 0.5, 1.9), 0.5, 1.9)
    return {"fine_pops": fine_pops, "coarse_pops": coarse_pops, "obstacle": obstacle, "block_level": block_level, "relax_rates": relax_rates}


def weight_table():
    single = jnp.where(jnp.arange(3) == 1, 2.0 / 3.0, 1.0 / 6.0).astype(jnp.float32)
    return single[:, None, None] * single[None, :, None] * single[None, None, :]


def central(moments, velocity, axis):
    minus_part = lax.index_in_dim(moments, 0, axis, False)
    zero_part = lax.index_in_dim(moments, 1, axis, False)
    plus_part = lax.index_in_dim(moments, 2, axis, False)
    summed = minus_part + zero_part + plus_part
    difference = plus_part - minus_part
    sum_pair = plus_part + minus_part
    first_order = difference - velocity * summed
    second = sum_pair - 2.0 * velocity * difference + velocity * velocity * summed
    return jnp.stack([summed, first_order, second], axis=axis)


def restore(moments, velocity, axis):
    zeroth = lax.index_in_dim(moments, 0, axis, False)
    first_order = lax.index_in_dim(moments, 1, axis, False)
    second = lax.index_in_dim(moments, 2, axis, False)
    square = velocity * velocity
    zero_part = zeroth * (1.0 - square) - 2.0 * velocity * first_order - second
    plus_part = 0.5 * (second + (2.0 * velocity + 1.0) * first_order + (square + velocity) * zeroth)
    minus_part = 0.5 * (second + (2.0 * velocity - 1.0) * first_order + (square - velocity) * zeroth)
    return jnp.stack([minus_part, zero_part, plus_part], axis=axis)


def collide(scaled, rates):
    others = scaled.shape[1:]
    table = weight_table().reshape(3, 3, 3, 1, 1, 1)
    pops = scaled.reshape((3, 3, 3) + others) * table
    density = jnp.sum(pops, axis=(0, 1, 2))
    velocity_x = jnp.sum(pops[2] - pops[0], axis=(0, 1)) / density
    velocity_y = jnp.sum(pops[:, 2] - pops[:, 0], axis=(0, 1)) / density
    velocity_z = jnp.sum(pops[:, :, 2] - pops[:, :, 0], axis=(0, 1)) / density
    moments = central(pops, velocity_x, 0)
    moments = central(moments, velocity_y, 1)
    moments = central(moments, velocity_z, 2)
    single = jnp.where(jnp.arange(3) == 0, 1.0, jnp.where(jnp.arange(3) == 1, 0.0, 1.0 / 3.0)).astype(jnp.float32)
    target = (single[:, None, None] * single[None, :, None] * single[None, None, :]).reshape(3, 3, 3, 1, 1, 1) * density
    moments = moments - rates.reshape(3, 3, 3, 1, 1, 1) * (moments - target)
    moments = restore(moments, velocity_z, 2)
    moments = restore(moments, velocity_y, 1)
    moments = restore(moments, velocity_x, 0)
    return (moments / table).reshape((27,) + others)


def shift_height(source, bounce, step):
    if step == 0:
        return source, bounce
    edge_value = jnp.zeros_like(source[..., :1])
    edge_bounce = jnp.ones_like(bounce[..., :1])
    if step == 1:
        return (jnp.concatenate([edge_value, source[..., :-1]], axis=-1),
                jnp.concatenate([edge_bounce, bounce[..., :-1]], axis=-1))
    return (jnp.concatenate([source[..., 1:], edge_value], axis=-1),
            jnp.concatenate([bounce[..., 1:], edge_bounce], axis=-1))


def stream_pull(padded, blocked):
    size_x = padded.shape[1] - 2
    size_y = padded.shape[2] - 2
    center = padded[:, 1:-1, 1:-1]
    pieces = []
    for pop_index in range(27):
        step_x = pop_index // 9 - 1
        step_y = pop_index // 3 % 3 - 1
        step_z = pop_index % 3 - 1
        source = padded[pop_index, 1 - step_x:1 - step_x + size_x, 1 - step_y:1 - step_y + size_y]
        bounce = blocked[1 - step_x:1 - step_x + size_x, 1 - step_y:1 - step_y + size_y]
        source, bounce = shift_height(source, bounce, step_z)
        pieces.append(jnp.where(bounce, center[26 - pop_index], source))
    return jnp.stack(pieces)


def refine_axis(values, axis):
    length = values.shape[axis]
    middle = lax.slice_in_dim(values, 1, length - 1, axis=axis)
    before = lax.slice_in_dim(values, 0, length - 2, axis=axis)
    after = lax.slice_in_dim(values, 2, length, axis=axis)
    lower = 0.75 * middle + 0.25 * before
    higher = 0.75 * middle + 0.25 * after
    shape = list(middle.shape)
    shape[axis] = shape[axis] * 2
    return jnp.stack([lower, higher], axis=axis + 1).reshape(shape)


def explode(coarse_pad):
    tall = jnp.concatenate([coarse_pad[..., :1], coarse_pad, coarse_pad[..., -1:]], axis=3)
    return refine_axis(refine_axis(refine_axis(tall, 1), 2), 3)


def coalesce(fine_values):
    count, size_x, size_y, height = fine_values.shape
    shaped = fine_values.reshape(count, size_x // 2, 2, size_y // 2, 2, height // 2, 2)
    return jnp.mean(shaped, axis=(2, 4, 6))


def coarsen(flags):
    size_x, size_y, height = flags.shape
    shaped = flags.reshape(size_x // 2, 2, size_y // 2, 2, height // 2, 2)
    return jnp.max(shaped, axis=(1, 3, 5))


def wrap_span(values, axis):
    length = values.shape[axis]
    return jnp.concatenate([lax.slice_in_dim(values, length - 1, length, axis=axis), values,
                            lax.slice_in_dim(values, 0, 1, axis=axis)], axis=axis)


def reference(fine_pops, coarse_pops, obstacle, block_level, relax_rates):
    fine_rates = relax_rates.reshape(3, 3, 3)
    coarse_rates = 1.0 / (2.0 / fine_rates - 0.5)
    half_x = BX // 2
    level_fine = jnp.repeat(block_level, BY, axis=1)
    level_coarse = jnp.repeat(block_level, BY // 2, axis=1)
    coarse_walls = coarsen(obstacle)

    def slab_rows(slab):
        rows = ((jnp.arange(BX + 2, dtype=jnp.int32) + slab * BX - 1) % NX).astype(jnp.int32)
        coarse_rows = ((jnp.arange(half_x + 4, dtype=jnp.int32) + slab * half_x - 2) % (NX // 2)).astype(jnp.int32)
        coarse_pad = wrap_span(jnp.take(coarse_pops, coarse_rows, axis=1), 2)
        exploded = explode(coarse_pad)[:, 1:BX + 3]
        fine_rows = jnp.take(fine_pops, rows, axis=1)
        refined = jnp.take(level_fine, (rows // BX).astype(jnp.int32), axis=0) == 1
        active = jnp.where(refined[None, :, :, None], fine_rows, exploded)
        padded = wrap_span(active, 2)
        walls = wrap_span(jnp.take(obstacle, rows, axis=0), 1) == 1
        passed = stream_pull(padded, walls)
        fine_new = jnp.where(walls[None, 1:-1, 1:-1], active[:, 1:-1], collide(passed, fine_rates))
        fine_next = jnp.where(refined[None, 1:-1, :, None], fine_new, exploded[:, 1:-1])
        coarse_mid = coarse_pad[:, 1:-1]
        coarse_flags = wrap_span(jnp.take(coarse_walls, coarse_rows[1:-1], axis=0), 1) == 1
        coarse_passed = stream_pull(coarse_mid, coarse_flags)
        coarse_new = jnp.where(coarse_flags[None, 1:-1, 1:-1], coarse_mid[:, 1:-1, 1:-1],
                               collide(coarse_passed, coarse_rates))
        coarse_refined = jnp.take(level_coarse, slab, axis=0) == 1
        coarse_next = jnp.where(coarse_refined[None, None, :, None], coalesce(fine_next), coarse_new)
        return fine_next, coarse_next

    fine_all, coarse_all = lax.map(slab_rows, jnp.arange(N_STREAM, dtype=jnp.int32))
    fine_next = jnp.moveaxis(fine_all, 0, 1).reshape(27, NX, NY, BZ)
    coarse_next = jnp.moveaxis(coarse_all, 0, 1).reshape(27, NX // 2, NY // 2, BZ // 2)
    return fine_next, coarse_next
```

```python
import jax
import jax.numpy as jnp
from jax import lax
from jax.experimental import pallas as pl
from jax.experimental.pallas import tpu as pltpu
from jax.sharding import PartitionSpec as P

F32 = jnp.float32
Q = 27
LANES = 128
OCTETS = [(8 * o, min(8, Q - 8 * o)) for o in range(4)]
STEP = [(q // 9 - 1, q // 3 % 3 - 1, q % 3 - 1) for q in range(Q)]
HIGH_X = [q for q in range(Q) if STEP[q][0] == 1]
LOW_X = [q for q in range(Q) if STEP[q][0] == -1]
HIGH_Y = [q for q in range(Q) if STEP[q][1] == 1]
LOW_Y = [q for q in range(Q) if STEP[q][1] == -1]

VMEM = pl.BlockSpec(memory_space=pltpu.VMEM)
SMEM = pl.BlockSpec(memory_space=pltpu.SMEM)
ANY = pl.BlockSpec(memory_space=pl.ANY)
LIMIT = 16 << 20


def params(**more):
    return pltpu.CompilerParams(vmem_limit_bytes=LIMIT, **more)


def struct(shape, dtype=F32):
    return jax.ShapeDtypeStruct(shape, dtype)


def ring(axis, by):
    peers = lax.axis_size(axis)
    return [(i, (i + by) % peers) for i in range(peers)]


X_SECOND, X_FINE = 32, 48
Y_FINE = 72


def roll_lane(v, by):
    return v if by == 0 else pltpu.roll(v, by % v.shape[1], 1)


def roll_sub(v, by):
    return v if by == 0 else pltpu.roll(v, by % v.shape[0], 0)


def lane_iota():
    return lax.broadcasted_iota(jnp.int32, (8, LANES), 1)


def sub_iota():
    return lax.broadcasted_iota(jnp.int32, (8, LANES), 0)


def take(v, idx, axis):
    return jnp.take_along_axis(v, idx, axis=axis)


def pack_x_kernel(sx, fine, coarse, up, down, f_low, f_high, c_low, c_high, sems):
    cx = sx // 2
    copies = [
        pltpu.make_async_copy(fine.at[sx - 1], f_high, sems.at[0]),
        pltpu.make_async_copy(coarse.at[cx - 1], c_high, sems.at[1]),
        pltpu.make_async_copy(fine.at[0], f_low, sems.at[2]),
        pltpu.make_async_copy(coarse.at[0], c_low, sems.at[3]),
    ]
    for c in copies:
        c.start()
    sy = f_low.shape[0]
    nzc = c_low.shape[2]
    for k, (out, f, c, qs) in enumerate(((up, f_high, c_high, HIGH_X), (down, f_low, c_low, LOW_X))):
        copies[2 * k].wait()
        copies[2 * k + 1].wait()
        out[0:Q, 0:nzc] = c[0]
        out[0:Q, nzc : 2 * nzc] = c[1]
        out[X_SECOND : X_SECOND + 16, 0:nzc] = c[2, 0:16]
        out[X_SECOND : X_SECOND + Q - 16, nzc : 2 * nzc] = c[2, 16:Q]
        for y in range(sy):
            out[X_FINE + 9 * y : X_FINE + 9 * y + 9] = f[y, qs[0] : qs[0] + 9]


def fine_plane(fine, from_low, from_high, y):
    sx = fine.shape[0]
    base = X_FINE + 9 * y
    rows = [None] * Q
    for q0, n in OCTETS:
        cells = [fine[x, y, q0 : q0 + n] for x in range(sx)]
        low, high = (cells[0], cells[0])
        if q0 == 16:
            low = from_low[base - 2 : base + 6]
        if q0 == 24:
            low = from_low[base + 6 : base + 9]
        if q0 == 0:
            high = from_high[base : base + 8]
        if q0 == 8:
            high = jnp.broadcast_to(from_high[base + 8 : base + 9], (8, LANES))
        tile = jnp.swapaxes(jnp.stack([low, *cells, high]), 0, 1)
        for k in range(n):
            rows[q0 + k] = tile[k]
    return rows


def coarse_ghost(msg, Y, q0, n, nzc):
    if Y == 0:
        return msg[q0 : q0 + n, 0:nzc]
    if Y == 1:
        return roll_lane(msg[q0 : q0 + n], nzc)[:, 0:nzc]
    if q0 < 16:
        return msg[X_SECOND + q0 : X_SECOND + q0 + n, 0:nzc]
    return roll_lane(msg[X_SECOND + q0 - 16 : X_SECOND + q0 - 16 + n], nzc)[:, 0:nzc]


def coarse_plane(coarse, from_low, from_high, Y):
    cx, nzc = coarse.shape[0], coarse.shape[3]
    rows = [None] * Q
    for q0, n in OCTETS:
        cells = [coarse[X, Y, q0 : q0 + n] for X in range(cx)]
        low = coarse_ghost(from_low, Y, q0, n, nzc)
        high = coarse_ghost(from_high, Y, q0, n, nzc)
        fill = [high] * (8 - cx - 2)
        tile = jnp.swapaxes(jnp.stack([low, *cells, high, *fill]), 0, 1)
        for k in range(n):
            rows[q0 + k] = tile[k]
    return rows


def pack_y_kernel(fine, coarse, from_low, from_high, up, down, w_edge, c_all):
    sy, cy, nzc = fine.shape[1], coarse.shape[1], coarse.shape[3]
    for Y in range(cy):
        for q, v in enumerate(coarse_plane(coarse, from_low, from_high, Y)):
            c_all[q, Y, :, 0:nzc] = v
    low_half = lane_iota() < nzc
    for out, e, y, Y, qs in ((up, 1, sy - 1, cy - 1, HIGH_Y), (down, 0, 0, 0, LOW_Y)):
        for p in range((Q + 1) // 2):
            a = c_all[2 * p, Y]
            if 2 * p + 1 < Q:
                a = jnp.where(low_half, a, roll_lane(c_all[2 * p + 1, Y], nzc))
            out[5 * p : 5 * p + 5] = a[0:5]
        rows = fine_plane(fine, from_low, from_high, y)
        for q in range(Q):
            w_edge[q, e] = rows[q]
        for k, q in enumerate(qs):
            out[Y_FINE + 8 * k : Y_FINE + 8 * k + 8] = rows[q]


def explode_tables(nzc):
    lane, sub = lane_iota(), sub_iota()
    za = lane >> 1
    zb = jnp.clip(za + jnp.where((lane & 1) == 1, 1, -1), 0, nzc - 1)
    x = sub + 1
    xa = x >> 1
    xb = xa + jnp.where((x & 1) == 1, 1, -1)
    return za, zb, xa, xb


def explode_zx(v, tables):
    za, zb, xa, xb = tables
    t = 0.75 * take(v, za, 1) + 0.25 * take(v, zb, 1)
    return 0.75 * take(t, xa, 0) + 0.25 * take(t, xb, 0)


def y_pair(j):
    a = (j + 1) >> 1
    return a, a + (1 if (j + 1) & 1 else -1)


def explode_y(ex, j):
    a, b = y_pair(j)
    return 0.75 * ex[a] + 0.25 * ex[b]


def forward(m0, m1, m2):
    pair = m0 + m2
    return pair + 4.0 * m1, m2 - m0, pair


def collide(g, keep, gain):
    t = [None] * Q
    for r in range(9):
        t[r], t[9 + r], t[18 + r] = forward(g[r], g[9 + r], g[18 + r])
    cols = [(t[c] + t[6 + c]) + 4.0 * t[3 + c] for c in range(3)]
    density = (cols[0] + cols[2]) + 4.0 * cols[1]
    inv = 1.0 / density
    rows = [(t[3 * b] + t[3 * b + 2]) + 4.0 * t[3 * b + 1] for b in (0, 2)]
    uy = (rows[1] - rows[0]) * inv
    uz = (cols[2] - cols[0]) * inv
    dcols = [(t[9 + c] + t[15 + c]) + 4.0 * t[12 + c] for c in range(3)]
    ux = ((dcols[0] + dcols[2]) + 4.0 * dcols[1]) * inv
    for r in range(9):
        t0, d, pair = t[r], t[9 + r], t[18 + r]
        t1 = d - ux * t0
        t[9 + r], t[18 + r] = t1, pair - ux * (d + t1)
    for u, lines in ((uy, [(9 * a + c, 3) for a in range(3) for c in range(3)]),
                     (uz, [(9 * a + 3 * b, 1) for a in range(3) for b in range(3)])):
        for at, by in lines:
            t0, d, pair = forward(t[at], t[at + by], t[at + 2 * by])
            t1 = d - u * t0
            t[at], t[at + by], t[at + 2 * by] = t0, t1, pair - u * (d + t1)
    for q in range(Q):
        t[q] = keep[q] * t[q]
        if q in gain:
            t[q] = t[q] + gain[q] * density
    for u, lines in ((uz, [(9 * a + 3 * b, 1) for a in range(3) for b in range(3)]),
                     (uy, [(9 * a + c, 3) for a in range(3) for c in range(3)]),
                     (ux, [(r, 9) for r in range(9)])):
        for at, by in lines:
            t0, t1, t2 = t[at], t[at + by], t[at + 2 * by]
            d = t1 + u * t0
            s = t2 + u * (t1 + d)
            t[at], t[at + by], t[at + 2 * by] = s - d, 0.5 * (t0 - s), s + d
    return t


EVEN = [9 * a + 3 * b + c for a in (0, 2) for b in (0, 2) for c in (0, 2)]


def gain_of(q):
    return (1.0 if q // 9 == 0 else 1.0 / 3.0) * (1.0 if q // 3 % 3 == 0 else 1.0 / 3.0) * (
        1.0 if q % 3 == 0 else 1.0 / 3.0)


def pull(source, center, step_mask):
    out = []
    for q in range(Q):
        ex, ey, ez = STEP[q]
        v = roll_lane(roll_sub(source(q), ex), ez)
        mask = step_mask(ex, ey, ez)
        if mask is not None:
            v = jnp.where(mask, center(26 - q), v)
        out.append(v)
    return out


def edge_masks(height):
    lane = lane_iota()
    return {1: lane == 0, -1: lane == height - 1}


def fine_mask(y, first_wall, flags, edges):
    def mask_of(ex, ey, ez):
        m = None
        if (ex, ey, ez) == (0, 0, 0):
            return None
        s = y - ey - first_wall
        if s in (0, 1):
            m = roll_lane(roll_sub(flags[s], ex), ez) == 1
        if ez != 0:
            m = edges[ez] if m is None else m | edges[ez]
        return m

    return mask_of


def store_rows(rows, out, y, xs, width):
    for q0, n in OCTETS:
        tile = jnp.swapaxes(jnp.stack(rows[q0 : q0 + n]), 0, 1)
        for k, x in enumerate(xs):
            out[k, y, q0 : q0 + n] = tile[x][:, 0:width]


def coalesce(first, second, index):
    rows = []
    for a, b in zip(first, second):
        s = a + b
        s = s + roll_sub(s, -1)
        s = s + roll_lane(s, -1)
        rows.append(0.125 * take(s, index, 1))
    return rows


def inner_kernel(fine, coarse, from_low, from_high, c_all, obstacle, level, rates,
                 out, c_out, w_in, ex_in, coef, levels, flag_out, c_wall, f_buf, c_buf, sems):
    sx, sy, nz = fine.shape[0], fine.shape[1], fine.shape[3]
    cx, cy, nzc = coarse.shape[0], coarse.shape[1], coarse.shape[3]
    row, col = lax.axis_index("stream"), lax.axis_index("span")
    n_row, n_col = level.shape
    own = level[row, col]
    lane, sub = lane_iota(), sub_iota()
    at_row = [lax.rem(row + n_row - 1, n_row), row, lax.rem(row + 1, n_row)]
    at_col = [lax.rem(col + n_col - 1, n_col), col, lax.rem(col + 1, n_col)]
    for k in range(3):
        v = jnp.where(sub == 0, level[at_row[0], at_col[k]],
                      jnp.where(sub == sx + 1, level[at_row[2], at_col[k]], level[at_row[1], at_col[k]]))
        levels[k] = v
    refined_block = jnp.full((8, LANES), own, jnp.int32) == 1
    keep, gain = {}, {}
    for q in range(Q):
        s = jnp.full((8, LANES), rates[q], F32)
        s = jnp.where(refined_block, s, 1.0 / (2.0 / s - 0.5))
        keep[q] = 0.125 - 0.125 * s
        coef[q] = keep[q]
        if q in EVEN:
            gain[q] = (0.125 * gain_of(q)) * s
            coef[Q + EVEN.index(q)] = gain[q]
    tables = explode_tables(nzc)
    for Y in range(cy):
        for q in range(Q):
            ex_in[q, Y] = explode_zx(c_all[q, Y], tables)
    mid = sy // 2
    flags = []
    for y in (mid - 1, mid):
        v = jnp.zeros((8, LANES), jnp.int32)
        for x in (sx // 2 - 1, sx // 2):
            v = jnp.where(sub == x + 1, jnp.broadcast_to(obstacle[x, y : y + 1, :], (8, LANES)), v)
        flags.append(v)
        flag_out[len(flags) - 1] = v
    both = jnp.maximum(flags[0], flags[1])
    both = jnp.maximum(both, roll_sub(both, -1))
    both = jnp.maximum(both, roll_lane(both, -1))
    half = (2 * lane) & (LANES - 1)
    both = take(both, half, 1)
    both = jnp.broadcast_to(both[sx // 2 : sx // 2 + 1], (8, LANES))
    wall = jnp.where((sub == 1 + cx // 2) & (lane < nzc), both, 0)
    c_wall[...] = wall
    edges = edge_masks(nz)

    @pl.when(own == 1)
    def _():
        near = levels[1] == 1
        for y in range(1, sy - 1):
            rows = fine_plane(fine, from_low, from_high, y)
            for q in range(Q):
                v = rows[q]
                if STEP[q][0] != 0:
                    a, b = y_pair(y + 1)
                    v = jnp.where(near, v, 0.75 * ex_in[q, a - 1] + 0.25 * ex_in[q, b - 1])
                w_in[q, y - 1] = v
        results = []
        for t, y in enumerate((mid - 1, mid)):
            pulled = pull(lambda q: w_in[q, y - 1 - STEP[q][1]], lambda q: w_in[q, y - 1],
                          fine_mask(y, mid - 1, flags, edges))
            new = collide(pulled, coef, {q: coef[Q + k] for k, q in enumerate(EVEN)})
            stay = flags[t] == 1
            new = [jnp.where(stay, w_in[q, y - 1], new[q]) for q in range(Q)]
            store_rows(new, f_buf, t, range(1, sx + 1), nz)
            results.append(new)
        store_rows(coalesce(results[0], results[1], half), c_buf, 0, range(1, sx + 1, 2), nzc)

    @pl.when(own != 1)
    def _():
        for t, y in enumerate((mid - 1, mid)):
            a, b = y_pair(y + 1)
            rows = [0.75 * ex_in[q, a - 1] + 0.25 * ex_in[q, b - 1] for q in range(Q)]
            store_rows(rows, f_buf, t, range(1, sx + 1), nz)
        Y = cy // 2
        coarse_pull(lambda q, J: c_all[q, J - 1], Y + 1, wall, coef, c_buf, 0, nzc, cx, 1 + cy // 2)

    copies = [pltpu.make_async_copy(f_buf, out.at[:, pl.ds(mid - 1, 2)], sems.at[0]),
              pltpu.make_async_copy(c_buf, c_out.at[:, pl.ds(cy // 2, 1)], sems.at[1])]
    for c in copies:
        c.start()
    for c in copies:
        c.wait()


def coarse_pull(plane, J, wall, coef, buf, at, nzc, cx, wall_row):
    edges = edge_masks(nzc)

    def mask_of(ex, ey, ez):
        m = None
        if (ex, ey, ez) == (0, 0, 0):
            return None
        if J - ey == wall_row:
            m = roll_lane(roll_sub(wall, ex), ez) == 1
        if ez != 0:
            m = edges[ez] if m is None else m | edges[ez]
        return m

    pulled = pull(lambda q: plane(q, J - STEP[q][1]), lambda q: plane(q, J), mask_of)
    new = collide(pulled, coef, {q: coef[Q + k] for k, q in enumerate(EVEN)})
    if J == wall_row:
        stay = wall == 1
        new = [jnp.where(stay, plane(q, J), new[q]) for q in range(Q)]
    store_rows(new, buf, at, range(1, cx + 1), nzc)


def outer_kernel(from_below, from_above, w_edge, w_in, c_all, ex_in, coef, levels, flags, c_wall, level,
                 _out_in, _c_in, out, c_out, ex_g, c_g, w_g, w_e, f_low, f_high, c_low, c_high, sems):
    sx, sy, nz = out.shape[0], out.shape[1], out.shape[3]
    cx, cy, nzc = c_out.shape[0], c_out.shape[1], c_out.shape[3]
    own = level[lax.axis_index("stream"), lax.axis_index("span")]
    lane = lane_iota()
    tables = explode_tables(nzc)
    for e, msg in enumerate((from_below, from_above)):
        for p in range((Q + 1) // 2):
            v = msg[5 * p : 5 * p + 8]
            c_g[2 * p, e] = v
            ex_g[2 * p, e] = explode_zx(v, tables)
            if 2 * p + 1 < Q:
                v = roll_lane(v, nzc)
                c_g[2 * p + 1, e] = v
                ex_g[2 * p + 1, e] = explode_zx(v, tables)

    def exploded(q, J):
        if J == 0:
            return ex_g[q, 0]
        if J == cy + 1:
            return ex_g[q, 1]
        return ex_in[q, J - 1]

    def explode_at(q, j):
        a, b = y_pair(j)
        return 0.75 * exploded(q, a) + 0.25 * exploded(q, b)

    half = (2 * lane) & (LANES - 1)
    edges = edge_masks(nz)
    parts = ((0, f_low, c_low, (0, 1)), (1, f_high, c_high, (sy - 2, sy - 1)))

    def copies(e):
        _, f_buf, c_buf, ys = parts[e]
        return (pltpu.make_async_copy(f_buf, out.at[:, pl.ds(ys[0], 2)], sems.at[2 * e]),
                pltpu.make_async_copy(c_buf, c_out.at[:, pl.ds((cy - 1) * e, 1)], sems.at[2 * e + 1]))

    @pl.when(own == 1)
    def _():
        for e, f_buf, c_buf, ys in parts:
            msg = from_below if e == 0 else from_above
            ghost_j = 0 if e == 0 else sy + 1
            edge_j = 1 if e == 0 else sy
            far = levels[0 if e == 0 else 2] == 1
            near = levels[1] == 1
            qs = HIGH_Y if e == 0 else LOW_Y
            for k, q in enumerate(qs):
                w_g[k] = jnp.where(far, msg[Y_FINE + 8 * k : Y_FINE + 8 * k + 8], explode_at(q, ghost_j))
            for q in range(Q):
                if STEP[q][0] != 0:
                    w_e[q, e] = jnp.where(near, w_edge[q, e], explode_at(q, edge_j))
                else:
                    w_e[q, e] = w_edge[q, e]

            def plane(q, j):
                if j == ghost_j:
                    return w_g[qs.index(q)]
                if j == edge_j:
                    return w_e[q, e]
                return w_in[q, j - 2]

            results = []
            for t, y in enumerate(ys):
                pulled = pull(lambda q: plane(q, y + 1 - STEP[q][1]), lambda q: plane(q, y + 1),
                              fine_mask(y, sy // 2 - 1, flags, edges))
                new = collide(pulled, coef, {q: coef[Q + k] for k, q in enumerate(EVEN)})
                store_rows(new, f_buf, t, range(1, sx + 1), nz)
                results.append(new)
            store_rows(coalesce(results[0], results[1], half), c_buf, 0, range(1, sx + 1, 2), nzc)
            for c in copies(e):
                c.start()

    @pl.when(own != 1)
    def _():
        wall = c_wall[...]

        def plane(q, J):
            if J == 0:
                return c_g[q, 0]
            if J == cy + 1:
                return c_g[q, 1]
            return c_all[q, J - 1]

        for e, f_buf, c_buf, ys in parts:
            for t, y in enumerate(ys):
                store_rows([explode_at(q, y + 1) for q in range(Q)], f_buf, t, range(1, sx + 1), nz)
            J = 1 if e == 0 else cy
            coarse_pull(plane, J, wall, coef, c_buf, 0, nzc, cx, 1 + cy // 2)
            for c in copies(e):
                c.start()

    for e in range(2):
        for c in copies(e):
            c.wait()


def cost(flops, nbytes):
    return pl.CostEstimate(flops=flops, bytes_accessed=nbytes, transcendentals=0)


def local(fine_pops, coarse_pops, obstacle, block_level, relax_rates):
    fine = jnp.transpose(fine_pops, (1, 2, 0, 3))
    coarse = jnp.transpose(coarse_pops, (1, 2, 0, 3))
    sx, sy, _, nz = fine.shape
    cx, cy, _, nzc = coarse.shape

    x_rows = X_FINE + 8 * ((9 * sy + 7) // 8)
    x_message = struct((x_rows, LANES))
    up, down = pl.pallas_call(
        lambda *refs: pack_x_kernel(sx, *refs),
        out_shape=(x_message, x_message),
        in_specs=[ANY, ANY],
        out_specs=(VMEM, VMEM),
        scratch_shapes=[
            pltpu.VMEM((sy, Q, nz), F32),
            pltpu.VMEM((sy, Q, nz), F32),
            pltpu.VMEM((cy, Q, nzc), F32),
            pltpu.VMEM((cy, Q, nzc), F32),
            pltpu.SemaphoreType.DMA((4,)),
        ],
        compiler_params=params(),
        name="pack_x",
    )(fine, coarse)
    from_low = lax.ppermute(up, "stream", ring("stream", 1))
    from_high = lax.ppermute(down, "stream", ring("stream", -1))

    y_message = struct((Y_FINE + 72, LANES))
    up, down, w_edge, c_all = pl.pallas_call(
        pack_y_kernel,
        out_shape=(y_message, y_message, struct((Q, 2, 8, LANES)), struct((Q, cy, 8, LANES))),
        in_specs=[VMEM] * 4,
        out_specs=(VMEM,) * 4,
        compiler_params=params(),
        name="pack_y",
    )(fine, coarse, from_low, from_high)
    from_below = lax.ppermute(up, "span", ring("span", 1))
    from_above = lax.ppermute(down, "span", ring("span", -1))

    fine_shape, coarse_shape = struct(fine.shape), struct(coarse.shape)
    out, c_out, w_in, ex_in, coef, levels, flags, c_wall = pl.pallas_call(
        inner_kernel,
        out_shape=(
            fine_shape,
            coarse_shape,
            struct((Q, sy - 2, 8, LANES)),
            struct((Q, cy, 8, LANES)),
            struct((Q + len(EVEN), 8, LANES)),
            struct((3, 8, LANES), jnp.int32),
            struct((2, 8, LANES), jnp.int32),
            struct((8, LANES), jnp.int32),
        ),
        in_specs=[VMEM] * 6 + [SMEM] * 2,
        out_specs=(ANY, ANY) + (VMEM,) * 6,
        scratch_shapes=[
            pltpu.VMEM((sx, 2, Q, nz), F32),
            pltpu.VMEM((cx, 1, Q, nzc), F32),
            pltpu.SemaphoreType.DMA((2,)),
        ],
        compiler_params=params(),
        cost_estimate=cost(20_000_000, 1_000_000),
        name="inner",
    )(fine, coarse, from_low, from_high, c_all, obstacle, block_level, relax_rates)

    out, c_out = pl.pallas_call(
        outer_kernel,
        out_shape=(fine_shape, coarse_shape),
        in_specs=[VMEM] * 10 + [SMEM, ANY, ANY],
        out_specs=(ANY, ANY),
        scratch_shapes=[
            pltpu.VMEM((Q, 2, 8, LANES), F32),
            pltpu.VMEM((Q, 2, 8, LANES), F32),
            pltpu.VMEM((9, 8, LANES), F32),
            pltpu.VMEM((Q, 2, 8, LANES), F32),
            pltpu.VMEM((sx, 2, Q, nz), F32),
            pltpu.VMEM((sx, 2, Q, nz), F32),
            pltpu.VMEM((cx, 1, Q, nzc), F32),
            pltpu.VMEM((cx, 1, Q, nzc), F32),
            pltpu.SemaphoreType.DMA((4,)),
        ],
        input_output_aliases={11: 0, 12: 1},
        compiler_params=params(),
        name="outer",
    )(from_below, from_above, w_edge, w_in, c_all, ex_in, coef, levels, flags, c_wall, block_level,
      out, c_out)
    return jnp.transpose(out, (2, 0, 1, 3)), jnp.transpose(c_out, (2, 0, 1, 3))


def solution(mesh):
    placed = (
        P(None, "stream", "span", None),
        P(None, "stream", "span", None),
        P("stream", "span", None),
        P(),
        P(),
    )
    return jax.shard_map(
        local,
        mesh=mesh,
        in_specs=placed,
        out_specs=(P(None, "stream", "span", None), P(None, "stream", "span", None)),
        check_vma=False,
    )
```

```python
import jax
import jax.numpy as jnp
from jax import lax
from jax.experimental import pallas as pl
from jax.experimental.pallas import tpu as pltpu
from jax.sharding import PartitionSpec as P

F32 = jnp.float32
Q = 27
LANES = 128
OCTETS = [(8 * o, min(8, Q - 8 * o)) for o in range(4)]
STEP = [(q // 9 - 1, q // 3 % 3 - 1, q % 3 - 1) for q in range(Q)]
HIGH_X = [q for q in range(Q) if STEP[q][0] == 1]
LOW_X = [q for q in range(Q) if STEP[q][0] == -1]
HIGH_Y = [q for q in range(Q) if STEP[q][1] == 1]
LOW_Y = [q for q in range(Q) if STEP[q][1] == -1]

VMEM = pl.BlockSpec(memory_space=pltpu.VMEM)
SMEM = pl.BlockSpec(memory_space=pltpu.SMEM)
ANY = pl.BlockSpec(memory_space=pl.ANY)
HBM = pl.BlockSpec(memory_space=pltpu.HBM)
LIMIT = 16 << 20


def params(**more):
    return pltpu.CompilerParams(vmem_limit_bytes=LIMIT, **more)


def struct(shape, dtype=F32):
    return jax.ShapeDtypeStruct(shape, dtype)


def ring(axis, by):
    peers = lax.axis_size(axis)
    return [(i, (i + by) % peers) for i in range(peers)]


X_SECOND, X_FINE = 32, 48
Y_FINE = 72


def roll_lane(v, by):
    return v if by == 0 else pltpu.roll(v, by % v.shape[1], 1)


def roll_sub(v, by):
    return v if by == 0 else pltpu.roll(v, by % v.shape[0], 0)


def lane_iota():
    return lax.broadcasted_iota(jnp.int32, (8, LANES), 1)


def sub_iota():
    return lax.broadcasted_iota(jnp.int32, (8, LANES), 0)


def take(v, idx, axis):
    return jnp.take_along_axis(v, idx, axis=axis)


def pack_x_kernel(sx, fine, coarse, up, down, f_low, f_high, c_low, c_high, sems):
    cx = sx // 2
    copies = [
        pltpu.make_async_copy(fine.at[sx - 1], f_high, sems.at[0]),
        pltpu.make_async_copy(coarse.at[cx - 1], c_high, sems.at[1]),
        pltpu.make_async_copy(fine.at[0], f_low, sems.at[2]),
        pltpu.make_async_copy(coarse.at[0], c_low, sems.at[3]),
    ]
    for c in copies:
        c.start()
    sy = f_low.shape[0]
    nzc = c_low.shape[2]
    for k, (out, f, c, qs) in enumerate(((up, f_high, c_high, HIGH_X), (down, f_low, c_low, LOW_X))):
        copies[2 * k].wait()
        copies[2 * k + 1].wait()
        out[0:Q, 0:nzc] = c[0]
        out[0:Q, nzc : 2 * nzc] = c[1]
        out[X_SECOND : X_SECOND + 16, 0:nzc] = c[2, 0:16]
        out[X_SECOND : X_SECOND + Q - 16, nzc : 2 * nzc] = c[2, 16:Q]
        for y in range(sy):
            out[X_FINE + 9 * y : X_FINE + 9 * y + 9] = f[y, qs[0] : qs[0] + 9]


def fine_plane(fine, from_low, from_high, y):
    sx = fine.shape[0]
    base = X_FINE + 9 * y
    rows = [None] * Q
    for q0, n in OCTETS:
        cells = [fine[x, y, q0 : q0 + n] for x in range(sx)]
        low, high = (cells[0], cells[0])
        if q0 == 16:
            low = from_low[base - 2 : base + 6]
        if q0 == 24:
            low = from_low[base + 6 : base + 9]
        if q0 == 0:
            high = from_high[base : base + 8]
        if q0 == 8:
            high = jnp.broadcast_to(from_high[base + 8 : base + 9], (8, LANES))
        tile = jnp.swapaxes(jnp.stack([low, *cells, high]), 0, 1)
        for k in range(n):
            rows[q0 + k] = tile[k]
    return rows


def coarse_ghost(msg, Y, q0, n, nzc):
    if Y == 0:
        return msg[q0 : q0 + n, 0:nzc]
    if Y == 1:
        return roll_lane(msg[q0 : q0 + n], nzc)[:, 0:nzc]
    if q0 < 16:
        return msg[X_SECOND + q0 : X_SECOND + q0 + n, 0:nzc]
    return roll_lane(msg[X_SECOND + q0 - 16 : X_SECOND + q0 - 16 + n], nzc)[:, 0:nzc]


def coarse_plane(coarse, from_low, from_high, Y):
    cx, nzc = coarse.shape[0], coarse.shape[3]
    rows = [None] * Q
    for q0, n in OCTETS:
        cells = [coarse[X, Y, q0 : q0 + n] for X in range(cx)]
        low = coarse_ghost(from_low, Y, q0, n, nzc)
        high = coarse_ghost(from_high, Y, q0, n, nzc)
        fill = [high] * (8 - cx - 2)
        tile = jnp.swapaxes(jnp.stack([low, *cells, high, *fill]), 0, 1)
        for k in range(n):
            rows[q0 + k] = tile[k]
    return rows


def pack_y_kernel(fine, coarse, from_low, from_high, up, down, w_edge, c_all):
    sy, cy, nzc = fine.shape[1], coarse.shape[1], coarse.shape[3]
    for Y in range(cy):
        for q, v in enumerate(coarse_plane(coarse, from_low, from_high, Y)):
            c_all[q, Y, :, 0:nzc] = v
    low_half = lane_iota() < nzc
    for out, e, y, Y, qs in ((up, 1, sy - 1, cy - 1, HIGH_Y), (down, 0, 0, 0, LOW_Y)):
        for p in range((Q + 1) // 2):
            a = c_all[2 * p, Y]
            if 2 * p + 1 < Q:
                a = jnp.where(low_half, a, roll_lane(c_all[2 * p + 1, Y], nzc))
            out[5 * p : 5 * p + 5] = a[0:5]
        rows = fine_plane(fine, from_low, from_high, y)
        for q in range(Q):
            w_edge[q, e] = rows[q]
        for k, q in enumerate(qs):
            out[Y_FINE + 8 * k : Y_FINE + 8 * k + 8] = rows[q]


def explode_tables(nzc):
    lane, sub = lane_iota(), sub_iota()
    za = lane >> 1
    zb = jnp.clip(za + jnp.where((lane & 1) == 1, 1, -1), 0, nzc - 1)
    x = sub + 1
    xa = x >> 1
    xb = xa + jnp.where((x & 1) == 1, 1, -1)
    return za, zb, xa, xb


def explode_zx(v, tables):
    za, zb, xa, xb = tables
    t = 0.75 * take(v, za, 1) + 0.25 * take(v, zb, 1)
    return 0.75 * take(t, xa, 0) + 0.25 * take(t, xb, 0)


def y_pair(j):
    a = (j + 1) >> 1
    return a, a + (1 if (j + 1) & 1 else -1)


def explode_y(ex, j):
    a, b = y_pair(j)
    return 0.75 * ex[a] + 0.25 * ex[b]


def forward(m0, m1, m2):
    pair = m0 + m2
    return pair + 4.0 * m1, m2 - m0, pair


def collide(g, keep, gain):
    t = [None] * Q
    for r in range(9):
        t[r], t[9 + r], t[18 + r] = forward(g[r], g[9 + r], g[18 + r])
    cols = [(t[c] + t[6 + c]) + 4.0 * t[3 + c] for c in range(3)]
    density = (cols[0] + cols[2]) + 4.0 * cols[1]
    inv = 1.0 / density
    rows = [(t[3 * b] + t[3 * b + 2]) + 4.0 * t[3 * b + 1] for b in (0, 2)]
    uy = (rows[1] - rows[0]) * inv
    uz = (cols[2] - cols[0]) * inv
    dcols = [(t[9 + c] + t[15 + c]) + 4.0 * t[12 + c] for c in range(3)]
    ux = ((dcols[0] + dcols[2]) + 4.0 * dcols[1]) * inv
    for r in range(9):
        t0, d, pair = t[r], t[9 + r], t[18 + r]
        t1 = d - ux * t0
        t[9 + r], t[18 + r] = t1, pair - ux * (d + t1)
    for u, lines in ((uy, [(9 * a + c, 3) for a in range(3) for c in range(3)]),
                     (uz, [(9 * a + 3 * b, 1) for a in range(3) for b in range(3)])):
        for at, by in lines:
            t0, d, pair = forward(t[at], t[at + by], t[at + 2 * by])
            t1 = d - u * t0
            t[at], t[at + by], t[at + 2 * by] = t0, t1, pair - u * (d + t1)
    for q in range(Q):
        t[q] = keep[q] * t[q]
        if q in gain:
            t[q] = t[q] + gain[q] * density
    for u, lines in ((uz, [(9 * a + 3 * b, 1) for a in range(3) for b in range(3)]),
                     (uy, [(9 * a + c, 3) for a in range(3) for c in range(3)]),
                     (ux, [(r, 9) for r in range(9)])):
        for at, by in lines:
            t0, t1, t2 = t[at], t[at + by], t[at + 2 * by]
            d = t1 + u * t0
            s = t2 + u * (t1 + d)
            t[at], t[at + by], t[at + 2 * by] = s - d, 0.5 * (t0 - s), s + d
    return t


EVEN = [9 * a + 3 * b + c for a in (0, 2) for b in (0, 2) for c in (0, 2)]


def gain_of(q):
    return (1.0 if q // 9 == 0 else 1.0 / 3.0) * (1.0 if q // 3 % 3 == 0 else 1.0 / 3.0) * (
        1.0 if q % 3 == 0 else 1.0 / 3.0)


def pull(source, center, step_mask):
    out = []
    for q in range(Q):
        ex, ey, ez = STEP[q]
        v = roll_lane(roll_sub(source(q), ex), ez)
        mask = step_mask(ex, ey, ez)
        if mask is not None:
            v = jnp.where(mask, center(26 - q), v)
        out.append(v)
    return out


def edge_masks(height):
    lane = lane_iota()
    return {1: lane == 0, -1: lane == height - 1}


def fine_mask(y, first_wall, flags, edges):
    def mask_of(ex, ey, ez):
        m = None
        if (ex, ey, ez) == (0, 0, 0):
            return None
        s = y - ey - first_wall
        if s in (0, 1):
            m = roll_lane(roll_sub(flags[s], ex), ez) == 1
        if ez != 0:
            m = edges[ez] if m is None else m | edges[ez]
        return m

    return mask_of


def store_rows(rows, out, y, xs, width):
    for q0, n in OCTETS:
        tile = jnp.swapaxes(jnp.stack(rows[q0 : q0 + n]), 0, 1)
        for k, x in enumerate(xs):
            out[k, y, q0 : q0 + n] = tile[x][:, 0:width]


def coalesce(first, second, index):
    rows = []
    for a, b in zip(first, second):
        s = a + b
        s = s + roll_sub(s, -1)
        s = s + roll_lane(s, -1)
        rows.append(0.125 * take(s, index, 1))
    return rows


def inner_kernel(fine, coarse, from_low, from_high, c_all, obstacle, level, rates,
                 out, c_out, w_in, ex_in, coef, levels, flag_out, c_wall, f_buf, c_buf, sems):
    sx, sy, nz = fine.shape[0], fine.shape[1], fine.shape[3]
    cx, cy, nzc = coarse.shape[0], coarse.shape[1], coarse.shape[3]
    row, col = lax.axis_index("stream"), lax.axis_index("span")
    n_row, n_col = level.shape
    own = level[row, col]
    lane, sub = lane_iota(), sub_iota()
    at_row = [lax.rem(row + n_row - 1, n_row), row, lax.rem(row + 1, n_row)]
    at_col = [lax.rem(col + n_col - 1, n_col), col, lax.rem(col + 1, n_col)]
    for k in range(3):
        v = jnp.where(sub == 0, level[at_row[0], at_col[k]],
                      jnp.where(sub == sx + 1, level[at_row[2], at_col[k]], level[at_row[1], at_col[k]]))
        levels[k] = v
    refined_block = jnp.full((8, LANES), own, jnp.int32) == 1
    keep, gain = {}, {}
    for q in range(Q):
        s = jnp.full((8, LANES), rates[q], F32)
        s = jnp.where(refined_block, s, 1.0 / (2.0 / s - 0.5))
        keep[q] = 0.125 - 0.125 * s
        coef[q] = keep[q]
        if q in EVEN:
            gain[q] = (0.125 * gain_of(q)) * s
            coef[Q + EVEN.index(q)] = gain[q]
    tables = explode_tables(nzc)
    for Y in range(cy):
        for q in range(Q):
            ex_in[q, Y] = explode_zx(c_all[q, Y], tables)
    mid = sy // 2
    flags = []
    for y in (mid - 1, mid):
        v = jnp.zeros((8, LANES), jnp.int32)
        for x in (sx // 2 - 1, sx // 2):
            v = jnp.where(sub == x + 1, jnp.broadcast_to(obstacle[x, y : y + 1, :], (8, LANES)), v)
        flags.append(v)
        flag_out[len(flags) - 1] = v
    both = jnp.maximum(flags[0], flags[1])
    both = jnp.maximum(both, roll_sub(both, -1))
    both = jnp.maximum(both, roll_lane(both, -1))
    half = (2 * lane) & (LANES - 1)
    both = take(both, half, 1)
    both = jnp.broadcast_to(both[sx // 2 : sx // 2 + 1], (8, LANES))
    wall = jnp.where((sub == 1 + cx // 2) & (lane < nzc), both, 0)
    c_wall[...] = wall
    edges = edge_masks(nz)

    @pl.when(own == 1)
    def _():
        near = levels[1] == 1
        for y in range(1, sy - 1):
            rows = fine_plane(fine, from_low, from_high, y)
            for q in range(Q):
                v = rows[q]
                if STEP[q][0] != 0:
                    a, b = y_pair(y + 1)
                    v = jnp.where(near, v, 0.75 * ex_in[q, a - 1] + 0.25 * ex_in[q, b - 1])
                w_in[q, y - 1] = v
        results = []
        for t, y in enumerate((mid - 1, mid)):
            pulled = pull(lambda q: w_in[q, y - 1 - STEP[q][1]], lambda q: w_in[q, y - 1],
                          fine_mask(y, mid - 1, flags, edges))
            new = collide(pulled, coef, {q: coef[Q + k] for k, q in enumerate(EVEN)})
            stay = flags[t] == 1
            new = [jnp.where(stay, w_in[q, y - 1], new[q]) for q in range(Q)]
            store_rows(new, f_buf, t, range(1, sx + 1), nz)
            results.append(new)
        store_rows(coalesce(results[0], results[1], half), c_buf, 0, range(1, sx + 1, 2), nzc)

    @pl.when(own != 1)
    def _():
        for t, y in enumerate((mid - 1, mid)):
            a, b = y_pair(y + 1)
            rows = [0.75 * ex_in[q, a - 1] + 0.25 * ex_in[q, b - 1] for q in range(Q)]
            store_rows(rows, f_buf, t, range(1, sx + 1), nz)
        Y = cy // 2
        coarse_pull(lambda q, J: c_all[q, J - 1], Y + 1, wall, coef, c_buf, 0, nzc, cx, 1 + cy // 2)

    copies = [pltpu.make_async_copy(f_buf, out.at[:, pl.ds(mid - 1, 2)], sems.at[0]),
              pltpu.make_async_copy(c_buf, c_out.at[:, pl.ds(cy // 2, 1)], sems.at[1])]
    for c in copies:
        c.start()
    for c in copies:
        c.wait()


def coarse_pull(plane, J, wall, coef, buf, at, nzc, cx, wall_row):
    edges = edge_masks(nzc)

    def mask_of(ex, ey, ez):
        m = None
        if (ex, ey, ez) == (0, 0, 0):
            return None
        if J - ey == wall_row:
            m = roll_lane(roll_sub(wall, ex), ez) == 1
        if ez != 0:
            m = edges[ez] if m is None else m | edges[ez]
        return m

    pulled = pull(lambda q: plane(q, J - STEP[q][1]), lambda q: plane(q, J), mask_of)
    new = collide(pulled, coef, {q: coef[Q + k] for k, q in enumerate(EVEN)})
    if J == wall_row:
        stay = wall == 1
        new = [jnp.where(stay, plane(q, J), new[q]) for q in range(Q)]
    store_rows(new, buf, at, range(1, cx + 1), nzc)


def outer_kernel(from_below, from_above, w_edge, w_in, c_all, ex_in, coef, levels, flags, c_wall, level,
                 _out_in, _c_in, out, c_out, ex_g, c_g, w_g, w_e, f_low, f_high, c_low, c_high, sems):
    sx, sy, nz = out.shape[0], out.shape[1], out.shape[3]
    cx, cy, nzc = c_out.shape[0], c_out.shape[1], c_out.shape[3]
    own = level[lax.axis_index("stream"), lax.axis_index("span")]
    lane = lane_iota()
    tables = explode_tables(nzc)
    for e, msg in enumerate((from_below, from_above)):
        for p in range((Q + 1) // 2):
            v = msg[5 * p : 5 * p + 8]
            c_g[2 * p, e] = v
            ex_g[2 * p, e] = explode_zx(v, tables)
            if 2 * p + 1 < Q:
                v = roll_lane(v, nzc)
                c_g[2 * p + 1, e] = v
                ex_g[2 * p + 1, e] = explode_zx(v, tables)

    def exploded(q, J):
        if J == 0:
            return ex_g[q, 0]
        if J == cy + 1:
            return ex_g[q, 1]
        return ex_in[q, J - 1]

    def explode_at(q, j):
        a, b = y_pair(j)
        return 0.75 * exploded(q, a) + 0.25 * exploded(q, b)

    half = (2 * lane) & (LANES - 1)
    edges = edge_masks(nz)
    parts = ((0, f_low, c_low, (0, 1)), (1, f_high, c_high, (sy - 2, sy - 1)))

    def copies(e):
        _, f_buf, c_buf, ys = parts[e]
        return (pltpu.make_async_copy(f_buf, out.at[:, pl.ds(ys[0], 2)], sems.at[2 * e]),
                pltpu.make_async_copy(c_buf, c_out.at[:, pl.ds((cy - 1) * e, 1)], sems.at[2 * e + 1]))

    @pl.when(own == 1)
    def _():
        for e, f_buf, c_buf, ys in parts:
            msg = from_below if e == 0 else from_above
            ghost_j = 0 if e == 0 else sy + 1
            edge_j = 1 if e == 0 else sy
            far = levels[0 if e == 0 else 2] == 1
            near = levels[1] == 1
            qs = HIGH_Y if e == 0 else LOW_Y
            for k, q in enumerate(qs):
                w_g[k] = jnp.where(far, msg[Y_FINE + 8 * k : Y_FINE + 8 * k + 8], explode_at(q, ghost_j))
            for q in range(Q):
                if STEP[q][0] != 0:
                    w_e[q, e] = jnp.where(near, w_edge[q, e], explode_at(q, edge_j))
                else:
                    w_e[q, e] = w_edge[q, e]

            def plane(q, j):
                if j == ghost_j:
                    return w_g[qs.index(q)]
                if j == edge_j:
                    return w_e[q, e]
                return w_in[q, j - 2]

            results = []
            for t, y in enumerate(ys):
                pulled = pull(lambda q: plane(q, y + 1 - STEP[q][1]), lambda q: plane(q, y + 1),
                              fine_mask(y, sy // 2 - 1, flags, edges))
                new = collide(pulled, coef, {q: coef[Q + k] for k, q in enumerate(EVEN)})
                store_rows(new, f_buf, t, range(1, sx + 1), nz)
                results.append(new)
            store_rows(coalesce(results[0], results[1], half), c_buf, 0, range(1, sx + 1, 2), nzc)
            for c in copies(e):
                c.start()

    @pl.when(own != 1)
    def _():
        wall = c_wall[...]

        def plane(q, J):
            if J == 0:
                return c_g[q, 0]
            if J == cy + 1:
                return c_g[q, 1]
            return c_all[q, J - 1]

        for e, f_buf, c_buf, ys in parts:
            for t, y in enumerate(ys):
                store_rows([explode_at(q, y + 1) for q in range(Q)], f_buf, t, range(1, sx + 1), nz)
            J = 1 if e == 0 else cy
            coarse_pull(plane, J, wall, coef, c_buf, 0, nzc, cx, 1 + cy // 2)
            for c in copies(e):
                c.start()

    for e in range(2):
        for c in copies(e):
            c.wait()


def cost(flops, nbytes):
    return pl.CostEstimate(flops=flops, bytes_accessed=nbytes, transcendentals=0)


def in_hbm(x):
    return pltpu.with_memory_space_constraint(x, pltpu.HBM)


def local(fine_pops, coarse_pops, obstacle, block_level, relax_rates):
    fine = jnp.transpose(fine_pops, (1, 2, 0, 3))
    coarse = jnp.transpose(coarse_pops, (1, 2, 0, 3))
    sx, sy, _, nz = fine.shape
    cx, cy, _, nzc = coarse.shape

    x_rows = X_FINE + 8 * ((9 * sy + 7) // 8)
    x_message = struct((x_rows, LANES))
    up, down = pl.pallas_call(
        lambda *refs: pack_x_kernel(sx, *refs),
        out_shape=(x_message, x_message),
        in_specs=[HBM, HBM],
        out_specs=(VMEM, VMEM),
        scratch_shapes=[
            pltpu.VMEM((sy, Q, nz), F32),
            pltpu.VMEM((sy, Q, nz), F32),
            pltpu.VMEM((cy, Q, nzc), F32),
            pltpu.VMEM((cy, Q, nzc), F32),
            pltpu.SemaphoreType.DMA((4,)),
        ],
        compiler_params=params(),
        name="pack_x",
    )(in_hbm(fine), in_hbm(coarse))
    from_low = lax.ppermute(up, "stream", ring("stream", 1))
    from_high = lax.ppermute(down, "stream", ring("stream", -1))

    y_message = struct((Y_FINE + 72, LANES))
    up, down, w_edge, c_all = pl.pallas_call(
        pack_y_kernel,
        out_shape=(y_message, y_message, struct((Q, 2, 8, LANES)), struct((Q, cy, 8, LANES))),
        in_specs=[VMEM] * 4,
        out_specs=(VMEM,) * 4,
        compiler_params=params(),
        name="pack_y",
    )(fine, coarse, from_low, from_high)
    from_below = lax.ppermute(up, "span", ring("span", 1))
    from_above = lax.ppermute(down, "span", ring("span", -1))

    fine_shape, coarse_shape = struct(fine.shape), struct(coarse.shape)
    out, c_out, w_in, ex_in, coef, levels, flags, c_wall = pl.pallas_call(
        inner_kernel,
        out_shape=(
            fine_shape,
            coarse_shape,
            struct((Q, sy - 2, 8, LANES)),
            struct((Q, cy, 8, LANES)),
            struct((Q + len(EVEN), 8, LANES)),
            struct((3, 8, LANES), jnp.int32),
            struct((2, 8, LANES), jnp.int32),
            struct((8, LANES), jnp.int32),
        ),
        in_specs=[VMEM] * 6 + [SMEM] * 2,
        out_specs=(ANY, ANY) + (VMEM,) * 6,
        scratch_shapes=[
            pltpu.VMEM((sx, 2, Q, nz), F32),
            pltpu.VMEM((cx, 1, Q, nzc), F32),
            pltpu.SemaphoreType.DMA((2,)),
        ],
        compiler_params=params(),
        cost_estimate=cost(20_000_000, 1_000_000),
        name="inner",
    )(fine, coarse, from_low, from_high, c_all, obstacle, block_level, relax_rates)

    out, c_out = pl.pallas_call(
        outer_kernel,
        out_shape=(fine_shape, coarse_shape),
        in_specs=[VMEM] * 10 + [SMEM, ANY, ANY],
        out_specs=(ANY, ANY),
        scratch_shapes=[
            pltpu.VMEM((Q, 2, 8, LANES), F32),
            pltpu.VMEM((Q, 2, 8, LANES), F32),
            pltpu.VMEM((9, 8, LANES), F32),
            pltpu.VMEM((Q, 2, 8, LANES), F32),
            pltpu.VMEM((sx, 2, Q, nz), F32),
            pltpu.VMEM((sx, 2, Q, nz), F32),
            pltpu.VMEM((cx, 1, Q, nzc), F32),
            pltpu.VMEM((cx, 1, Q, nzc), F32),
            pltpu.SemaphoreType.DMA((4,)),
        ],
        input_output_aliases={11: 0, 12: 1},
        compiler_params=params(),
        name="outer",
    )(from_below, from_above, w_edge, w_in, c_all, ex_in, coef, levels, flags, c_wall, block_level,
      out, c_out)
    return jnp.transpose(out, (2, 0, 1, 3)), jnp.transpose(c_out, (2, 0, 1, 3))


def solution(mesh):
    placed = (
        P(None, "stream", "span", None),
        P(None, "stream", "span", None),
        P("stream", "span", None),
        P(),
        P(),
    )
    return jax.shard_map(
        local,
        mesh=mesh,
        in_specs=placed,
        out_specs=(P(None, "stream", "span", None), P(None, "stream", "span", None)),
        check_vma=False,
    )
```

```python
import jax
import jax.numpy as jnp
from jax import lax
from jax.experimental import pallas as pl
from jax.experimental.pallas import tpu as pltpu
from jax.sharding import PartitionSpec as P

F32 = jnp.float32
I32 = jnp.int32
BF16 = jnp.bfloat16
Q = 27
QPAD = 32
LANES = 128
OCTETS = [(8 * o, min(8, Q - 8 * o)) for o in range(4)]
STEP = [(q // 9 - 1, q // 3 % 3 - 1, q % 3 - 1) for q in range(Q)]
HIGH_X = [q for q in range(Q) if STEP[q][0] == 1]
LOW_X = [q for q in range(Q) if STEP[q][0] == -1]
HIGH_Y = [q for q in range(Q) if STEP[q][1] == 1]
LOW_Y = [q for q in range(Q) if STEP[q][1] == -1]
EVEN = [9 * a + 3 * b + c for a in (0, 2) for b in (0, 2) for c in (0, 2)]

VMEM = pl.BlockSpec(memory_space=pltpu.VMEM)
SMEM = pl.BlockSpec(memory_space=pltpu.SMEM)
ANY = pl.BlockSpec(memory_space=pl.ANY)
LIMIT = 16 << 20

LEV_BELOW, LEV_ROW, LEV_ABOVE = 0, 1, 2
LEV_X_LOW, LEV_X_HIGH, LEV_OWN, LEV_Y_LOW, LEV_Y_HIGH = 3, 4, 5, 6, 7

X_FINE, X_MIDDLE = Q, Q + 9
Y_SECOND, Y_THIRD, Y_CORNER = Q, 2 * Q, 2 * Q + 16
Y_ROWS = 80


def fine_slot(k):
    ex = k // 3 - 1
    if ex == 0:
        return 6 * (k % 3), 6, 1
    return 36 + 7 * (k % 3 if ex < 0 else 3 + k % 3), 7, (1 if ex < 0 else 0)


def params(**more):
    return pltpu.CompilerParams(vmem_limit_bytes=LIMIT, **more)


def struct(shape, dtype=F32):
    return jax.ShapeDtypeStruct(shape, dtype)


def ring(axis, by):
    peers = lax.axis_size(axis)
    return [(i, (i + by) % peers) for i in range(peers)]


def roll_lane(v, by):
    return v if by == 0 else pltpu.roll(v, by % v.shape[1], 1)


def roll_sub(v, by):
    return v if by == 0 else pltpu.roll(v, by % v.shape[0], 0)


def iota(axis, shape=(8, LANES)):
    return lax.broadcasted_iota(I32, shape, axis)


def row8(ref, at):
    return jnp.broadcast_to(ref[at : at + 1], (8, LANES))


def dot_exact(x, m):
    high = x.astype(BF16)
    rest = x - high.astype(F32)
    middle = rest.astype(BF16)
    low = (rest - middle.astype(F32)).astype(BF16)
    return sum(jnp.dot(p, m, preferred_element_type=F32) for p in (low, middle, high))


def pair_of(i):
    a = (i + 1) >> 1
    return a, a + (1 if (i + 1) & 1 else -1)


def blend(a, b):
    return 0.75 * a + 0.25 * b


def pack_x_kernel(fine, coarse, level, up, down, f_low, f_high, c_low, c_high, lev, sems):
    sx, sy, cx = fine.shape[0], fine.shape[1], coarse.shape[0]
    copies = [
        pltpu.make_async_copy(level, lev, sems.at[4]),
        pltpu.make_async_copy(fine.at[sx - 1], f_high, sems.at[0]),
        pltpu.make_async_copy(coarse.at[cx - 1], c_high, sems.at[1]),
        pltpu.make_async_copy(fine.at[0], f_low, sems.at[2]),
        pltpu.make_async_copy(coarse.at[0], c_low, sems.at[3]),
    ]
    for c in copies:
        c.start()
    for c in copies:
        c.wait()
    cy, nzc = c_low.shape[0], c_low.shape[2]
    n_row = lev.shape[0]
    row, col = lax.axis_index("stream"), lax.axis_index("span")
    own = lev[row, col]
    for out, f, c, qs, to in ((up, f_high, c_high, HIGH_X, row + 1), (down, f_low, c_low, LOW_X, row + n_row - 1)):
        out[0:Q, 0:nzc] = c[0]
        out[0:Q, nzc : 2 * nzc] = c[cy - 1]
        for y in range(sy):
            out[X_FINE + 9 * y : X_FINE + 9 * y + 9] = f[y, qs[0] : qs[0] + 9]

        @pl.when((own != 1) | (lev[lax.rem(to, n_row), col] != 1))
        def _(out=out, c=c):
            out[X_MIDDLE : X_MIDDLE + 16, 0:nzc] = c[1, 0:16]
            out[X_MIDDLE : X_MIDDLE + Q - 16, nzc : 2 * nzc] = c[1, 16:Q]


def gain_of(q):
    return (1.0 if q // 9 == 0 else 1.0 / 3.0) * (1.0 if q // 3 % 3 == 0 else 1.0 / 3.0) * (
        1.0 if q % 3 == 0 else 1.0 / 3.0)


def tables_kernel(coarse, obstacle, level, rates, levels, coef, flags, c_wall, c_wide, refine, thin):
    cx, cy, nzc = coarse.shape[0], coarse.shape[1], coarse.shape[3]
    sx, sy, nz = obstacle.shape
    row, col = lax.axis_index("stream"), lax.axis_index("span")
    n_row, n_col = level.shape
    at_row = [lax.rem(row + n_row - 1, n_row), row, lax.rem(row + 1, n_row)]
    at_col = [lax.rem(col + n_col - 1, n_col), col, lax.rem(col + 1, n_col)]
    lane, sub = iota(1), iota(0)
    for k in range(3):
        levels[k] = jnp.where(sub == 0, level[at_row[0], at_col[k]],
                              jnp.where(sub == sx + 1, level[at_row[2], at_col[k]], level[at_row[1], at_col[k]]))
    for k, (r, c) in ((LEV_X_LOW, (0, 1)), (LEV_X_HIGH, (2, 1)), (LEV_OWN, (1, 1)), (LEV_Y_LOW, (1, 0)),
                      (LEV_Y_HIGH, (1, 2))):
        levels[k] = jnp.full((8, LANES), level[at_row[r], at_col[c]], I32)
    refined = levels[LEV_OWN] == 1
    for q in range(Q):
        s = jnp.full((8, LANES), rates[q], F32)
        s = jnp.where(refined, s, 1.0 / (2.0 / s - 0.5))
        coef[q] = 0.125 - 0.125 * s
        if q in EVEN:
            coef[Q + EVEN.index(q)] = (0.125 * gain_of(q)) * s
    planes = []
    for k, y in enumerate((sy // 2 - 1, sy // 2)):
        v = jnp.zeros((8, LANES), I32)
        for x in (sx // 2 - 1, sx // 2):
            v = jnp.where(sub == x + 1, jnp.broadcast_to(obstacle[x, y : y + 1, :], (8, LANES)), v)
        flags[k] = v
        planes.append(v)
    both = jnp.maximum(planes[0], planes[1])
    both = jnp.maximum(both, roll_sub(both, -1))
    both = jnp.maximum(both, roll_lane(both, -1))
    both = jnp.take_along_axis(both, (2 * lane) & (LANES - 1), axis=1)
    both = jnp.broadcast_to(both[sx // 2 : sx // 2 + 1], (8, LANES))
    c_wall[...] = jnp.where((sub == 1 + cx // 2) & (lane < nzc), both, 0)
    shape = (2 * nzc, 2 * nz)
    i, l = iota(0, shape), iota(1, shape)
    half, l = l // nz, l % nz
    za = (l >> 1) + half * nzc
    zb = jnp.clip((l >> 1) + jnp.where((l & 1) == 1, 1, -1), 0, nzc - 1) + half * nzc
    refine[...] = (jnp.where(i == za, 0.75, 0.0) + jnp.where(i == zb, 0.25, 0.0)).astype(BF16)
    shape = (nz, nz)
    thin[...] = jnp.where((iota(0, shape) >> 1) == iota(1, shape), 0.125, 0.0).astype(BF16)
    for Y in range(cy):
        for X in range(cx):
            c_wide[Y, X, 0:Q] = dot_exact(coarse[X, Y], refine[0:nzc, 0:nz])


def fine_plane(fine, from_low, from_high, y, mixed=None):
    sx = fine.shape[0]
    base = X_FINE + 9 * y
    rows = [None] * Q
    for q0, n in OCTETS:
        cells = [fine[x, y, q0 : q0 + n] for x in range(sx)]
        low = high = cells[0]
        if q0 == 16:
            low = from_low[base - 2 : base + 6]
        if q0 == 24:
            low = from_low[base + 6 : base + 9]
        if q0 == 0:
            high = from_high[base : base + 8]
        if q0 == 8:
            high = row8(from_high, base + 8)
        if mixed is not None:
            if q0 >= 16:
                low = mixed(0, q0, n, low)
            else:
                high = mixed(1, q0, n, high)
        tile = jnp.swapaxes(jnp.stack([low, *cells, high]), 0, 1)
        for k in range(n):
            rows[q0 + k] = tile[k]
    return rows


def coarse_plane(tile_of):
    rows = [None] * Q
    for q0, n in OCTETS:
        tiles = [tile_of(I, q0, n) for I in range(5)]
        tile = jnp.swapaxes(jnp.stack(tiles + tiles[:3]), 0, 1)
        for k in range(n):
            rows[q0 + k] = tile[k]
    return rows


def pack_y_kernel(fine, coarse, from_low, from_high, levels, up, down, w_edge):
    sy, cy, nzc = fine.shape[1], coarse.shape[1], coarse.shape[3]
    low_half = iota(1, (Q, LANES)) < nzc
    own = levels[LEV_OWN] == 1
    for out, e, y, Y, qs, to in ((up, 1, sy - 1, cy - 1, HIGH_Y, LEV_Y_HIGH), (down, 0, 0, 0, LOW_Y, LEV_Y_LOW)):
        both = own & (levels[to] == 1)
        g_low, g_high = from_low[0:Q], from_high[0:Q]
        if e == 0:
            g_high = roll_lane(g_high, nzc)
        else:
            g_low = roll_lane(g_low, nzc)
        out[0:Q] = g_low
        out[0:Q, nzc : 2 * nzc] = coarse[0, Y]
        out[Y_SECOND : Y_SECOND + Q] = g_high
        out[Y_SECOND : Y_SECOND + Q, 0:nzc] = coarse[2, Y]
        out[Y_THIRD : Y_THIRD + 16, 0:nzc] = coarse[1, Y, 0:16]
        out[Y_THIRD : Y_THIRD + Q - 16, nzc : 2 * nzc] = coarse[1, Y, 16:Q]
        rows = fine_plane(fine, from_low, from_high, y)
        for q in range(Q):
            w_edge[q, e] = rows[q]
        for k in range(3):
            out[Y_CORNER + k : Y_CORNER + k + 1] = rows[qs[6 + k]][0:1]
            out[Y_CORNER + 3 + k : Y_CORNER + 4 + k] = rows[qs[k]][7:8]
        for k, q in enumerate(qs):
            at, n, s = fine_slot(k)
            out[at : at + n] = jnp.where(both[0:n], rows[q][s : s + n], out[at : at + n])


def forward(m0, m1, m2):
    pair = m0 + m2
    return pair + 4.0 * m1, m2 - m0, pair


ALONG_Y = [(9 * a + c, 3) for a in range(3) for c in range(3)]
ALONG_Z = [(9 * a + 3 * b, 1) for a in range(3) for b in range(3)]
ALONG_X = [(r, 9) for r in range(9)]


def collide(g, coef):
    t = [None] * Q
    for r in range(9):
        t[r], t[9 + r], t[18 + r] = forward(g[r], g[9 + r], g[18 + r])
    cols = [(t[c] + t[6 + c]) + 4.0 * t[3 + c] for c in range(3)]
    density = (cols[0] + cols[2]) + 4.0 * cols[1]
    inv = 1.0 / density
    rows = [(t[3 * b] + t[3 * b + 2]) + 4.0 * t[3 * b + 1] for b in (0, 2)]
    uy = (rows[1] - rows[0]) * inv
    uz = (cols[2] - cols[0]) * inv
    dcols = [(t[9 + c] + t[15 + c]) + 4.0 * t[12 + c] for c in range(3)]
    ux = ((dcols[0] + dcols[2]) + 4.0 * dcols[1]) * inv
    for r in range(9):
        t0, d, pair = t[r], t[9 + r], t[18 + r]
        t1 = d - ux * t0
        t[9 + r], t[18 + r] = t1, pair - ux * (d + t1)
    for u, lines in ((uy, ALONG_Y), (uz, ALONG_Z)):
        for at, by in lines:
            t0, d, pair = forward(t[at], t[at + by], t[at + 2 * by])
            t1 = d - u * t0
            t[at], t[at + by], t[at + 2 * by] = t0, t1, pair - u * (d + t1)
    for q in range(Q):
        t[q] = coef[q] * t[q]
        if q in EVEN:
            t[q] = t[q] + coef[Q + EVEN.index(q)] * density
    for u, lines in ((uz, ALONG_Z), (uy, ALONG_Y), (ux, ALONG_X)):
        for at, by in lines:
            t0, t1, t2 = t[at], t[at + by], t[at + 2 * by]
            d = t1 + u * t0
            s = t2 + u * (t1 + d)
            t[at], t[at + by], t[at + 2 * by] = s - d, 0.5 * (t0 - s), s + d
    return t


def pull(source, center, step_mask):
    out = []
    for q in range(Q):
        ex, ey, ez = STEP[q]
        v = roll_lane(roll_sub(source(q), ex), ez)
        mask = step_mask(ex, ey, ez)
        if mask is not None:
            v = jnp.where(mask, center(26 - q), v)
        out.append(v)
    return out


def bounce_mask(height, wall_of):
    lane = iota(1)
    edges = {1: lane == 0, -1: lane == height - 1}

    def mask_of(ex, ey, ez):
        m = None
        if (ex, ey, ez) == (0, 0, 0):
            return None
        wall = wall_of(ey)
        if wall is not None:
            m = roll_lane(roll_sub(wall, ex), ez) == 1
        if ez != 0:
            m = edges[ez] if m is None else m | edges[ez]
        return m

    return mask_of


def wall_plane(flags, y, first):
    def wall_of(ey):
        k = y - ey - first
        return flags[k] if k in (0, 1) else None

    return wall_of


def store_rows(rows, out, t, xs, width):
    for q0, n in OCTETS:
        tile = jnp.swapaxes(jnp.stack(rows[q0 : q0 + n]), 0, 1)
        for k, x in enumerate(xs):
            out[k, t, q0 : q0 + n] = tile[x][:, 0:width]


def coalesce(buf, t, out, at, thin):
    nzc = out.shape[3]
    for X in range(out.shape[0]):
        s = (buf[2 * X, t] + buf[2 * X + 1, t]) + (buf[2 * X, t + 1] + buf[2 * X + 1, t + 1])
        out[X, at] = dot_exact(s, thin[...])[:, 0:nzc]


def coarse_step(plane, J, wall, coef, buf, at, nzc, cx, wall_row):
    mask_of = bounce_mask(nzc, lambda ey: wall if J - ey == wall_row else None)
    new = collide(pull(lambda q: plane(q, J - STEP[q][1]), lambda q: plane(q, J), mask_of), coef)
    if J == wall_row:
        stay = wall == 1
        new = [jnp.where(stay, plane(q, J), new[q]) for q in range(Q)]
    store_rows(new, buf, at, range(1, cx + 1), nzc)


def inner_kernel(fine, coarse, from_low, from_high, levels, coef, flags, c_wall, c_wide, refine, thin,
                 out, c_out, w_in, ex_side, c_all, ghost, ex_mid, f_buf, c_buf, sems):
    sx, sy, nz = fine.shape[0], fine.shape[1], fine.shape[3]
    cx, cy, nzc = coarse.shape[0], coarse.shape[1], coarse.shape[3]
    mid = sy // 2
    own = jnp.max(levels[LEV_OWN])
    for side, msg in enumerate((from_low, from_high)):
        v = dot_exact(msg[0:Q], refine[...])
        ghost[side, 0, 0:Q] = v[:, 0:nz]
        ghost[side, cy - 1, 0:Q] = v[:, nz : 2 * nz]
        v = dot_exact(msg[X_MIDDLE : X_MIDDLE + 16], refine[...])
        ghost[side, 1, 0:16] = v[:, 0:nz]
        ghost[side, 1, 16:Q] = v[0 : Q - 16, nz : 2 * nz]

    def wide(J, I):
        if I == 0:
            return ghost[0, J - 1]
        if I == cx + 1:
            return ghost[1, J - 1]
        return c_wide[J - 1, I - 1]

    for J in range(1, cy + 1):
        for i in range(sx + 2):
            a, b = pair_of(i)
            v = blend(wide(J, a), wide(J, b))
            if J == 2:
                ex_mid[i] = v
            else:
                ex_side[J // 2, i] = v

    def exploded(J, i):
        return ex_mid.at[i] if J == 2 else ex_side.at[J // 2, i]

    copies = [pltpu.make_async_copy(f_buf.at[:, pl.ds(1, 2)], out.at[:, pl.ds(mid - 1, 2)], sems.at[0]),
              pltpu.make_async_copy(c_buf, c_out.at[:, pl.ds(cy // 2, 1)], sems.at[1]),
              pltpu.make_async_copy(f_buf, out.at[:, pl.ds(1, 4)], sems.at[0])]

    @pl.when(own == 1)
    def _():
        refined = (levels[LEV_X_LOW] == 1, levels[LEV_X_HIGH] == 1)
        for y in range(1, sy - 1):
            a, b = pair_of(y + 1)

            def mixed(side, q0, n, tile):
                i = 0 if side == 0 else sx + 1
                e = blend(exploded(a, i)[q0 : q0 + n], exploded(b, i)[q0 : q0 + n])
                return jnp.where(refined[side][0:n], tile, e)

            rows = fine_plane(fine, from_low, from_high, y, mixed)
            for q in range(Q):
                w_in[q, y - 1] = rows[q]
        for y in (mid - 1, mid):
            pulled = pull(lambda q: w_in[q, y - 1 - STEP[q][1]], lambda q: w_in[q, y - 1],
                          bounce_mask(nz, wall_plane(flags, y, mid - 1)))
            new = collide(pulled, coef)
            stay = flags[y - mid + 1] == 1
            new = [jnp.where(stay, w_in[q, y - 1], new[q]) for q in range(Q)]
            store_rows(new, f_buf, y - 1, range(1, sx + 1), nz)
        copies[0].start()
        coalesce(f_buf, 1, c_buf, 0, thin)
        copies[1].start()
        copies[0].wait()

    @pl.when(own != 1)
    def _():
        for y in range(1, sy - 1):
            a, b = pair_of(y + 1)
            for x in range(sx):
                f_buf[x, y - 1] = blend(exploded(a, x + 1)[0:Q], exploded(b, x + 1)[0:Q])
        copies[2].start()

        def tile_of(Y):
            def tile(I, q0, n):
                if 1 <= I <= cx:
                    return coarse[I - 1, Y, q0 : q0 + n]
                msg = from_low if I == 0 else from_high
                if Y != 1:
                    v = msg[q0 : q0 + n]
                    return (v if Y == 0 else roll_lane(v, nzc))[:, 0:nzc]
                if q0 < 16:
                    return msg[X_MIDDLE + q0 : X_MIDDLE + q0 + n, 0:nzc]
                return roll_lane(msg[X_MIDDLE + q0 - 16 : X_MIDDLE + q0 - 16 + n], nzc)[:, 0:nzc]

            return tile

        for Y in range(cy):
            for q, v in enumerate(coarse_plane(tile_of(Y))):
                c_all[q, Y, :, 0:nzc] = v
        coarse_step(lambda q, J: c_all[q, J - 1], 2, c_wall[...], coef, c_buf, 0, nzc, cx, 2)
        copies[1].start()
        copies[2].wait()

    copies[1].wait()


def outer_kernel(from_below, from_above, w_edge, w_in, c_all, ex_side, levels, coef, flags, c_wall, refine, thin,
                 _out_in, _c_in, out, c_out, wide, ex_g, w_g, w_e, c_g, f_buf, c_buf, sems):
    sx, sy, nz = out.shape[0], out.shape[1], out.shape[3]
    cx, cy, nzc = c_out.shape[0], c_out.shape[1], c_out.shape[3]
    own = jnp.max(levels[LEV_OWN])
    sub = iota(0)
    for e, msg in enumerate((from_below, from_above)):
        v = dot_exact(msg[0:72], refine[...])
        wide[0, 0:Q] = v[0:Q, 0:nz]
        wide[1, 0:Q] = v[0:Q, nz : 2 * nz]
        wide[3, 0:Q] = v[Y_SECOND : Y_SECOND + Q, 0:nz]
        wide[4, 0:Q] = v[Y_SECOND : Y_SECOND + Q, nz : 2 * nz]
        wide[2, 0:16] = v[Y_THIRD : Y_THIRD + 16, 0:nz]
        wide[2, 16:Q] = v[Y_THIRD : Y_THIRD + Q - 16, nz : 2 * nz]
        for i in range(sx + 2):
            a, b = pair_of(i)
            ex_g[e, i] = blend(wide[a], wide[b])

    def plane_copy(y):
        return pltpu.make_async_copy(f_buf.at[:, pl.ds(y, 1)], out.at[:, pl.ds(y, 1)], sems.at[y])

    def coarse_copy(e):
        return pltpu.make_async_copy(c_buf.at[:, pl.ds(e, 1)], c_out.at[:, pl.ds((cy - 1) * e, 1)],
                                     sems.at[sy + e])

    @pl.when(own == 1)
    def _():
        for e, msg in enumerate((from_below, from_above)):
            qs = HIGH_Y if e == 0 else LOW_Y
            ghost_j, edge_j = (0, 1) if e == 0 else (sy + 1, sy)
            far = levels[LEV_BELOW if e == 0 else LEV_ABOVE] == 1
            near = levels[LEV_Y_LOW if e == 0 else LEV_Y_HIGH] == 1
            for q0, n in OCTETS:
                tiles = [blend(ex_g[e, i, q0 : q0 + n], ex_side[e, i, q0 : q0 + n]) for i in range(sx + 2)]
                tile = jnp.swapaxes(jnp.stack(tiles), 0, 1)
                for k, q in enumerate(qs):
                    if q0 <= q < q0 + n:
                        at, _, s = fine_slot(k)
                        v = roll_sub(msg[at : at + 8], s)
                        if STEP[q][0] != 0:
                            corner = Y_CORNER + k % 3 + (0 if STEP[q][0] > 0 else 3)
                            v = jnp.where(near, v, row8(msg, corner))
                        w_g[k] = jnp.where(far, v, tile[q - q0])
            coarse_low = (levels[LEV_X_LOW] != 1) & (sub == 0)
            coarse_high = (levels[LEV_X_HIGH] != 1) & (sub == sx + 1)
            v_low = blend(ex_side[e, 0], ex_g[e, 0])
            v_high = blend(ex_side[e, sx + 1], ex_g[e, sx + 1])
            for q in range(Q):
                v = w_edge[q, e]
                if STEP[q][0] > 0:
                    v = jnp.where(coarse_low, jnp.broadcast_to(v_low[q : q + 1], (8, LANES)), v)
                if STEP[q][0] < 0:
                    v = jnp.where(coarse_high, jnp.broadcast_to(v_high[q : q + 1], (8, LANES)), v)
                w_e[q] = v

            def plane(q, j):
                if j == ghost_j:
                    return w_g[qs.index(q)]
                if j == edge_j:
                    return w_e[q]
                return w_in[q, j - 2]

            for y in ((0, 1) if e == 0 else (sy - 1, sy - 2)):
                pulled = pull(lambda q: plane(q, y + 1 - STEP[q][1]), lambda q: plane(q, y + 1),
                              bounce_mask(nz, wall_plane(flags, y, sy // 2 - 1)))
                store_rows(collide(pulled, coef), f_buf, y, range(1, sx + 1), nz)
                plane_copy(y).start()
            coalesce(f_buf, 0 if e == 0 else sy - 2, c_buf, e, thin)
            coarse_copy(e).start()
        plane_copy(1).wait()
        plane_copy(sy - 2).wait()

    @pl.when(own != 1)
    def _():
        wall = c_wall[...]

        for e, msg in enumerate((from_below, from_above)):
            y = 0 if e == 0 else sy - 1
            for x in range(sx):
                f_buf[x, y] = blend(ex_side[e, x + 1, 0:Q], ex_g[e, x + 1, 0:Q])
            plane_copy(y).start()

            def tile(I, q0, n):
                at = Y_SECOND if I >= 3 else 0
                if I == 2:
                    at = Y_THIRD - (16 if q0 >= 16 else 0)
                v = msg[at + q0 : at + q0 + n]
                if I in (1, 4) or (I == 2 and q0 >= 16):
                    v = roll_lane(v, nzc)
                return v[:, 0:nzc]

            for q, v in enumerate(coarse_plane(tile)):
                c_g[q, e, :, 0:nzc] = v

        def plane(q, J):
            if J == 0:
                return c_g[q, 0]
            if J == cy + 1:
                return c_g[q, 1]
            return c_all[q, J - 1]

        for e in range(2):
            coarse_step(plane, 1 if e == 0 else cy, wall, coef, c_buf, e, nzc, cx, 2)
            coarse_copy(e).start()

    plane_copy(0).wait()
    plane_copy(sy - 1).wait()
    for e in range(2):
        coarse_copy(e).wait()


def cost(flops, nbytes):
    return pl.CostEstimate(flops=flops, bytes_accessed=nbytes, transcendentals=0)


def in_hbm(x):
    return pltpu.with_memory_space_constraint(x, pltpu.HBM)


def local(fine_pops, coarse_pops, obstacle, block_level, relax_rates):
    fine = jnp.transpose(fine_pops, (1, 2, 0, 3))
    coarse = jnp.transpose(coarse_pops, (1, 2, 0, 3))
    sx, sy, _, nz = fine.shape
    cx, cy, _, nzc = coarse.shape

    x_message = struct((8 * ((X_FINE + 9 * sy + 7) // 8), LANES))
    up, down = pl.pallas_call(
        pack_x_kernel,
        out_shape=(x_message, x_message),
        in_specs=[ANY] * 3,
        out_specs=(VMEM, VMEM),
        scratch_shapes=[
            pltpu.VMEM((sy, Q, nz), F32),
            pltpu.VMEM((sy, Q, nz), F32),
            pltpu.VMEM((cy, Q, nzc), F32),
            pltpu.VMEM((cy, Q, nzc), F32),
            pltpu.SMEM(block_level.shape, I32),
            pltpu.SemaphoreType.DMA((5,)),
        ],
        compiler_params=params(),
        name="pack_x",
    )(in_hbm(fine), in_hbm(coarse), in_hbm(block_level))
    from_low = lax.ppermute(up, "stream", ring("stream", 1))
    from_high = lax.ppermute(down, "stream", ring("stream", -1))

    levels, coef, flags, c_wall, c_wide, refine, thin = pl.pallas_call(
        tables_kernel,
        out_shape=(
            struct((8, 8, LANES), I32),
            struct((Q + len(EVEN), 8, LANES)),
            struct((2, 8, LANES), I32),
            struct((8, LANES), I32),
            struct((cy, cx, QPAD, nz)),
            struct((2 * nzc, 2 * nz), BF16),
            struct((nz, nz), BF16),
        ),
        in_specs=[VMEM] * 2 + [SMEM] * 2,
        out_specs=(VMEM,) * 7,
        compiler_params=params(),
        cost_estimate=cost(10_000_000, 1_000_000),
        name="tables",
    )(coarse, obstacle, block_level, relax_rates)

    y_message = struct((Y_ROWS, LANES))
    up, down, w_edge = pl.pallas_call(
        pack_y_kernel,
        out_shape=(y_message, y_message, struct((Q, 2, 8, LANES))),
        in_specs=[VMEM] * 5,
        out_specs=(VMEM,) * 3,
        compiler_params=params(),
        name="pack_y",
    )(fine, coarse, from_low, from_high, levels)
    from_below = lax.ppermute(up, "span", ring("span", 1))
    from_above = lax.ppermute(down, "span", ring("span", -1))

    fine_shape, coarse_shape = struct(fine.shape), struct(coarse.shape)
    out, c_out, w_in, ex_side, c_all = pl.pallas_call(
        inner_kernel,
        out_shape=(
            fine_shape,
            coarse_shape,
            struct((Q, sy - 2, 8, LANES)),
            struct((2, sx + 2, QPAD, nz)),
            struct((Q, cy, 8, LANES)),
        ),
        in_specs=[VMEM] * 11,
        out_specs=(ANY, ANY) + (VMEM,) * 3,
        scratch_shapes=[
            pltpu.VMEM((2, cy, QPAD, nz), F32),
            pltpu.VMEM((sx + 2, QPAD, nz), F32),
            pltpu.VMEM((sx, sy - 2, Q, nz), F32),
            pltpu.VMEM((cx, 1, Q, nzc), F32),
            pltpu.SemaphoreType.DMA((2,)),
        ],
        compiler_params=params(),
        cost_estimate=cost(20_000_000, 1_000_000),
        name="inner",
    )(fine, coarse, from_low, from_high, levels, coef, flags, c_wall, c_wide, refine, thin)

    out, c_out = pl.pallas_call(
        outer_kernel,
        out_shape=(fine_shape, coarse_shape),
        in_specs=[VMEM] * 12 + [ANY, ANY],
        out_specs=(ANY, ANY),
        scratch_shapes=[
            pltpu.VMEM((5, QPAD, nz), F32),
            pltpu.VMEM((2, sx + 2, QPAD, nz), F32),
            pltpu.VMEM((9, 8, LANES), F32),
            pltpu.VMEM((Q, 8, LANES), F32),
            pltpu.VMEM((Q, 2, 8, LANES), F32),
            pltpu.VMEM((sx, sy, Q, nz), F32),
            pltpu.VMEM((cx, 2, Q, nzc), F32),
            pltpu.SemaphoreType.DMA((sy + 2,)),
        ],
        input_output_aliases={12: 0, 13: 1},
        compiler_params=params(),
        name="outer",
    )(from_below, from_above, w_edge, w_in, c_all, ex_side, levels, coef, flags, c_wall, refine, thin,
      out, c_out)
    return jnp.transpose(out, (2, 0, 1, 3)), jnp.transpose(c_out, (2, 0, 1, 3))


def solution(mesh):
    placed = (
        P(None, "stream", "span", None),
        P(None, "stream", "span", None),
        P("stream", "span", None),
        P(),
        P(),
    )
    return jax.shard_map(
        local,
        mesh=mesh,
        in_specs=placed,
        out_specs=(P(None, "stream", "span", None), P(None, "stream", "span", None)),
        check_vma=False,
    )
```

```python
import jax
import jax.numpy as jnp
from jax import lax
from jax.experimental import pallas as pl
from jax.experimental.pallas import tpu as pltpu
from jax.sharding import PartitionSpec as P

F32 = jnp.float32
I32 = jnp.int32
BF16 = jnp.bfloat16
Q = 27
QPAD = 32
LANES = 128
OCTETS = [(8 * o, min(8, Q - 8 * o)) for o in range(4)]
STEP = [(q // 9 - 1, q // 3 % 3 - 1, q % 3 - 1) for q in range(Q)]
HIGH_X = [q for q in range(Q) if STEP[q][0] == 1]
LOW_X = [q for q in range(Q) if STEP[q][0] == -1]
HIGH_Y = [q for q in range(Q) if STEP[q][1] == 1]
LOW_Y = [q for q in range(Q) if STEP[q][1] == -1]
EVEN = [9 * a + 3 * b + c for a in (0, 2) for b in (0, 2) for c in (0, 2)]

VMEM = pl.BlockSpec(memory_space=pltpu.VMEM)
SMEM = pl.BlockSpec(memory_space=pltpu.SMEM)
ANY = pl.BlockSpec(memory_space=pl.ANY)
LIMIT = 16 << 20

LEV_BELOW, LEV_ROW, LEV_ABOVE = 0, 1, 2
LEV_X_LOW, LEV_X_HIGH, LEV_OWN, LEV_Y_LOW, LEV_Y_HIGH, EVEN_SPAN = 3, 4, 5, 6, 7, 8

X_FINE, X_MIDDLE = Q, Q + 9
Y_SECOND, Y_THIRD, Y_CORNER = Q, 2 * Q, 2 * Q + 16
Y_ROWS = 80


def fine_slot(k):
    ex = k // 3 - 1
    if ex == 0:
        return 6 * (k % 3), 6, 1
    return 36 + 7 * (k % 3 if ex < 0 else 3 + k % 3), 7, (1 if ex < 0 else 0)


def params(**more):
    return pltpu.CompilerParams(vmem_limit_bytes=LIMIT, **more)


def struct(shape, dtype=F32):
    return jax.ShapeDtypeStruct(shape, dtype)


def ring(axis, by):
    peers = lax.axis_size(axis)
    return [(i, (i + by) % peers) for i in range(peers)]


def pairs(axis, odd):
    peers = lax.axis_size(axis)
    return [(i, (i + (1 if i % 2 == odd else -1)) % peers) for i in range(peers)]


def roll_lane(v, by):
    return v if by == 0 else pltpu.roll(v, by % v.shape[1], 1)


def roll_sub(v, by):
    return v if by == 0 else pltpu.roll(v, by % v.shape[0], 0)


def iota(axis, shape=(8, LANES)):
    return lax.broadcasted_iota(I32, shape, axis)


def row8(ref, at):
    return jnp.broadcast_to(ref[at : at + 1], (8, LANES))


def dot_exact(x, m):
    high = x.astype(BF16)
    rest = x - high.astype(F32)
    middle = rest.astype(BF16)
    low = (rest - middle.astype(F32)).astype(BF16)
    return sum(jnp.dot(p, m, preferred_element_type=F32) for p in (low, middle, high))


def pair_of(i):
    a = (i + 1) >> 1
    return a, a + (1 if (i + 1) & 1 else -1)


def blend(a, b):
    return 0.75 * a + 0.25 * b


def pack_x_kernel(fine, coarse, level, up, down, f_low, f_high, c_low, c_high, lev, sems):
    sx, sy, cx = fine.shape[0], fine.shape[1], coarse.shape[0]
    copies = [
        pltpu.make_async_copy(level, lev, sems.at[4]),
        pltpu.make_async_copy(fine.at[sx - 1], f_high, sems.at[0]),
        pltpu.make_async_copy(coarse.at[cx - 1], c_high, sems.at[1]),
        pltpu.make_async_copy(fine.at[0], f_low, sems.at[2]),
        pltpu.make_async_copy(coarse.at[0], c_low, sems.at[3]),
    ]
    for c in copies:
        c.start()
    for c in copies:
        c.wait()
    cy, nzc = c_low.shape[0], c_low.shape[2]
    n_row = lev.shape[0]
    row, col = lax.axis_index("stream"), lax.axis_index("span")
    own = lev[row, col]
    for out, f, c, qs, to in ((up, f_high, c_high, HIGH_X, row + 1), (down, f_low, c_low, LOW_X, row + n_row - 1)):
        out[0:Q, 0:nzc] = c[0]
        out[0:Q, nzc : 2 * nzc] = c[cy - 1]
        for y in range(sy):
            out[X_FINE + 9 * y : X_FINE + 9 * y + 9] = f[y, qs[0] : qs[0] + 9]

        @pl.when((own != 1) | (lev[lax.rem(to, n_row), col] != 1))
        def _(out=out, c=c):
            out[X_MIDDLE : X_MIDDLE + 16, 0:nzc] = c[1, 0:16]
            out[X_MIDDLE : X_MIDDLE + Q - 16, nzc : 2 * nzc] = c[1, 16:Q]


def gain_of(q):
    return (1.0 if q // 9 == 0 else 1.0 / 3.0) * (1.0 if q // 3 % 3 == 0 else 1.0 / 3.0) * (
        1.0 if q % 3 == 0 else 1.0 / 3.0)


def tables_kernel(coarse, obstacle, level, rates, levels, coef, flags, c_wall, c_wide, refine, thin):
    cx, cy, nzc = coarse.shape[0], coarse.shape[1], coarse.shape[3]
    sx, sy, nz = obstacle.shape
    row, col = lax.axis_index("stream"), lax.axis_index("span")
    n_row, n_col = level.shape
    at_row = [lax.rem(row + n_row - 1, n_row), row, lax.rem(row + 1, n_row)]
    at_col = [lax.rem(col + n_col - 1, n_col), col, lax.rem(col + 1, n_col)]
    lane, sub = iota(1), iota(0)
    for k in range(3):
        levels[k] = jnp.where(sub == 0, level[at_row[0], at_col[k]],
                              jnp.where(sub == sx + 1, level[at_row[2], at_col[k]], level[at_row[1], at_col[k]]))
    for k, (r, c) in ((LEV_X_LOW, (0, 1)), (LEV_X_HIGH, (2, 1)), (LEV_OWN, (1, 1)), (LEV_Y_LOW, (1, 0)),
                      (LEV_Y_HIGH, (1, 2))):
        levels[k] = jnp.full((8, LANES), level[at_row[r], at_col[c]], I32)
    even = lax.rem(col, 2) == 0 if n_col % 2 == 0 else True
    levels[EVEN_SPAN] = jnp.full((8, LANES), jnp.where(even, 1, 0), I32)
    refined = levels[LEV_OWN] == 1
    for q in range(Q):
        s = jnp.full((8, LANES), rates[q], F32)
        s = jnp.where(refined, s, 1.0 / (2.0 / s - 0.5))
        coef[q] = 0.125 - 0.125 * s
        if q in EVEN:
            coef[Q + EVEN.index(q)] = (0.125 * gain_of(q)) * s
    planes = []
    for k, y in enumerate((sy // 2 - 1, sy // 2)):
        v = jnp.zeros((8, LANES), I32)
        for x in (sx // 2 - 1, sx // 2):
            v = jnp.where(sub == x + 1, jnp.broadcast_to(obstacle[x, y : y + 1, :], (8, LANES)), v)
        flags[k] = v
        planes.append(v)
    both = jnp.maximum(planes[0], planes[1])
    both = jnp.maximum(both, roll_sub(both, -1))
    both = jnp.maximum(both, roll_lane(both, -1))
    both = jnp.take_along_axis(both, (2 * lane) & (LANES - 1), axis=1)
    both = jnp.broadcast_to(both[sx // 2 : sx // 2 + 1], (8, LANES))
    c_wall[...] = jnp.where((sub == 1 + cx // 2) & (lane < nzc), both, 0)
    shape = (2 * nzc, 2 * nz)
    i, l = iota(0, shape), iota(1, shape)
    half, l = l // nz, l % nz
    za = (l >> 1) + half * nzc
    zb = jnp.clip((l >> 1) + jnp.where((l & 1) == 1, 1, -1), 0, nzc - 1) + half * nzc
    refine[...] = (jnp.where(i == za, 0.75, 0.0) + jnp.where(i == zb, 0.25, 0.0)).astype(BF16)
    shape = (nz, nz)
    thin[...] = jnp.where((iota(0, shape) >> 1) == iota(1, shape), 0.125, 0.0).astype(BF16)
    for Y in range(cy):
        for X in range(cx):
            c_wide[Y, X, 0:Q] = dot_exact(coarse[X, Y], refine[0:nzc, 0:nz])


def fine_plane(fine, from_low, from_high, y, mixed=None):
    sx = fine.shape[0]
    base = X_FINE + 9 * y
    rows = [None] * Q
    for q0, n in OCTETS:
        cells = [fine[x, y, q0 : q0 + n] for x in range(sx)]
        low = high = cells[0]
        if q0 == 16:
            low = from_low[base - 2 : base + 6]
        if q0 == 24:
            low = from_low[base + 6 : base + 9]
        if q0 == 0:
            high = from_high[base : base + 8]
        if q0 == 8:
            high = row8(from_high, base + 8)
        if mixed is not None:
            if q0 >= 16:
                low = mixed(0, q0, n, low)
            else:
                high = mixed(1, q0, n, high)
        tile = jnp.swapaxes(jnp.stack([low, *cells, high]), 0, 1)
        for k in range(n):
            rows[q0 + k] = tile[k]
    return rows


def coarse_plane(tile_of):
    rows = [None] * Q
    for q0, n in OCTETS:
        tiles = [tile_of(I, q0, n) for I in range(5)]
        tile = jnp.swapaxes(jnp.stack(tiles + tiles[:3]), 0, 1)
        for k in range(n):
            rows[q0 + k] = tile[k]
    return rows


def pack_y_kernel(fine, coarse, from_low, from_high, levels, first, second, w_edge, up, down):
    sy, cy, nzc = fine.shape[1], coarse.shape[1], coarse.shape[3]
    low_half = iota(1, (Q, LANES)) < nzc
    own = levels[LEV_OWN] == 1
    for out, e, y, Y, qs, to in ((up, 1, sy - 1, cy - 1, HIGH_Y, LEV_Y_HIGH), (down, 0, 0, 0, LOW_Y, LEV_Y_LOW)):
        both = own & (levels[to] == 1)
        g_low, g_high = from_low[0:Q], from_high[0:Q]
        if e == 0:
            g_high = roll_lane(g_high, nzc)
        else:
            g_low = roll_lane(g_low, nzc)
        out[0:Q] = g_low
        out[0:Q, nzc : 2 * nzc] = coarse[0, Y]
        out[Y_SECOND : Y_SECOND + Q] = g_high
        out[Y_SECOND : Y_SECOND + Q, 0:nzc] = coarse[2, Y]
        out[Y_THIRD : Y_THIRD + 16, 0:nzc] = coarse[1, Y, 0:16]
        out[Y_THIRD : Y_THIRD + Q - 16, nzc : 2 * nzc] = coarse[1, Y, 16:Q]
        rows = fine_plane(fine, from_low, from_high, y)
        for q in range(Q):
            w_edge[q, e] = rows[q]
        for k in range(3):
            out[Y_CORNER + k : Y_CORNER + k + 1] = rows[qs[6 + k]][0:1]
            out[Y_CORNER + 3 + k : Y_CORNER + 4 + k] = rows[qs[k]][7:8]
        for k, q in enumerate(qs):
            at, n, s = fine_slot(k)
            out[at : at + n] = jnp.where(both[0:n], rows[q][s : s + n], out[at : at + n])
    even = levels[EVEN_SPAN] == 1
    for at in range(0, Y_ROWS, 8):
        a, b = up[at : at + 8], down[at : at + 8]
        first[at : at + 8] = jnp.where(even, a, b)
        second[at : at + 8] = jnp.where(even, b, a)


def forward(m0, m1, m2):
    pair = m0 + m2
    return pair + 4.0 * m1, m2 - m0, pair


ALONG_Y = [(9 * a + c, 3) for a in range(3) for c in range(3)]
ALONG_Z = [(9 * a + 3 * b, 1) for a in range(3) for b in range(3)]
ALONG_X = [(r, 9) for r in range(9)]


def collide(g, coef):
    t = [None] * Q
    for r in range(9):
        t[r], t[9 + r], t[18 + r] = forward(g[r], g[9 + r], g[18 + r])
    cols = [(t[c] + t[6 + c]) + 4.0 * t[3 + c] for c in range(3)]
    density = (cols[0] + cols[2]) + 4.0 * cols[1]
    inv = 1.0 / density
    rows = [(t[3 * b] + t[3 * b + 2]) + 4.0 * t[3 * b + 1] for b in (0, 2)]
    uy = (rows[1] - rows[0]) * inv
    uz = (cols[2] - cols[0]) * inv
    dcols = [(t[9 + c] + t[15 + c]) + 4.0 * t[12 + c] for c in range(3)]
    ux = ((dcols[0] + dcols[2]) + 4.0 * dcols[1]) * inv
    for r in range(9):
        t0, d, pair = t[r], t[9 + r], t[18 + r]
        t1 = d - ux * t0
        t[9 + r], t[18 + r] = t1, pair - ux * (d + t1)
    for u, lines in ((uy, ALONG_Y), (uz, ALONG_Z)):
        for at, by in lines:
            t0, d, pair = forward(t[at], t[at + by], t[at + 2 * by])
            t1 = d - u * t0
            t[at], t[at + by], t[at + 2 * by] = t0, t1, pair - u * (d + t1)
    for q in range(Q):
        t[q] = coef[q] * t[q]
        if q in EVEN:
            t[q] = t[q] + coef[Q + EVEN.index(q)] * density
    for u, lines in ((uz, ALONG_Z), (uy, ALONG_Y), (ux, ALONG_X)):
        for at, by in lines:
            t0, t1, t2 = t[at], t[at + by], t[at + 2 * by]
            d = t1 + u * t0
            s = t2 + u * (t1 + d)
            t[at], t[at + by], t[at + 2 * by] = s - d, 0.5 * (t0 - s), s + d
    return t


def pull(source, center, step_mask):
    out = []
    for q in range(Q):
        ex, ey, ez = STEP[q]
        v = roll_lane(roll_sub(source(q), ex), ez)
        mask = step_mask(ex, ey, ez)
        if mask is not None:
            v = jnp.where(mask, center(26 - q), v)
        out.append(v)
    return out


def bounce_mask(height, wall_of):
    lane = iota(1)
    edges = {1: lane == 0, -1: lane == height - 1}

    def mask_of(ex, ey, ez):
        m = None
        if (ex, ey, ez) == (0, 0, 0):
            return None
        wall = wall_of(ey)
        if wall is not None:
            m = roll_lane(roll_sub(wall, ex), ez) == 1
        if ez != 0:
            m = edges[ez] if m is None else m | edges[ez]
        return m

    return mask_of


def wall_plane(flags, y, first):
    def wall_of(ey):
        k = y - ey - first
        return flags[k] if k in (0, 1) else None

    return wall_of


def store_rows(rows, out, t, xs, width):
    for q0, n in OCTETS:
        tile = jnp.swapaxes(jnp.stack(rows[q0 : q0 + n]), 0, 1)
        for k, x in enumerate(xs):
            out[k, t, q0 : q0 + n] = tile[x][:, 0:width]


def coalesce(planes, out, at, thin):
    nzc = out.shape[3]
    for X in range(out.shape[0]):
        s = sum(p[2 * X] + p[2 * X + 1] for p in planes)
        out[X, at] = dot_exact(s, thin[...])[:, 0:nzc]


def coarse_step(plane, J, wall, coef, buf, at, nzc, cx, wall_row):
    mask_of = bounce_mask(nzc, lambda ey: wall if J - ey == wall_row else None)
    new = collide(pull(lambda q: plane(q, J - STEP[q][1]), lambda q: plane(q, J), mask_of), coef)
    if J == wall_row:
        stay = wall == 1
        new = [jnp.where(stay, plane(q, J), new[q]) for q in range(Q)]
    store_rows(new, buf, at, range(1, cx + 1), nzc)


def inner_kernel(fine, coarse, from_low, from_high, w_edge, levels, coef, flags, c_wall, c_wide, refine, thin,
                 out, c_out, w_in, ex_side, c_all, f_in, aux, ghost, ex_mid, c_buf, sems):
    sx, sy, nz = fine.shape[0], fine.shape[1], fine.shape[3]
    cx, cy, nzc = coarse.shape[0], coarse.shape[1], coarse.shape[3]
    mid = sy // 2
    own = jnp.max(levels[LEV_OWN])
    n = 8 * ((X_MIDDLE + 16 + 7) // 8)
    both = dot_exact(jnp.concatenate([from_low[0:n], from_high[0:n]], axis=0), refine[...])
    for side in range(2):
        v = both[side * n : side * n + n]
        ghost[side, 0, 0:Q] = v[0:Q, 0:nz]
        ghost[side, cy - 1, 0:Q] = v[0:Q, nz : 2 * nz]
        ghost[side, 1, 0:16] = v[X_MIDDLE : X_MIDDLE + 16, 0:nz]
        ghost[side, 1, 16:Q] = v[X_MIDDLE : X_MIDDLE + Q - 16, nz : 2 * nz]

    def wide(J, I):
        if I == 0:
            return ghost[0, J - 1]
        if I == cx + 1:
            return ghost[1, J - 1]
        return c_wide[J - 1, I - 1]

    for J in range(1, cy + 1):
        for i in range(sx + 2):
            a, b = pair_of(i)
            v = blend(wide(J, a), wide(J, b))
            if J == 2:
                ex_mid[i] = v
            else:
                ex_side[J // 2, i] = v

    def exploded(J, i):
        return ex_mid.at[i] if J == 2 else ex_side.at[J // 2, i]

    copies = [pltpu.make_async_copy(f_in.at[:, pl.ds(mid - 2, 2)], out.at[:, pl.ds(mid - 1, 2)], sems.at[0]),
              pltpu.make_async_copy(c_buf, c_out.at[:, pl.ds(cy // 2, 1)], sems.at[1]),
              pltpu.make_async_copy(f_in, out.at[:, pl.ds(1, sy - 2)], sems.at[0])]

    @pl.when(own == 1)
    def _():
        refined = (levels[LEV_X_LOW] == 1, levels[LEV_X_HIGH] == 1)
        sub = iota(0)
        for y in range(1, sy - 1):
            a, b = pair_of(y + 1)

            def mixed(side, q0, n, tile):
                i = 0 if side == 0 else sx + 1
                e = blend(exploded(a, i)[q0 : q0 + n], exploded(b, i)[q0 : q0 + n])
                return jnp.where(refined[side][0:n], tile, e)

            rows = fine_plane(fine, from_low, from_high, y, mixed)
            for q in range(Q):
                w_in[q, y - 1] = rows[q]

        def plane(q, y):
            if y in (0, sy - 1):
                return w_edge[q, 0 if y == 0 else 1]
            return w_in[q, y - 1]

        for y in (mid - 1, mid, 1, sy - 2):
            pulled = pull(lambda q: plane(q, y - STEP[q][1]), lambda q: plane(q, y),
                          bounce_mask(nz, wall_plane(flags, y, mid - 1)))
            if y in (1, sy - 2):
                for q in range(Q):
                    aux[q, 0 if y == 1 else 1] = jnp.where(sub == 0, roll_sub(pulled[q], -1), roll_sub(pulled[q], 1))
            new = collide(pulled, coef)
            if y in (mid - 1, mid):
                stay = flags[y - mid + 1] == 1
                new = [jnp.where(stay, w_in[q, y - 1], new[q]) for q in range(Q)]
            store_rows(new, f_in, y - 1, range(1, sx + 1), nz)
            if y == mid:
                copies[0].start()
                coalesce([f_in.at[:, mid - 2], f_in.at[:, mid - 1]], c_buf, 0, thin)
                copies[1].start()
        copies[0].wait()

    @pl.when(own != 1)
    def _():
        for y in range(1, sy - 1):
            a, b = pair_of(y + 1)
            for x in range(sx):
                f_in[x, y - 1] = blend(exploded(a, x + 1)[0:Q], exploded(b, x + 1)[0:Q])
        copies[2].start()

        def tile_of(Y):
            def tile(I, q0, n):
                if 1 <= I <= cx:
                    return coarse[I - 1, Y, q0 : q0 + n]
                msg = from_low if I == 0 else from_high
                if Y != 1:
                    v = msg[q0 : q0 + n]
                    return (v if Y == 0 else roll_lane(v, nzc))[:, 0:nzc]
                if q0 < 16:
                    return msg[X_MIDDLE + q0 : X_MIDDLE + q0 + n, 0:nzc]
                return roll_lane(msg[X_MIDDLE + q0 - 16 : X_MIDDLE + q0 - 16 + n], nzc)[:, 0:nzc]

            return tile

        for Y in range(cy):
            for q, v in enumerate(coarse_plane(tile_of(Y))):
                c_all[q, Y, :, 0:nzc] = v
        coarse_step(lambda q, J: c_all[q, J - 1], 2, c_wall[...], coef, c_buf, 0, nzc, cx, 2)
        copies[1].start()
        copies[2].wait()

    copies[1].wait()


def outer_kernel(first, second, w_edge, w_in, c_all, ex_side, f_in, aux, levels, coef, c_wall, refine, thin,
                 _out_in, _c_in, out, c_out, msgs, wide, ex_g, w_g, w_e, c_g, f_buf, f_fix, s_buf, c_buf, sems):
    sx, sy, nz = out.shape[0], out.shape[1], out.shape[3]
    cx, cy, nzc = c_out.shape[0], c_out.shape[1], c_out.shape[3]
    own = jnp.max(levels[LEV_OWN])
    sub = iota(0)
    even = levels[EVEN_SPAN] == 1
    for at in range(0, Y_ROWS, 8):
        a, b = first[at : at + 8], second[at : at + 8]
        msgs[at : at + 8] = jnp.where(even, b, a)
        msgs[Y_ROWS + at : Y_ROWS + at + 8] = jnp.where(even, a, b)
    v = dot_exact(msgs[...], refine[...])
    for e in range(2):
        at = Y_ROWS * e
        wide[0, 0:Q] = v[at : at + Q, 0:nz]
        wide[1, 0:Q] = v[at : at + Q, nz : 2 * nz]
        wide[3, 0:Q] = v[at + Y_SECOND : at + Y_SECOND + Q, 0:nz]
        wide[4, 0:Q] = v[at + Y_SECOND : at + Y_SECOND + Q, nz : 2 * nz]
        wide[2, 0:16] = v[at + Y_THIRD : at + Y_THIRD + 16, 0:nz]
        wide[2, 16:Q] = v[at + Y_THIRD : at + Y_THIRD + Q - 16, nz : 2 * nz]
        for i in range(sx + 2):
            a, b = pair_of(i)
            ex_g[e, i] = blend(wide[a], wide[b])

    def edge_copy(e):
        y = (sy - 1) * e
        return pltpu.make_async_copy(f_buf.at[:, pl.ds(e, 1)], out.at[:, pl.ds(y, 1)], sems.at[e])

    def coarse_copy(e):
        return pltpu.make_async_copy(c_buf.at[:, pl.ds(e, 1)], c_out.at[:, pl.ds((cy - 1) * e, 1)], sems.at[2 + e])

    @pl.when(own == 1)
    def _():
        ready = [pltpu.make_async_copy(f_in.at[pl.ds(1, sx - 2), pl.ds((sy - 3) * e, 1)],
                                       out.at[pl.ds(1, sx - 2), pl.ds(1 + (sy - 3) * e, 1)], sems.at[4 + e])
                 for e in range(2)]
        fixed = [[pltpu.make_async_copy(f_fix.at[pl.ds(side, 1), pl.ds(e, 1)],
                                        out.at[pl.ds((sx - 1) * side, 1), pl.ds(1 + (sy - 3) * e, 1)],
                                        sems.at[6 + 2 * e + side]) for side in range(2)] for e in range(2)]
        for c in ready:
            c.start()
        lane = iota(1)
        inside = {0: None, 1: lane != 0, -1: lane != nz - 1}
        for e in range(2):
            msg = msgs.at[pl.ds(Y_ROWS * e, Y_ROWS)]
            qs = HIGH_Y if e == 0 else LOW_Y
            far = levels[LEV_BELOW if e == 0 else LEV_ABOVE] == 1
            near = levels[LEV_Y_LOW if e == 0 else LEV_Y_HIGH] == 1
            for q0, n in OCTETS:
                tiles = [blend(ex_g[e, i, q0 : q0 + n], ex_side[e, i, q0 : q0 + n]) for i in range(sx + 2)]
                tile = jnp.swapaxes(jnp.stack(tiles), 0, 1)
                for k, q in enumerate(qs):
                    if q0 <= q < q0 + n:
                        at, _, s = fine_slot(k)
                        v = roll_sub(msg[at : at + 8], s)
                        if STEP[q][0] != 0:
                            corner = Y_CORNER + k % 3 + (0 if STEP[q][0] > 0 else 3)
                            v = jnp.where(near, v, row8(msg, corner))
                        w_g[k] = jnp.where(far, v, tile[q - q0])
            coarse_low = (levels[LEV_X_LOW] != 1) & (sub == 0)
            coarse_high = (levels[LEV_X_HIGH] != 1) & (sub == sx + 1)
            v_low = blend(ex_side[e, 0], ex_g[e, 0])
            v_high = blend(ex_side[e, sx + 1], ex_g[e, sx + 1])
            for q in range(Q):
                v = w_edge[q, e]
                if STEP[q][0] > 0:
                    v = jnp.where(coarse_low, jnp.broadcast_to(v_low[q : q + 1], (8, LANES)), v)
                if STEP[q][0] < 0:
                    v = jnp.where(coarse_high, jnp.broadcast_to(v_high[q : q + 1], (8, LANES)), v)
                w_e[q] = v

            def source(q):
                return (w_g[qs.index(q)] if q in qs else
                        w_e[q] if STEP[q][1] == 0 else w_in[q, (sy - 3) * e])

            pulled = pull(source, lambda q: w_e[q], bounce_mask(nz, lambda ey: None))
            spare = (sub == 0) | (sub == sx + 1)
            for q in range(Q):
                ex, _, ez = STEP[q]
                v = aux[q, e]
                if q in qs and ex != 0:
                    m = sub == (0 if ex > 0 else sx + 1)
                    if ez != 0:
                        m = m & inside[ez]
                    v = jnp.where(m, roll_lane(w_e[q], ez), v)
                pulled[q] = jnp.where(spare, v, pulled[q])
            new = collide(pulled, coef)
            for q0, n in OCTETS:
                tile = jnp.swapaxes(jnp.stack(new[q0 : q0 + n]), 0, 1)
                for x in range(sx):
                    f_buf[x, e, q0 : q0 + n] = tile[x + 1]
                f_fix[0, e, q0 : q0 + n] = tile[0]
                f_fix[1, e, q0 : q0 + n] = tile[sx + 1]
            edge_copy(e).start()
            for c in fixed[e]:
                c.start()

            def beside(x):
                if x in (0, sx - 1):
                    return f_fix[0 if x == 0 else 1, e]
                return f_in[x, (sy - 3) * e]

            for X in range(cx):
                s_buf[QPAD * X : QPAD * X + Q] = ((f_buf[2 * X, e] + f_buf[2 * X + 1, e])
                                                  + (beside(2 * X) + beside(2 * X + 1)))
            mean = dot_exact(s_buf[...], thin[...])
            for X in range(cx):
                c_buf[X, e] = mean[QPAD * X : QPAD * X + Q, 0:nzc]
            coarse_copy(e).start()
        for c in ready + fixed[0] + fixed[1]:
            c.wait()

    @pl.when(own != 1)
    def _():
        wall = c_wall[...]

        for e in range(2):
            msg = msgs.at[pl.ds(Y_ROWS * e, Y_ROWS)]
            for x in range(sx):
                f_buf[x, e] = blend(ex_side[e, x + 1, 0:Q], ex_g[e, x + 1, 0:Q])
            edge_copy(e).start()

            def tile(I, q0, n):
                at = Y_SECOND if I >= 3 else 0
                if I == 2:
                    at = Y_THIRD - (16 if q0 >= 16 else 0)
                v = msg[at + q0 : at + q0 + n]
                if I in (1, 4) or (I == 2 and q0 >= 16):
                    v = roll_lane(v, nzc)
                return v[:, 0:nzc]

            for q, v in enumerate(coarse_plane(tile)):
                c_g[q, e, :, 0:nzc] = v

        def plane(q, J):
            if J == 0:
                return c_g[q, 0]
            if J == cy + 1:
                return c_g[q, 1]
            return c_all[q, J - 1]

        for e in range(2):
            coarse_step(plane, 1 if e == 0 else cy, wall, coef, c_buf, e, nzc, cx, 2)
            coarse_copy(e).start()

    for e in range(2):
        edge_copy(e).wait()
        coarse_copy(e).wait()


def cost(flops, nbytes):
    return pl.CostEstimate(flops=flops, bytes_accessed=nbytes, transcendentals=0)


def in_hbm(x):
    return pltpu.with_memory_space_constraint(x, pltpu.HBM)


def local(fine_pops, coarse_pops, obstacle, block_level, relax_rates):
    fine = jnp.transpose(fine_pops, (1, 2, 0, 3))
    coarse = jnp.transpose(coarse_pops, (1, 2, 0, 3))
    sx, sy, _, nz = fine.shape
    cx, cy, _, nzc = coarse.shape

    x_message = struct((8 * ((X_FINE + 9 * sy + 7) // 8), LANES))
    up, down = pl.pallas_call(
        pack_x_kernel,
        out_shape=(x_message, x_message),
        in_specs=[ANY] * 3,
        out_specs=(VMEM, VMEM),
        scratch_shapes=[
            pltpu.VMEM((sy, Q, nz), F32),
            pltpu.VMEM((sy, Q, nz), F32),
            pltpu.VMEM((cy, Q, nzc), F32),
            pltpu.VMEM((cy, Q, nzc), F32),
            pltpu.SMEM(block_level.shape, I32),
            pltpu.SemaphoreType.DMA((5,)),
        ],
        compiler_params=params(),
        name="pack_x",
    )(in_hbm(fine), in_hbm(coarse), in_hbm(block_level))
    from_low = lax.ppermute(up, "stream", ring("stream", 1))
    from_high = lax.ppermute(down, "stream", ring("stream", -1))

    levels, coef, flags, c_wall, c_wide, refine, thin = pl.pallas_call(
        tables_kernel,
        out_shape=(
            struct((9, 8, LANES), I32),
            struct((Q + len(EVEN), 8, LANES)),
            struct((2, 8, LANES), I32),
            struct((8, LANES), I32),
            struct((cy, cx, QPAD, nz)),
            struct((2 * nzc, 2 * nz), BF16),
            struct((nz, nz), BF16),
        ),
        in_specs=[VMEM] * 2 + [SMEM] * 2,
        out_specs=(VMEM,) * 7,
        compiler_params=params(),
        cost_estimate=cost(10_000_000, 1_000_000),
        name="tables",
    )(coarse, obstacle, block_level, relax_rates)

    y_message = struct((Y_ROWS, LANES))
    first, second, w_edge = pl.pallas_call(
        pack_y_kernel,
        out_shape=(y_message, y_message, struct((Q, 2, 8, LANES))),
        in_specs=[VMEM] * 5,
        out_specs=(VMEM,) * 3,
        scratch_shapes=[pltpu.VMEM(y_message.shape, F32)] * 2,
        compiler_params=params(),
        name="pack_y",
    )(fine, coarse, from_low, from_high, levels)
    if lax.axis_size("span") % 2 == 0:
        second = lax.ppermute(second, "span", pairs("span", 1))
        first = lax.ppermute(first, "span", pairs("span", 0))
    else:
        second, first = (lax.ppermute(first, "span", ring("span", 1)),
                         lax.ppermute(second, "span", ring("span", -1)))

    fine_shape, coarse_shape = struct(fine.shape), struct(coarse.shape)
    out, c_out, w_in, ex_side, c_all, f_in, aux = pl.pallas_call(
        inner_kernel,
        out_shape=(
            fine_shape,
            coarse_shape,
            struct((Q, sy - 2, 8, LANES)),
            struct((2, sx + 2, QPAD, nz)),
            struct((Q, cy, 8, LANES)),
            struct((sx, sy - 2, Q, nz)),
            struct((Q, 2, 8, LANES)),
        ),
        in_specs=[VMEM] * 12,
        out_specs=(ANY, ANY) + (VMEM,) * 5,
        scratch_shapes=[
            pltpu.VMEM((2, cy, QPAD, nz), F32),
            pltpu.VMEM((sx + 2, QPAD, nz), F32),
            pltpu.VMEM((cx, 1, Q, nzc), F32),
            pltpu.SemaphoreType.DMA((2,)),
        ],
        compiler_params=params(),
        cost_estimate=cost(20_000_000, 1_000_000),
        name="inner",
    )(fine, coarse, from_low, from_high, w_edge, levels, coef, flags, c_wall, c_wide, refine, thin)

    out, c_out = pl.pallas_call(
        outer_kernel,
        out_shape=(fine_shape, coarse_shape),
        in_specs=[VMEM] * 13 + [ANY, ANY],
        out_specs=(ANY, ANY),
        scratch_shapes=[
            pltpu.VMEM((2 * Y_ROWS, LANES), F32),
            pltpu.VMEM((5, QPAD, nz), F32),
            pltpu.VMEM((2, sx + 2, QPAD, nz), F32),
            pltpu.VMEM((9, 8, LANES), F32),
            pltpu.VMEM((Q, 8, LANES), F32),
            pltpu.VMEM((Q, 2, 8, LANES), F32),
            pltpu.VMEM((sx, 2, Q, nz), F32),
            pltpu.VMEM((2, 2, Q, nz), F32),
            pltpu.VMEM((QPAD * cx, nz), F32),
            pltpu.VMEM((cx, 2, Q, nzc), F32),
            pltpu.SemaphoreType.DMA((10,)),
        ],
        input_output_aliases={13: 0, 14: 1},
        compiler_params=params(),
        name="outer",
    )(first, second, w_edge, w_in, c_all, ex_side, f_in, aux, levels, coef, c_wall, refine, thin,
      out, c_out)
    return jnp.transpose(out, (2, 0, 1, 3)), jnp.transpose(c_out, (2, 0, 1, 3))


def solution(mesh):
    placed = (
        P(None, "stream", "span", None),
        P(None, "stream", "span", None),
        P("stream", "span", None),
        P(),
        P(),
    )
    return jax.shard_map(
        local,
        mesh=mesh,
        in_specs=placed,
        out_specs=(P(None, "stream", "span", None), P(None, "stream", "span", None)),
        check_vma=False,
    )
```

```python
import jax
import jax.numpy as jnp
from jax import lax
from jax.experimental import pallas as pl
from jax.experimental.pallas import tpu as pltpu
from jax.sharding import PartitionSpec as P

F32 = jnp.float32
I32 = jnp.int32
BF16 = jnp.bfloat16
Q = 27
QPAD = 32
LANES = 128
OCTETS = [(8 * o, min(8, Q - 8 * o)) for o in range(4)]
STEP = [(q // 9 - 1, q // 3 % 3 - 1, q % 3 - 1) for q in range(Q)]
HIGH_X = [q for q in range(Q) if STEP[q][0] == 1]
LOW_X = [q for q in range(Q) if STEP[q][0] == -1]
HIGH_Y = [q for q in range(Q) if STEP[q][1] == 1]
LOW_Y = [q for q in range(Q) if STEP[q][1] == -1]
EVEN = [9 * a + 3 * b + c for a in (0, 2) for b in (0, 2) for c in (0, 2)]

VMEM = pl.BlockSpec(memory_space=pltpu.VMEM)
SMEM = pl.BlockSpec(memory_space=pltpu.SMEM)
ANY = pl.BlockSpec(memory_space=pl.ANY)
LIMIT = 16 << 20

LEV_BELOW, LEV_ROW, LEV_ABOVE = 0, 1, 2
LEV_X_LOW, LEV_X_HIGH, LEV_OWN, LEV_Y_LOW, LEV_Y_HIGH, EVEN_SPAN = 3, 4, 5, 6, 7, 8

X_FINE, X_MIDDLE = Q, Q + 9
Y_SECOND, Y_THIRD, Y_CORNER = Q, 2 * Q, 2 * Q + 16
Y_ROWS = 80


def fine_slot(k):
    ex = k // 3 - 1
    if ex == 0:
        return 6 * (k % 3), 6, 1
    return 36 + 7 * (k % 3 if ex < 0 else 3 + k % 3), 7, (1 if ex < 0 else 0)


def params(**more):
    return pltpu.CompilerParams(vmem_limit_bytes=LIMIT, **more)


def struct(shape, dtype=F32):
    return jax.ShapeDtypeStruct(shape, dtype)


def ring(axis, by):
    peers = lax.axis_size(axis)
    return [(i, (i + by) % peers) for i in range(peers)]


def pairs(axis, odd):
    peers = lax.axis_size(axis)
    return [(i, (i + (1 if i % 2 == odd else -1)) % peers) for i in range(peers)]


def roll_lane(v, by):
    return v if by == 0 else pltpu.roll(v, by % v.shape[1], 1)


def roll_sub(v, by):
    return v if by == 0 else pltpu.roll(v, by % v.shape[0], 0)


def iota(axis, shape=(8, LANES)):
    return lax.broadcasted_iota(I32, shape, axis)


def row8(ref, at):
    return jnp.broadcast_to(ref[at : at + 1], (8, LANES))


def dot_exact(x, m):
    high = x.astype(BF16)
    rest = x - high.astype(F32)
    middle = rest.astype(BF16)
    low = (rest - middle.astype(F32)).astype(BF16)
    return sum(jnp.dot(p, m, preferred_element_type=F32) for p in (low, middle, high))


def pair_of(i):
    a = (i + 1) >> 1
    return a, a + (1 if (i + 1) & 1 else -1)


def blend(a, b):
    return 0.75 * a + 0.25 * b


def pack_x_kernel(fine, coarse, level, up, down, f_low, f_high, c_low, c_high, lev, sems):
    sx, sy, cx = fine.shape[0], fine.shape[1], coarse.shape[0]
    copies = [
        pltpu.make_async_copy(level, lev, sems.at[4]),
        pltpu.make_async_copy(fine.at[sx - 1], f_high, sems.at[0]),
        pltpu.make_async_copy(coarse.at[cx - 1], c_high, sems.at[1]),
        pltpu.make_async_copy(fine.at[0], f_low, sems.at[2]),
        pltpu.make_async_copy(coarse.at[0], c_low, sems.at[3]),
    ]
    for c in copies:
        c.start()
    for c in copies:
        c.wait()
    cy, nzc = c_low.shape[0], c_low.shape[2]
    n_row = lev.shape[0]
    row, col = lax.axis_index("stream"), lax.axis_index("span")
    own = lev[row, col]
    for out, f, c, qs, to in ((up, f_high, c_high, HIGH_X, row + 1), (down, f_low, c_low, LOW_X, row + n_row - 1)):
        out[0:Q, 0:nzc] = c[0]
        out[0:Q, nzc : 2 * nzc] = c[cy - 1]
        for y in range(sy):
            out[X_FINE + 9 * y : X_FINE + 9 * y + 9] = f[y, qs[0] : qs[0] + 9]

        @pl.when((own != 1) | (lev[lax.rem(to, n_row), col] != 1))
        def _(out=out, c=c):
            out[X_MIDDLE : X_MIDDLE + 16, 0:nzc] = c[1, 0:16]
            out[X_MIDDLE : X_MIDDLE + Q - 16, nzc : 2 * nzc] = c[1, 16:Q]


def gain_of(q):
    return (1.0 if q // 9 == 0 else 1.0 / 3.0) * (1.0 if q // 3 % 3 == 0 else 1.0 / 3.0) * (
        1.0 if q % 3 == 0 else 1.0 / 3.0)


def tables_kernel(coarse, obstacle, level, rates, levels, coef, flags, c_wall, c_wide, refine, thin):
    cx, cy, nzc = coarse.shape[0], coarse.shape[1], coarse.shape[3]
    sx, sy, nz = obstacle.shape
    row, col = lax.axis_index("stream"), lax.axis_index("span")
    n_row, n_col = level.shape
    at_row = [lax.rem(row + n_row - 1, n_row), row, lax.rem(row + 1, n_row)]
    at_col = [lax.rem(col + n_col - 1, n_col), col, lax.rem(col + 1, n_col)]
    lane, sub = iota(1), iota(0)
    for k in range(3):
        levels[k] = jnp.where(sub == 0, level[at_row[0], at_col[k]],
                              jnp.where(sub == sx + 1, level[at_row[2], at_col[k]], level[at_row[1], at_col[k]]))
    for k, (r, c) in ((LEV_X_LOW, (0, 1)), (LEV_X_HIGH, (2, 1)), (LEV_OWN, (1, 1)), (LEV_Y_LOW, (1, 0)),
                      (LEV_Y_HIGH, (1, 2))):
        levels[k] = jnp.full((8, LANES), level[at_row[r], at_col[c]], I32)
    even = lax.rem(col, 2) == 0 if n_col % 2 == 0 else True
    levels[EVEN_SPAN] = jnp.full((8, LANES), jnp.where(even, 1, 0), I32)
    refined = levels[LEV_OWN] == 1
    for q in range(Q):
        s = jnp.full((8, LANES), rates[q], F32)
        s = jnp.where(refined, s, 1.0 / (2.0 / s - 0.5))
        coef[q] = 0.125 - 0.125 * s
        if q in EVEN:
            coef[Q + EVEN.index(q)] = (0.125 * gain_of(q)) * s
    planes = []
    for k, y in enumerate((sy // 2 - 1, sy // 2)):
        v = jnp.zeros((8, LANES), I32)
        for x in (sx // 2 - 1, sx // 2):
            v = jnp.where(sub == x + 1, jnp.broadcast_to(obstacle[x, y : y + 1, :], (8, LANES)), v)
        flags[k] = v
        planes.append(v)
    both = jnp.maximum(planes[0], planes[1])
    both = jnp.maximum(both, roll_sub(both, -1))
    both = jnp.maximum(both, roll_lane(both, -1))
    both = jnp.take_along_axis(both, (2 * lane) & (LANES - 1), axis=1)
    both = jnp.broadcast_to(both[sx // 2 : sx // 2 + 1], (8, LANES))
    c_wall[...] = jnp.where((sub == 1 + cx // 2) & (lane < nzc), both, 0)
    shape = (2 * nzc, 2 * nz)
    i, l = iota(0, shape), iota(1, shape)
    half, l = l // nz, l % nz
    za = (l >> 1) + half * nzc
    zb = jnp.clip((l >> 1) + jnp.where((l & 1) == 1, 1, -1), 0, nzc - 1) + half * nzc
    refine[...] = (jnp.where(i == za, 0.75, 0.0) + jnp.where(i == zb, 0.25, 0.0)).astype(BF16)
    shape = (nz, nz)
    thin[...] = jnp.where((iota(0, shape) >> 1) == iota(1, shape), 0.125, 0.0).astype(BF16)
    for Y in range(cy):
        for X in range(cx):
            c_wide[Y, X, 0:Q] = dot_exact(coarse[X, Y], refine[0:nzc, 0:nz])


def fine_plane(fine, from_low, from_high, y, mixed=None):
    sx = fine.shape[0]
    base = X_FINE + 9 * y
    rows = [None] * Q
    for q0, n in OCTETS:
        cells = [fine[x, y, q0 : q0 + n] for x in range(sx)]
        low = high = cells[0]
        if q0 == 16:
            low = from_low[base - 2 : base + 6]
        if q0 == 24:
            low = from_low[base + 6 : base + 9]
        if q0 == 0:
            high = from_high[base : base + 8]
        if q0 == 8:
            high = row8(from_high, base + 8)
        if mixed is not None:
            if q0 >= 16:
                low = mixed(0, q0, n, low)
            else:
                high = mixed(1, q0, n, high)
        tile = jnp.swapaxes(jnp.stack([low, *cells, high]), 0, 1)
        for k in range(n):
            rows[q0 + k] = tile[k]
    return rows


def coarse_plane(tile_of):
    rows = [None] * Q
    for q0, n in OCTETS:
        tiles = [tile_of(I, q0, n) for I in range(5)]
        tile = jnp.swapaxes(jnp.stack(tiles + tiles[:3]), 0, 1)
        for k in range(n):
            rows[q0 + k] = tile[k]
    return rows


def pack_y_kernel(fine, coarse, from_low, from_high, levels, second, first, w_edge, up, down):
    sy, cy, nzc = fine.shape[1], coarse.shape[1], coarse.shape[3]
    low_half = iota(1, (Q, LANES)) < nzc
    own = levels[LEV_OWN] == 1
    for out, e, y, Y, qs, to in ((up, 1, sy - 1, cy - 1, HIGH_Y, LEV_Y_HIGH), (down, 0, 0, 0, LOW_Y, LEV_Y_LOW)):
        both = own & (levels[to] == 1)
        g_low, g_high = from_low[0:Q], from_high[0:Q]
        if e == 0:
            g_high = roll_lane(g_high, nzc)
        else:
            g_low = roll_lane(g_low, nzc)
        out[0:Q] = g_low
        out[0:Q, nzc : 2 * nzc] = coarse[0, Y]
        out[Y_SECOND : Y_SECOND + Q] = g_high
        out[Y_SECOND : Y_SECOND + Q, 0:nzc] = coarse[2, Y]
        out[Y_THIRD : Y_THIRD + 16, 0:nzc] = coarse[1, Y, 0:16]
        out[Y_THIRD : Y_THIRD + Q - 16, nzc : 2 * nzc] = coarse[1, Y, 16:Q]
        rows = fine_plane(fine, from_low, from_high, y)
        for q in range(Q):
            w_edge[q, e] = rows[q]
        for k in range(3):
            out[Y_CORNER + k : Y_CORNER + k + 1] = rows[qs[6 + k]][0:1]
            out[Y_CORNER + 3 + k : Y_CORNER + 4 + k] = rows[qs[k]][7:8]
        for k, q in enumerate(qs):
            at, n, s = fine_slot(k)
            out[at : at + n] = jnp.where(both[0:n], rows[q][s : s + n], out[at : at + n])
    even = levels[EVEN_SPAN] == 1
    for at in range(0, Y_ROWS, 8):
        a, b = up[at : at + 8], down[at : at + 8]
        first[at : at + 8] = jnp.where(even, a, b)
        second[at : at + 8] = jnp.where(even, b, a)


def forward(m0, m1, m2):
    pair = m0 + m2
    return pair + 4.0 * m1, m2 - m0, pair


ALONG_Y = [(9 * a + c, 3) for a in range(3) for c in range(3)]
ALONG_Z = [(9 * a + 3 * b, 1) for a in range(3) for b in range(3)]
ALONG_X = [(r, 9) for r in range(9)]


def collide(g, coef):
    t = [None] * Q
    for r in range(9):
        t[r], t[9 + r], t[18 + r] = forward(g[r], g[9 + r], g[18 + r])
    cols = [(t[c] + t[6 + c]) + 4.0 * t[3 + c] for c in range(3)]
    density = (cols[0] + cols[2]) + 4.0 * cols[1]
    inv = 1.0 / density
    rows = [(t[3 * b] + t[3 * b + 2]) + 4.0 * t[3 * b + 1] for b in (0, 2)]
    uy = (rows[1] - rows[0]) * inv
    uz = (cols[2] - cols[0]) * inv
    dcols = [(t[9 + c] + t[15 + c]) + 4.0 * t[12 + c] for c in range(3)]
    ux = ((dcols[0] + dcols[2]) + 4.0 * dcols[1]) * inv
    for r in range(9):
        t0, d, pair = t[r], t[9 + r], t[18 + r]
        t1 = d - ux * t0
        t[9 + r], t[18 + r] = t1, pair - ux * (d + t1)
    for u, lines in ((uy, ALONG_Y), (uz, ALONG_Z)):
        for at, by in lines:
            t0, d, pair = forward(t[at], t[at + by], t[at + 2 * by])
            t1 = d - u * t0
            t[at], t[at + by], t[at + 2 * by] = t0, t1, pair - u * (d + t1)
    for q in range(Q):
        t[q] = coef[q] * t[q]
        if q in EVEN:
            t[q] = t[q] + coef[Q + EVEN.index(q)] * density
    for u, lines in ((uz, ALONG_Z), (uy, ALONG_Y), (ux, ALONG_X)):
        for at, by in lines:
            t0, t1, t2 = t[at], t[at + by], t[at + 2 * by]
            d = t1 + u * t0
            s = t2 + u * (t1 + d)
            t[at], t[at + by], t[at + 2 * by] = s - d, 0.5 * (t0 - s), s + d
    return t


def pull(source, center, step_mask):
    out = []
    for q in range(Q):
        ex, ey, ez = STEP[q]
        v = roll_lane(roll_sub(source(q), ex), ez)
        mask = step_mask(ex, ey, ez)
        if mask is not None:
            v = jnp.where(mask, center(26 - q), v)
        out.append(v)
    return out


def bounce_mask(height, wall_of):
    lane = iota(1)
    edges = {1: lane == 0, -1: lane == height - 1}

    def mask_of(ex, ey, ez):
        m = None
        if (ex, ey, ez) == (0, 0, 0):
            return None
        wall = wall_of(ey)
        if wall is not None:
            m = roll_lane(roll_sub(wall, ex), ez) == 1
        if ez != 0:
            m = edges[ez] if m is None else m | edges[ez]
        return m

    return mask_of


def wall_plane(flags, y, first):
    def wall_of(ey):
        k = y - ey - first
        return flags[k] if k in (0, 1) else None

    return wall_of


def store_rows(rows, out, t, xs, width):
    for q0, n in OCTETS:
        tile = jnp.swapaxes(jnp.stack(rows[q0 : q0 + n]), 0, 1)
        for k, x in enumerate(xs):
            out[k, t, q0 : q0 + n] = tile[x][:, 0:width]


def coalesce(planes, out, at, thin):
    nzc = out.shape[3]
    for X in range(out.shape[0]):
        s = sum(p[2 * X] + p[2 * X + 1] for p in planes)
        out[X, at] = dot_exact(s, thin[...])[:, 0:nzc]


def coarse_step(plane, J, wall, coef, buf, at, nzc, cx, wall_row):
    mask_of = bounce_mask(nzc, lambda ey: wall if J - ey == wall_row else None)
    new = collide(pull(lambda q: plane(q, J - STEP[q][1]), lambda q: plane(q, J), mask_of), coef)
    if J == wall_row:
        stay = wall == 1
        new = [jnp.where(stay, plane(q, J), new[q]) for q in range(Q)]
    store_rows(new, buf, at, range(1, cx + 1), nzc)


def inner_kernel(fine, coarse, from_low, from_high, w_edge, levels, coef, flags, c_wall, c_wide, refine, thin,
                 out, c_out, w_in, ex_side, c_all, f_in, aux, ghost, ex_mid, c_buf, sems):
    sx, sy, nz = fine.shape[0], fine.shape[1], fine.shape[3]
    cx, cy, nzc = coarse.shape[0], coarse.shape[1], coarse.shape[3]
    mid = sy // 2
    own = jnp.max(levels[LEV_OWN])
    n = 8 * ((X_MIDDLE + 16 + 7) // 8)
    both = dot_exact(jnp.concatenate([from_low[0:n], from_high[0:n]], axis=0), refine[...])
    for side in range(2):
        v = both[side * n : side * n + n]
        ghost[side, 0, 0:Q] = v[0:Q, 0:nz]
        ghost[side, cy - 1, 0:Q] = v[0:Q, nz : 2 * nz]
        ghost[side, 1, 0:16] = v[X_MIDDLE : X_MIDDLE + 16, 0:nz]
        ghost[side, 1, 16:Q] = v[X_MIDDLE : X_MIDDLE + Q - 16, nz : 2 * nz]

    def wide(J, I):
        if I == 0:
            return ghost[0, J - 1]
        if I == cx + 1:
            return ghost[1, J - 1]
        return c_wide[J - 1, I - 1]

    for J in range(1, cy + 1):
        for i in range(sx + 2):
            a, b = pair_of(i)
            v = blend(wide(J, a), wide(J, b))
            if J == 2:
                ex_mid[i] = v
            else:
                ex_side[J // 2, i] = v

    def exploded(J, i):
        return ex_mid.at[i] if J == 2 else ex_side.at[J // 2, i]

    copies = [pltpu.make_async_copy(f_in.at[:, pl.ds(mid - 2, 2)], out.at[:, pl.ds(mid - 1, 2)], sems.at[0]),
              pltpu.make_async_copy(c_buf, c_out.at[:, pl.ds(cy // 2, 1)], sems.at[1]),
              pltpu.make_async_copy(f_in, out.at[:, pl.ds(1, sy - 2)], sems.at[0])]

    @pl.when(own == 1)
    def _():
        refined = (levels[LEV_X_LOW] == 1, levels[LEV_X_HIGH] == 1)
        sub = iota(0)
        for y in range(1, sy - 1):
            a, b = pair_of(y + 1)

            def mixed(side, q0, n, tile):
                i = 0 if side == 0 else sx + 1
                e = blend(exploded(a, i)[q0 : q0 + n], exploded(b, i)[q0 : q0 + n])
                return jnp.where(refined[side][0:n], tile, e)

            rows = fine_plane(fine, from_low, from_high, y, mixed)
            for q in range(Q):
                w_in[q, y - 1] = rows[q]

        def plane(q, y):
            if y in (0, sy - 1):
                return w_edge[q, 0 if y == 0 else 1]
            return w_in[q, y - 1]

        for y in (mid - 1, mid, 1, sy - 2):
            pulled = pull(lambda q: plane(q, y - STEP[q][1]), lambda q: plane(q, y),
                          bounce_mask(nz, wall_plane(flags, y, mid - 1)))
            if y in (1, sy - 2):
                for q in range(Q):
                    aux[q, 0 if y == 1 else 1] = jnp.where(sub == 0, roll_sub(pulled[q], -1), roll_sub(pulled[q], 1))
            new = collide(pulled, coef)
            if y in (mid - 1, mid):
                stay = flags[y - mid + 1] == 1
                new = [jnp.where(stay, w_in[q, y - 1], new[q]) for q in range(Q)]
            store_rows(new, f_in, y - 1, range(1, sx + 1), nz)
            if y == mid:
                copies[0].start()
                coalesce([f_in.at[:, mid - 2], f_in.at[:, mid - 1]], c_buf, 0, thin)
                copies[1].start()
        copies[0].wait()

    @pl.when(own != 1)
    def _():
        for y in range(1, sy - 1):
            a, b = pair_of(y + 1)
            for x in range(sx):
                f_in[x, y - 1] = blend(exploded(a, x + 1)[0:Q], exploded(b, x + 1)[0:Q])
        copies[2].start()

        def tile_of(Y):
            def tile(I, q0, n):
                if 1 <= I <= cx:
                    return coarse[I - 1, Y, q0 : q0 + n]
                msg = from_low if I == 0 else from_high
                if Y != 1:
                    v = msg[q0 : q0 + n]
                    return (v if Y == 0 else roll_lane(v, nzc))[:, 0:nzc]
                if q0 < 16:
                    return msg[X_MIDDLE + q0 : X_MIDDLE + q0 + n, 0:nzc]
                return roll_lane(msg[X_MIDDLE + q0 - 16 : X_MIDDLE + q0 - 16 + n], nzc)[:, 0:nzc]

            return tile

        for Y in range(cy):
            for q, v in enumerate(coarse_plane(tile_of(Y))):
                c_all[q, Y, :, 0:nzc] = v
        coarse_step(lambda q, J: c_all[q, J - 1], 2, c_wall[...], coef, c_buf, 0, nzc, cx, 2)
        copies[1].start()
        copies[2].wait()

    copies[1].wait()


def outer_kernel(second, first, w_edge, w_in, c_all, ex_side, f_in, aux, levels, coef, c_wall, refine, thin,
                 _out_in, _c_in, out, c_out, msgs, wide, ex_g, w_g, w_e, c_g, f_buf, f_fix, s_buf, c_buf, sems):
    sx, sy, nz = out.shape[0], out.shape[1], out.shape[3]
    cx, cy, nzc = c_out.shape[0], c_out.shape[1], c_out.shape[3]
    own = jnp.max(levels[LEV_OWN])
    sub = iota(0)
    even = levels[EVEN_SPAN] == 1
    for at in range(0, Y_ROWS, 8):
        a, b = first[at : at + 8], second[at : at + 8]
        msgs[at : at + 8] = jnp.where(even, b, a)
        msgs[Y_ROWS + at : Y_ROWS + at + 8] = jnp.where(even, a, b)
    v = dot_exact(msgs[...], refine[...])
    for e in range(2):
        at = Y_ROWS * e
        wide[0, 0:Q] = v[at : at + Q, 0:nz]
        wide[1, 0:Q] = v[at : at + Q, nz : 2 * nz]
        wide[3, 0:Q] = v[at + Y_SECOND : at + Y_SECOND + Q, 0:nz]
        wide[4, 0:Q] = v[at + Y_SECOND : at + Y_SECOND + Q, nz : 2 * nz]
        wide[2, 0:16] = v[at + Y_THIRD : at + Y_THIRD + 16, 0:nz]
        wide[2, 16:Q] = v[at + Y_THIRD : at + Y_THIRD + Q - 16, nz : 2 * nz]
        for i in range(sx + 2):
            a, b = pair_of(i)
            ex_g[e, i] = blend(wide[a], wide[b])

    def edge_copy(e):
        y = (sy - 1) * e
        return pltpu.make_async_copy(f_buf.at[:, pl.ds(e, 1)], out.at[:, pl.ds(y, 1)], sems.at[e])

    def coarse_copy(e):
        return pltpu.make_async_copy(c_buf.at[:, pl.ds(e, 1)], c_out.at[:, pl.ds((cy - 1) * e, 1)], sems.at[2 + e])

    @pl.when(own == 1)
    def _():
        ready = [pltpu.make_async_copy(f_in.at[pl.ds(1, sx - 2), pl.ds((sy - 3) * e, 1)],
                                       out.at[pl.ds(1, sx - 2), pl.ds(1 + (sy - 3) * e, 1)], sems.at[4 + e])
                 for e in range(2)]
        fixed = [[pltpu.make_async_copy(f_fix.at[pl.ds(side, 1), pl.ds(e, 1)],
                                        out.at[pl.ds((sx - 1) * side, 1), pl.ds(1 + (sy - 3) * e, 1)],
                                        sems.at[6 + 2 * e + side]) for side in range(2)] for e in range(2)]
        for c in ready:
            c.start()
        lane = iota(1)
        inside = {0: None, 1: lane != 0, -1: lane != nz - 1}
        for e in range(2):
            msg = msgs.at[pl.ds(Y_ROWS * e, Y_ROWS)]
            qs = HIGH_Y if e == 0 else LOW_Y
            far = levels[LEV_BELOW if e == 0 else LEV_ABOVE] == 1
            near = levels[LEV_Y_LOW if e == 0 else LEV_Y_HIGH] == 1
            for q0, n in OCTETS:
                tiles = [blend(ex_g[e, i, q0 : q0 + n], ex_side[e, i, q0 : q0 + n]) for i in range(sx + 2)]
                tile = jnp.swapaxes(jnp.stack(tiles), 0, 1)
                for k, q in enumerate(qs):
                    if q0 <= q < q0 + n:
                        at, _, s = fine_slot(k)
                        v = roll_sub(msg[at : at + 8], s)
                        if STEP[q][0] != 0:
                            corner = Y_CORNER + k % 3 + (0 if STEP[q][0] > 0 else 3)
                            v = jnp.where(near, v, row8(msg, corner))
                        w_g[k] = jnp.where(far, v, tile[q - q0])
            coarse_low = (levels[LEV_X_LOW] != 1) & (sub == 0)
            coarse_high = (levels[LEV_X_HIGH] != 1) & (sub == sx + 1)
            v_low = blend(ex_side[e, 0], ex_g[e, 0])
            v_high = blend(ex_side[e, sx + 1], ex_g[e, sx + 1])
            for q in range(Q):
                v = w_edge[q, e]
                if STEP[q][0] > 0:
                    v = jnp.where(coarse_low, jnp.broadcast_to(v_low[q : q + 1], (8, LANES)), v)
                if STEP[q][0] < 0:
                    v = jnp.where(coarse_high, jnp.broadcast_to(v_high[q : q + 1], (8, LANES)), v)
                w_e[q] = v

            def source(q):
                return (w_g[qs.index(q)] if q in qs else
                        w_e[q] if STEP[q][1] == 0 else w_in[q, (sy - 3) * e])

            pulled = pull(source, lambda q: w_e[q], bounce_mask(nz, lambda ey: None))
            spare = (sub == 0) | (sub == sx + 1)
            for q in range(Q):
                ex, _, ez = STEP[q]
                v = aux[q, e]
                if q in qs and ex != 0:
                    m = sub == (0 if ex > 0 else sx + 1)
                    if ez != 0:
                        m = m & inside[ez]
                    v = jnp.where(m, roll_lane(w_e[q], ez), v)
                pulled[q] = jnp.where(spare, v, pulled[q])
            new = collide(pulled, coef)
            for q0, n in OCTETS:
                tile = jnp.swapaxes(jnp.stack(new[q0 : q0 + n]), 0, 1)
                for x in range(sx):
                    f_buf[x, e, q0 : q0 + n] = tile[x + 1]
                f_fix[0, e, q0 : q0 + n] = tile[0]
                f_fix[1, e, q0 : q0 + n] = tile[sx + 1]
            edge_copy(e).start()
            for c in fixed[e]:
                c.start()

            def beside(x):
                if x in (0, sx - 1):
                    return f_fix[0 if x == 0 else 1, e]
                return f_in[x, (sy - 3) * e]

            for X in range(cx):
                s_buf[QPAD * X : QPAD * X + Q] = ((f_buf[2 * X, e] + f_buf[2 * X + 1, e])
                                                  + (beside(2 * X) + beside(2 * X + 1)))
            mean = dot_exact(s_buf[...], thin[...])
            for X in range(cx):
                c_buf[X, e] = mean[QPAD * X : QPAD * X + Q, 0:nzc]
            coarse_copy(e).start()
        for c in ready + fixed[0] + fixed[1]:
            c.wait()

    @pl.when(own != 1)
    def _():
        wall = c_wall[...]

        for e in range(2):
            msg = msgs.at[pl.ds(Y_ROWS * e, Y_ROWS)]
            for x in range(sx):
                f_buf[x, e] = blend(ex_side[e, x + 1, 0:Q], ex_g[e, x + 1, 0:Q])
            edge_copy(e).start()

            def tile(I, q0, n):
                at = Y_SECOND if I >= 3 else 0
                if I == 2:
                    at = Y_THIRD - (16 if q0 >= 16 else 0)
                v = msg[at + q0 : at + q0 + n]
                if I in (1, 4) or (I == 2 and q0 >= 16):
                    v = roll_lane(v, nzc)
                return v[:, 0:nzc]

            for q, v in enumerate(coarse_plane(tile)):
                c_g[q, e, :, 0:nzc] = v

        def plane(q, J):
            if J == 0:
                return c_g[q, 0]
            if J == cy + 1:
                return c_g[q, 1]
            return c_all[q, J - 1]

        for e in range(2):
            coarse_step(plane, 1 if e == 0 else cy, wall, coef, c_buf, e, nzc, cx, 2)
            coarse_copy(e).start()

    for e in range(2):
        edge_copy(e).wait()
        coarse_copy(e).wait()


def cost(flops, nbytes):
    return pl.CostEstimate(flops=flops, bytes_accessed=nbytes, transcendentals=0)


def in_hbm(x):
    return pltpu.with_memory_space_constraint(x, pltpu.HBM)


def local(fine_pops, coarse_pops, obstacle, block_level, relax_rates):
    fine = jnp.transpose(fine_pops, (1, 2, 0, 3))
    coarse = jnp.transpose(coarse_pops, (1, 2, 0, 3))
    sx, sy, _, nz = fine.shape
    cx, cy, _, nzc = coarse.shape

    x_message = struct((8 * ((X_FINE + 9 * sy + 7) // 8), LANES))
    up, down = pl.pallas_call(
        pack_x_kernel,
        out_shape=(x_message, x_message),
        in_specs=[ANY] * 3,
        out_specs=(VMEM, VMEM),
        scratch_shapes=[
            pltpu.VMEM((sy, Q, nz), F32),
            pltpu.VMEM((sy, Q, nz), F32),
            pltpu.VMEM((cy, Q, nzc), F32),
            pltpu.VMEM((cy, Q, nzc), F32),
            pltpu.SMEM(block_level.shape, I32),
            pltpu.SemaphoreType.DMA((5,)),
        ],
        compiler_params=params(),
        name="pack_x",
    )(in_hbm(fine), in_hbm(coarse), in_hbm(block_level))
    from_low = lax.ppermute(up, "stream", ring("stream", 1))
    from_high = lax.ppermute(down, "stream", ring("stream", -1))

    levels, coef, flags, c_wall, c_wide, refine, thin = pl.pallas_call(
        tables_kernel,
        out_shape=(
            struct((9, 8, LANES), I32),
            struct((Q + len(EVEN), 8, LANES)),
            struct((2, 8, LANES), I32),
            struct((8, LANES), I32),
            struct((cy, cx, QPAD, nz)),
            struct((2 * nzc, 2 * nz), BF16),
            struct((nz, nz), BF16),
        ),
        in_specs=[VMEM] * 2 + [SMEM] * 2,
        out_specs=(VMEM,) * 7,
        compiler_params=params(),
        cost_estimate=cost(10_000_000, 1_000_000),
        name="tables",
    )(coarse, obstacle, block_level, relax_rates)

    y_message = struct((Y_ROWS, LANES))
    second, first, w_edge = pl.pallas_call(
        pack_y_kernel,
        out_shape=(y_message, y_message, struct((Q, 2, 8, LANES))),
        in_specs=[VMEM] * 5,
        out_specs=(VMEM,) * 3,
        scratch_shapes=[pltpu.VMEM(y_message.shape, F32)] * 2,
        compiler_params=params(),
        name="pack_y",
    )(fine, coarse, from_low, from_high, levels)
    if lax.axis_size("span") % 2 == 0:
        second = lax.ppermute(second, "span", pairs("span", 1))
        first = lax.ppermute(first, "span", pairs("span", 0))
    else:
        second, first = (lax.ppermute(first, "span", ring("span", 1)),
                         lax.ppermute(second, "span", ring("span", -1)))

    fine_shape, coarse_shape = struct(fine.shape), struct(coarse.shape)
    out, c_out, w_in, ex_side, c_all, f_in, aux = pl.pallas_call(
        inner_kernel,
        out_shape=(
            fine_shape,
            coarse_shape,
            struct((Q, sy - 2, 8, LANES)),
            struct((2, sx + 2, QPAD, nz)),
            struct((Q, cy, 8, LANES)),
            struct((sx, sy - 2, Q, nz)),
            struct((Q, 2, 8, LANES)),
        ),
        in_specs=[VMEM] * 12,
        out_specs=(ANY, ANY) + (VMEM,) * 5,
        scratch_shapes=[
            pltpu.VMEM((2, cy, QPAD, nz), F32),
            pltpu.VMEM((sx + 2, QPAD, nz), F32),
            pltpu.VMEM((cx, 1, Q, nzc), F32),
            pltpu.SemaphoreType.DMA((2,)),
        ],
        compiler_params=params(),
        cost_estimate=cost(20_000_000, 1_000_000),
        name="inner",
    )(fine, coarse, from_low, from_high, w_edge, levels, coef, flags, c_wall, c_wide, refine, thin)

    out, c_out = pl.pallas_call(
        outer_kernel,
        out_shape=(fine_shape, coarse_shape),
        in_specs=[VMEM] * 13 + [ANY, ANY],
        out_specs=(ANY, ANY),
        scratch_shapes=[
            pltpu.VMEM((2 * Y_ROWS, LANES), F32),
            pltpu.VMEM((5, QPAD, nz), F32),
            pltpu.VMEM((2, sx + 2, QPAD, nz), F32),
            pltpu.VMEM((9, 8, LANES), F32),
            pltpu.VMEM((Q, 8, LANES), F32),
            pltpu.VMEM((Q, 2, 8, LANES), F32),
            pltpu.VMEM((sx, 2, Q, nz), F32),
            pltpu.VMEM((2, 2, Q, nz), F32),
            pltpu.VMEM((QPAD * cx, nz), F32),
            pltpu.VMEM((cx, 2, Q, nzc), F32),
            pltpu.SemaphoreType.DMA((10,)),
        ],
        input_output_aliases={13: 0, 14: 1},
        compiler_params=params(),
        name="outer",
    )(second, first, w_edge, w_in, c_all, ex_side, f_in, aux, levels, coef, c_wall, refine, thin,
      out, c_out)
    return jnp.transpose(out, (2, 0, 1, 3)), jnp.transpose(c_out, (2, 0, 1, 3))


def solution(mesh):
    placed = (
        P(None, "stream", "span", None),
        P(None, "stream", "span", None),
        P("stream", "span", None),
        P(),
        P(),
    )
    return jax.shard_map(
        local,
        mesh=mesh,
        in_specs=placed,
        out_specs=(P(None, "stream", "span", None), P(None, "stream", "span", None)),
        check_vma=False,
    )
```

```python
import jax
import jax.numpy as jnp
from jax import lax
from jax.experimental import pallas as pl
from jax.experimental.pallas import tpu as pltpu
from jax.sharding import PartitionSpec as P

F32 = jnp.float32
I32 = jnp.int32
BF16 = jnp.bfloat16
Q = 27
QPAD = 32
LANES = 128
OCTETS = [(8 * o, min(8, Q - 8 * o)) for o in range(4)]
STEP = [(q // 9 - 1, q // 3 % 3 - 1, q % 3 - 1) for q in range(Q)]
HIGH_X = [q for q in range(Q) if STEP[q][0] == 1]
LOW_X = [q for q in range(Q) if STEP[q][0] == -1]
HIGH_Y = [q for q in range(Q) if STEP[q][1] == 1]
LOW_Y = [q for q in range(Q) if STEP[q][1] == -1]
EVEN = [9 * a + 3 * b + c for a in (0, 2) for b in (0, 2) for c in (0, 2)]

VMEM = pl.BlockSpec(memory_space=pltpu.VMEM)
SMEM = pl.BlockSpec(memory_space=pltpu.SMEM)
ANY = pl.BlockSpec(memory_space=pl.ANY)
LIMIT = 16 << 20

LEV_BELOW, LEV_ROW, LEV_ABOVE = 0, 1, 2
LEV_X_LOW, LEV_X_HIGH, LEV_OWN, LEV_Y_LOW, LEV_Y_HIGH, EVEN_SPAN = 3, 4, 5, 6, 7, 8

X_FINE, X_MIDDLE = Q, Q + 9
Y_SECOND, Y_THIRD, Y_CORNER = Q, 2 * Q, 2 * Q + 16
Y_ROWS = 80


def fine_slot(k):
    ex = k // 3 - 1
    if ex == 0:
        return 6 * (k % 3), 6, 1
    return 36 + 7 * (k % 3 if ex < 0 else 3 + k % 3), 7, (1 if ex < 0 else 0)


def params(**more):
    return pltpu.CompilerParams(vmem_limit_bytes=LIMIT, **more)


def struct(shape, dtype=F32):
    return jax.ShapeDtypeStruct(shape, dtype)


def ring(axis, by):
    peers = lax.axis_size(axis)
    return [(i, (i + by) % peers) for i in range(peers)]


def pairs(axis, odd):
    peers = lax.axis_size(axis)
    return [(i, (i + (1 if i % 2 == odd else -1)) % peers) for i in range(peers)]


def roll_lane(v, by):
    return v if by == 0 else pltpu.roll(v, by % v.shape[1], 1)


def roll_sub(v, by):
    return v if by == 0 else pltpu.roll(v, by % v.shape[0], 0)


def iota(axis, shape=(8, LANES)):
    return lax.broadcasted_iota(I32, shape, axis)


def row8(ref, at):
    return jnp.broadcast_to(ref[at : at + 1], (8, LANES))


def dot_parts(x, m, count):
    parts = []
    for _ in range(count):
        parts.append(x.astype(BF16))
        x = x - parts[-1].astype(F32)
    return sum(jnp.dot(p, m, preferred_element_type=F32) for p in reversed(parts))


def dot_exact(x, m):
    return dot_parts(x, m, 3)


def pair_of(i):
    a = (i + 1) >> 1
    return a, a + (1 if (i + 1) & 1 else -1)


def blend(a, b):
    return 0.75 * a + 0.25 * b


def pack_x_kernel(fine, coarse, level, up, down, f_low, f_high, c_low, c_high, middle, lev, sems):
    sx, sy, cx = fine.shape[0], fine.shape[1], coarse.shape[0]
    fetch_level = pltpu.make_async_copy(level, lev, sems.at[4])
    copies = [
        pltpu.make_async_copy(fine.at[sx - 1, :, pl.ds(16, Q - 16)], f_high, sems.at[0]),
        pltpu.make_async_copy(coarse.at[cx - 1], c_high, sems.at[1]),
        pltpu.make_async_copy(fine.at[0, :, pl.ds(0, 16)], f_low, sems.at[2]),
        pltpu.make_async_copy(coarse.at[0], c_low, sems.at[3]),
    ]
    fetch_level.start()
    for c in copies:
        c.start()
    for c in copies:
        c.wait()
    cy, nzc = c_low.shape[0], c_low.shape[2]
    for k, (out, f, c, q0) in enumerate(((up, f_high, c_high, HIGH_X[0] - 16), (down, f_low, c_low, LOW_X[0]))):
        middle[k, :, 0:nzc] = c[1, 0:16]
        middle[k, 0 : Q - 16, nzc : 2 * nzc] = c[1, 16:Q]
        out[0:Q, 0:nzc] = c[0]
        out[0:Q, nzc : 2 * nzc] = c[cy - 1]
        for y in range(sy):
            out[X_FINE + 9 * y : X_FINE + 9 * y + 9] = f[y, q0 : q0 + 9]
    fetch_level.wait()
    n_row = lev.shape[0]
    row, col = lax.axis_index("stream"), lax.axis_index("span")
    for k, (out, to) in enumerate(((up, row + 1), (down, row + n_row - 1))):
        both = lev[row, col] * lev[lax.rem(to, n_row), col]
        at = slice(X_MIDDLE, X_MIDDLE + 16)
        out[at] = jnp.where(jnp.full((16, LANES), both, I32) == 1, out[at], middle[k])


def gain_of(q):
    return (1.0 if q // 9 == 0 else 1.0 / 3.0) * (1.0 if q // 3 % 3 == 0 else 1.0 / 3.0) * (
        1.0 if q % 3 == 0 else 1.0 / 3.0)


def tables_kernel(coarse, obstacle, level, rates, levels, coef, flags, c_wall, c_wide, refine, thin):
    cx, cy, nzc = coarse.shape[0], coarse.shape[1], coarse.shape[3]
    sx, sy, nz = obstacle.shape
    row, col = lax.axis_index("stream"), lax.axis_index("span")
    n_row, n_col = level.shape
    at_row = [lax.rem(row + n_row - 1, n_row), row, lax.rem(row + 1, n_row)]
    at_col = [lax.rem(col + n_col - 1, n_col), col, lax.rem(col + 1, n_col)]
    lane, sub = iota(1), iota(0)
    for k in range(3):
        levels[k] = jnp.where(sub == 0, level[at_row[0], at_col[k]],
                              jnp.where(sub == sx + 1, level[at_row[2], at_col[k]], level[at_row[1], at_col[k]]))
    for k, (r, c) in ((LEV_X_LOW, (0, 1)), (LEV_X_HIGH, (2, 1)), (LEV_OWN, (1, 1)), (LEV_Y_LOW, (1, 0)),
                      (LEV_Y_HIGH, (1, 2))):
        levels[k] = jnp.full((8, LANES), level[at_row[r], at_col[c]], I32)
    even = lax.rem(col, 2) == 0 if n_col % 2 == 0 else True
    levels[EVEN_SPAN] = jnp.full((8, LANES), jnp.where(even, 1, 0), I32)
    refined = levels[LEV_OWN] == 1
    for q in range(Q):
        s = jnp.full((8, LANES), rates[q], F32)
        s = jnp.where(refined, s, 1.0 / (2.0 / s - 0.5))
        coef[q] = 0.125 - 0.125 * s
        if q in EVEN:
            coef[Q + EVEN.index(q)] = (0.125 * gain_of(q)) * s
    planes = []
    for k, y in enumerate((sy // 2 - 1, sy // 2)):
        v = jnp.zeros((8, LANES), I32)
        for x in (sx // 2 - 1, sx // 2):
            v = jnp.where(sub == x + 1, jnp.broadcast_to(obstacle[x, y : y + 1, :], (8, LANES)), v)
        flags[k] = v
        planes.append(v)
    both = jnp.maximum(planes[0], planes[1])
    both = jnp.maximum(both, roll_sub(both, -1))
    both = jnp.maximum(both, roll_lane(both, -1))
    both = jnp.take_along_axis(both, (2 * lane) & (LANES - 1), axis=1)
    both = jnp.broadcast_to(both[sx // 2 : sx // 2 + 1], (8, LANES))
    c_wall[...] = jnp.where((sub == 1 + cx // 2) & (lane < nzc), both, 0)
    shape = (2 * nzc, 2 * nz)
    i, l = iota(0, shape), iota(1, shape)
    half, l = l // nz, l % nz
    za = (l >> 1) + half * nzc
    zb = jnp.clip((l >> 1) + jnp.where((l & 1) == 1, 1, -1), 0, nzc - 1) + half * nzc
    refine[...] = (jnp.where(i == za, 0.75, 0.0) + jnp.where(i == zb, 0.25, 0.0)).astype(BF16)
    shape = (nz, nz)
    thin[...] = jnp.where((iota(0, shape) >> 1) == iota(1, shape), 0.125, 0.0).astype(BF16)
    for Y in range(cy):
        for X in range(cx):
            c_wide[Y, X, 0:Q] = dot_exact(coarse[X, Y], refine[0:nzc, 0:nz])


def fine_plane(fine, from_low, from_high, y, mixed=None):
    sx = fine.shape[0]
    base = X_FINE + 9 * y
    rows = [None] * Q
    for q0, n in OCTETS:
        cells = [fine[x, y, q0 : q0 + n] for x in range(sx)]
        low = high = cells[0]
        if q0 == 16:
            low = from_low[base - 2 : base + 6]
        if q0 == 24:
            low = from_low[base + 6 : base + 9]
        if q0 == 0:
            high = from_high[base : base + 8]
        if q0 == 8:
            high = row8(from_high, base + 8)
        if mixed is not None:
            if q0 >= 16:
                low = mixed(0, q0, n, low)
            else:
                high = mixed(1, q0, n, high)
        tile = jnp.swapaxes(jnp.stack([low, *cells, high]), 0, 1)
        for k in range(n):
            rows[q0 + k] = tile[k]
    return rows


def coarse_plane(tile_of):
    rows = [None] * Q
    for q0, n in OCTETS:
        tiles = [tile_of(I, q0, n) for I in range(5)]
        tile = jnp.swapaxes(jnp.stack(tiles + tiles[:3]), 0, 1)
        for k in range(n):
            rows[q0 + k] = tile[k]
    return rows


def pack_y_kernel(fine, coarse, from_low, from_high, levels, second, first, w_edge, up, down):
    sy, cy, nzc = fine.shape[1], coarse.shape[1], coarse.shape[3]
    low_half = iota(1, (Q, LANES)) < nzc
    own = levels[LEV_OWN] == 1
    for out, e, y, Y, qs, to in ((up, 1, sy - 1, cy - 1, HIGH_Y, LEV_Y_HIGH), (down, 0, 0, 0, LOW_Y, LEV_Y_LOW)):
        both = own & (levels[to] == 1)
        g_low, g_high = from_low[0:Q], from_high[0:Q]
        if e == 0:
            g_high = roll_lane(g_high, nzc)
        else:
            g_low = roll_lane(g_low, nzc)
        out[0:Q] = g_low
        out[0:Q, nzc : 2 * nzc] = coarse[0, Y]
        out[Y_SECOND : Y_SECOND + Q] = g_high
        out[Y_SECOND : Y_SECOND + Q, 0:nzc] = coarse[2, Y]
        out[Y_THIRD : Y_THIRD + 16, 0:nzc] = coarse[1, Y, 0:16]
        out[Y_THIRD : Y_THIRD + Q - 16, nzc : 2 * nzc] = coarse[1, Y, 16:Q]
        rows = fine_plane(fine, from_low, from_high, y)
        for q in range(Q):
            w_edge[q, e] = rows[q]
        for k in range(3):
            out[Y_CORNER + k : Y_CORNER + k + 1] = rows[qs[6 + k]][0:1]
            out[Y_CORNER + 3 + k : Y_CORNER + 4 + k] = rows[qs[k]][7:8]
        for k, q in enumerate(qs):
            at, n, s = fine_slot(k)
            out[at : at + n] = jnp.where(both[0:n], rows[q][s : s + n], out[at : at + n])
    even = levels[EVEN_SPAN] == 1
    for at in range(0, Y_ROWS, 8):
        a, b = up[at : at + 8], down[at : at + 8]
        first[at : at + 8] = jnp.where(even, a, b)
        second[at : at + 8] = jnp.where(even, b, a)


def forward(m0, m1, m2):
    pair = m0 + m2
    return pair + 4.0 * m1, m2 - m0, pair


ALONG_Y = [(9 * a + c, 3) for a in range(3) for c in range(3)]
ALONG_Z = [(9 * a + 3 * b, 1) for a in range(3) for b in range(3)]
ALONG_X = [(r, 9) for r in range(9)]


def collide(g, coef):
    t = [None] * Q
    for r in range(9):
        t[r], t[9 + r], t[18 + r] = forward(g[r], g[9 + r], g[18 + r])
    cols = [(t[c] + t[6 + c]) + 4.0 * t[3 + c] for c in range(3)]
    density = (cols[0] + cols[2]) + 4.0 * cols[1]
    inv = 1.0 / density
    rows = [(t[3 * b] + t[3 * b + 2]) + 4.0 * t[3 * b + 1] for b in (0, 2)]
    uy = (rows[1] - rows[0]) * inv
    uz = (cols[2] - cols[0]) * inv
    dcols = [(t[9 + c] + t[15 + c]) + 4.0 * t[12 + c] for c in range(3)]
    ux = ((dcols[0] + dcols[2]) + 4.0 * dcols[1]) * inv
    for r in range(9):
        t0, d, pair = t[r], t[9 + r], t[18 + r]
        t1 = d - ux * t0
        t[9 + r], t[18 + r] = t1, pair - ux * (d + t1)
    for u, lines in ((uy, ALONG_Y), (uz, ALONG_Z)):
        for at, by in lines:
            t0, d, pair = forward(t[at], t[at + by], t[at + 2 * by])
            t1 = d - u * t0
            t[at], t[at + by], t[at + 2 * by] = t0, t1, pair - u * (d + t1)
    for q in range(Q):
        t[q] = coef[q] * t[q]
        if q in EVEN:
            t[q] = t[q] + coef[Q + EVEN.index(q)] * density
    for u, lines in ((uz, ALONG_Z), (uy, ALONG_Y), (ux, ALONG_X)):
        for at, by in lines:
            t0, t1, t2 = t[at], t[at + by], t[at + 2 * by]
            d = t1 + u * t0
            s = t2 + u * (t1 + d)
            t[at], t[at + by], t[at + 2 * by] = s - d, 0.5 * (t0 - s), s + d
    return t


def pull(source, center, step_mask):
    out = []
    for q in range(Q):
        ex, ey, ez = STEP[q]
        v = roll_lane(roll_sub(source(q), ex), ez)
        mask = step_mask(ex, ey, ez)
        if mask is not None:
            v = jnp.where(mask, center(26 - q), v)
        out.append(v)
    return out


def bounce_mask(height, wall_of):
    lane = iota(1)
    edges = {1: lane == 0, -1: lane == height - 1}

    def mask_of(ex, ey, ez):
        m = None
        if (ex, ey, ez) == (0, 0, 0):
            return None
        wall = wall_of(ey)
        if wall is not None:
            m = roll_lane(roll_sub(wall, ex), ez) == 1
        if ez != 0:
            m = edges[ez] if m is None else m | edges[ez]
        return m

    return mask_of


def wall_plane(flags, y, first):
    def wall_of(ey):
        k = y - ey - first
        return flags[k] if k in (0, 1) else None

    return wall_of


def store_rows(rows, out, t, xs, width):
    for q0, n in OCTETS:
        tile = jnp.swapaxes(jnp.stack(rows[q0 : q0 + n]), 0, 1)
        for k, x in enumerate(xs):
            out[k, t, q0 : q0 + n] = tile[x][:, 0:width]


def coalesce(planes, out, at, thin):
    nzc = out.shape[3]
    for X in range(out.shape[0]):
        s = sum(p[2 * X] + p[2 * X + 1] for p in planes)
        out[X, at] = dot_exact(s, thin[...])[:, 0:nzc]


def coarse_step(plane, J, wall, coef, buf, at, nzc, cx, wall_row):
    mask_of = bounce_mask(nzc, lambda ey: wall if J - ey == wall_row else None)
    new = collide(pull(lambda q: plane(q, J - STEP[q][1]), lambda q: plane(q, J), mask_of), coef)
    if J == wall_row:
        stay = wall == 1
        new = [jnp.where(stay, plane(q, J), new[q]) for q in range(Q)]
    store_rows(new, buf, at, range(1, cx + 1), nzc)


def inner_kernel(fine, coarse, from_low, from_high, w_edge, levels, coef, flags, c_wall, c_wide, refine, thin,
                 out, c_out, w_in, ex_side, c_all, f_in, aux, ghost, ex_mid, c_buf, sems):
    sx, sy, nz = fine.shape[0], fine.shape[1], fine.shape[3]
    cx, cy, nzc = coarse.shape[0], coarse.shape[1], coarse.shape[3]
    mid = sy // 2
    own = jnp.max(levels[LEV_OWN])
    n = 8 * ((X_MIDDLE + 16 + 7) // 8)
    both = dot_exact(jnp.concatenate([from_low[0:n], from_high[0:n]], axis=0), refine[...])
    for side in range(2):
        v = both[side * n : side * n + n]
        ghost[side, 0, 0:Q] = v[0:Q, 0:nz]
        ghost[side, cy - 1, 0:Q] = v[0:Q, nz : 2 * nz]
        ghost[side, 1, 0:16] = v[X_MIDDLE : X_MIDDLE + 16, 0:nz]
        ghost[side, 1, 16:Q] = v[X_MIDDLE : X_MIDDLE + Q - 16, nz : 2 * nz]

    def wide(J, I):
        if I == 0:
            return ghost[0, J - 1]
        if I == cx + 1:
            return ghost[1, J - 1]
        return c_wide[J - 1, I - 1]

    for J in range(1, cy + 1):
        for i in range(sx + 2):
            a, b = pair_of(i)
            v = blend(wide(J, a), wide(J, b))
            if J == 2:
                ex_mid[i] = v
            else:
                ex_side[J // 2, i] = v

    def exploded(J, i):
        return ex_mid.at[i] if J == 2 else ex_side.at[J // 2, i]

    copies = [pltpu.make_async_copy(f_in.at[:, pl.ds(mid - 2, 2)], out.at[:, pl.ds(mid - 1, 2)], sems.at[0]),
              pltpu.make_async_copy(c_buf, c_out.at[:, pl.ds(cy // 2, 1)], sems.at[1]),
              pltpu.make_async_copy(f_in, out.at[:, pl.ds(1, sy - 2)], sems.at[0])]

    @pl.when(own == 1)
    def _():
        refined = (levels[LEV_X_LOW] == 1, levels[LEV_X_HIGH] == 1)
        sub = iota(0)
        for y in range(1, sy - 1):
            a, b = pair_of(y + 1)

            def mixed(side, q0, n, tile):
                i = 0 if side == 0 else sx + 1
                e = blend(exploded(a, i)[q0 : q0 + n], exploded(b, i)[q0 : q0 + n])
                return jnp.where(refined[side][0:n], tile, e)

            rows = fine_plane(fine, from_low, from_high, y, mixed)
            for q in range(Q):
                w_in[q, y - 1] = rows[q]

        def plane(q, y):
            if y in (0, sy - 1):
                return w_edge[q, 0 if y == 0 else 1]
            return w_in[q, y - 1]

        for y in (mid - 1, mid, 1, sy - 2):
            pulled = pull(lambda q: plane(q, y - STEP[q][1]), lambda q: plane(q, y),
                          bounce_mask(nz, wall_plane(flags, y, mid - 1)))
            if y in (1, sy - 2):
                for q in range(Q):
                    aux[q, 0 if y == 1 else 1] = jnp.where(sub == 0, roll_sub(pulled[q], -1), roll_sub(pulled[q], 1))
            new = collide(pulled, coef)
            if y in (mid - 1, mid):
                stay = flags[y - mid + 1] == 1
                new = [jnp.where(stay, w_in[q, y - 1], new[q]) for q in range(Q)]
            store_rows(new, f_in, y - 1, range(1, sx + 1), nz)
            if y == mid:
                copies[0].start()
                coalesce([f_in.at[:, mid - 2], f_in.at[:, mid - 1]], c_buf, 0, thin)
                copies[1].start()
        copies[0].wait()

    @pl.when(own != 1)
    def _():
        for y in range(1, sy - 1):
            a, b = pair_of(y + 1)
            for x in range(sx):
                f_in[x, y - 1] = blend(exploded(a, x + 1)[0:Q], exploded(b, x + 1)[0:Q])
        copies[2].start()

        def tile_of(Y):
            def tile(I, q0, n):
                if 1 <= I <= cx:
                    return coarse[I - 1, Y, q0 : q0 + n]
                msg = from_low if I == 0 else from_high
                if Y != 1:
                    v = msg[q0 : q0 + n]
                    return (v if Y == 0 else roll_lane(v, nzc))[:, 0:nzc]
                if q0 < 16:
                    return msg[X_MIDDLE + q0 : X_MIDDLE + q0 + n, 0:nzc]
                return roll_lane(msg[X_MIDDLE + q0 - 16 : X_MIDDLE + q0 - 16 + n], nzc)[:, 0:nzc]

            return tile

        for Y in range(cy):
            for q, v in enumerate(coarse_plane(tile_of(Y))):
                c_all[q, Y, :, 0:nzc] = v
        coarse_step(lambda q, J: c_all[q, J - 1], 2, c_wall[...], coef, c_buf, 0, nzc, cx, 2)
        copies[1].start()
        copies[2].wait()

    copies[1].wait()


def outer_kernel(second, first, w_edge, w_in, c_all, ex_side, f_in, aux, levels, coef, c_wall, refine, thin,
                 _out_in, _c_in, out, c_out, msgs, wide, ex_g, w_g, w_e, c_g, f_buf, f_fix, s_buf, c_buf, sems):
    sx, sy, nz = out.shape[0], out.shape[1], out.shape[3]
    cx, cy, nzc = c_out.shape[0], c_out.shape[1], c_out.shape[3]
    own = jnp.max(levels[LEV_OWN])
    sub = iota(0)
    even = levels[EVEN_SPAN] == 1
    for at in range(0, Y_ROWS, 8):
        a, b = first[at : at + 8], second[at : at + 8]
        msgs[at : at + 8] = jnp.where(even, b, a)
        msgs[Y_ROWS + at : Y_ROWS + at + 8] = jnp.where(even, a, b)
    v = dot_exact(msgs[...], refine[...])
    for e in range(2):
        at = Y_ROWS * e
        wide[0, 0:Q] = v[at : at + Q, 0:nz]
        wide[1, 0:Q] = v[at : at + Q, nz : 2 * nz]
        wide[3, 0:Q] = v[at + Y_SECOND : at + Y_SECOND + Q, 0:nz]
        wide[4, 0:Q] = v[at + Y_SECOND : at + Y_SECOND + Q, nz : 2 * nz]
        wide[2, 0:16] = v[at + Y_THIRD : at + Y_THIRD + 16, 0:nz]
        wide[2, 16:Q] = v[at + Y_THIRD : at + Y_THIRD + Q - 16, nz : 2 * nz]
        for i in range(sx + 2):
            a, b = pair_of(i)
            ex_g[e, i] = blend(wide[a], wide[b])

    def edge_copy(e):
        y = (sy - 1) * e
        return pltpu.make_async_copy(f_buf.at[:, pl.ds(e, 1)], out.at[:, pl.ds(y, 1)], sems.at[e])

    def coarse_copy(e):
        return pltpu.make_async_copy(c_buf.at[:, pl.ds(e, 1)], c_out.at[:, pl.ds((cy - 1) * e, 1)], sems.at[2 + e])

    @pl.when(own == 1)
    def _():
        ready = [pltpu.make_async_copy(f_in.at[pl.ds(1, sx - 2), pl.ds((sy - 3) * e, 1)],
                                       out.at[pl.ds(1, sx - 2), pl.ds(1 + (sy - 3) * e, 1)], sems.at[4 + e])
                 for e in range(2)]
        fixed = [[pltpu.make_async_copy(f_fix.at[pl.ds(side, 1), pl.ds(e, 1)],
                                        out.at[pl.ds((sx - 1) * side, 1), pl.ds(1 + (sy - 3) * e, 1)],
                                        sems.at[6 + 2 * e + side]) for side in range(2)] for e in range(2)]
        for c in ready:
            c.start()
        lane = iota(1)
        inside = {0: None, 1: lane != 0, -1: lane != nz - 1}
        for e in range(2):
            msg = msgs.at[pl.ds(Y_ROWS * e, Y_ROWS)]
            qs = HIGH_Y if e == 0 else LOW_Y
            far = levels[LEV_BELOW if e == 0 else LEV_ABOVE] == 1
            near = levels[LEV_Y_LOW if e == 0 else LEV_Y_HIGH] == 1
            for q0, n in OCTETS:
                tiles = [blend(ex_g[e, i, q0 : q0 + n], ex_side[e, i, q0 : q0 + n]) for i in range(sx + 2)]
                tile = jnp.swapaxes(jnp.stack(tiles), 0, 1)
                for k, q in enumerate(qs):
                    if q0 <= q < q0 + n:
                        at, _, s = fine_slot(k)
                        v = roll_sub(msg[at : at + 8], s)
                        if STEP[q][0] != 0:
                            corner = Y_CORNER + k % 3 + (0 if STEP[q][0] > 0 else 3)
                            v = jnp.where(near, v, row8(msg, corner))
                        w_g[k] = jnp.where(far, v, tile[q - q0])
            coarse_low = (levels[LEV_X_LOW] != 1) & (sub == 0)
            coarse_high = (levels[LEV_X_HIGH] != 1) & (sub == sx + 1)
            v_low = blend(ex_side[e, 0], ex_g[e, 0])
            v_high = blend(ex_side[e, sx + 1], ex_g[e, sx + 1])
            for q in range(Q):
                v = w_edge[q, e]
                if STEP[q][0] > 0:
                    v = jnp.where(coarse_low, jnp.broadcast_to(v_low[q : q + 1], (8, LANES)), v)
                if STEP[q][0] < 0:
                    v = jnp.where(coarse_high, jnp.broadcast_to(v_high[q : q + 1], (8, LANES)), v)
                w_e[q] = v

            def source(q):
                return (w_g[qs.index(q)] if q in qs else
                        w_e[q] if STEP[q][1] == 0 else w_in[q, (sy - 3) * e])

            pulled = pull(source, lambda q: w_e[q], bounce_mask(nz, lambda ey: None))
            spare = (sub == 0) | (sub == sx + 1)
            for q in range(Q):
                ex, _, ez = STEP[q]
                v = aux[q, e]
                if q in qs and ex != 0:
                    m = sub == (0 if ex > 0 else sx + 1)
                    if ez != 0:
                        m = m & inside[ez]
                    v = jnp.where(m, roll_lane(w_e[q], ez), v)
                pulled[q] = jnp.where(spare, v, pulled[q])
            new = collide(pulled, coef)
            for q0, n in OCTETS:
                tile = jnp.swapaxes(jnp.stack(new[q0 : q0 + n]), 0, 1)
                for x in range(sx):
                    f_buf[x, e, q0 : q0 + n] = tile[x + 1]
                f_fix[0, e, q0 : q0 + n] = tile[0]
                f_fix[1, e, q0 : q0 + n] = tile[sx + 1]
            edge_copy(e).start()
            for c in fixed[e]:
                c.start()

            def beside(x):
                if x in (0, sx - 1):
                    return f_fix[0 if x == 0 else 1, e]
                return f_in[x, (sy - 3) * e]

            for X in range(cx):
                at = QPAD * (cx * e + X)
                s_buf[at : at + Q] = ((f_buf[2 * X, e] + f_buf[2 * X + 1, e])
                                      + (beside(2 * X) + beside(2 * X + 1)))
        mean = dot_parts(s_buf[...], thin[...], 2)
        for e in range(2):
            for X in range(cx):
                at = QPAD * (cx * e + X)
                c_buf[X, e] = mean[at : at + Q, 0:nzc]
            coarse_copy(e).start()
        for c in ready + fixed[0] + fixed[1]:
            c.wait()

    @pl.when(own != 1)
    def _():
        wall = c_wall[...]

        for e in range(2):
            msg = msgs.at[pl.ds(Y_ROWS * e, Y_ROWS)]
            for x in range(sx):
                f_buf[x, e] = blend(ex_side[e, x + 1, 0:Q], ex_g[e, x + 1, 0:Q])
            edge_copy(e).start()

            def tile(I, q0, n):
                at = Y_SECOND if I >= 3 else 0
                if I == 2:
                    at = Y_THIRD - (16 if q0 >= 16 else 0)
                v = msg[at + q0 : at + q0 + n]
                if I in (1, 4) or (I == 2 and q0 >= 16):
                    v = roll_lane(v, nzc)
                return v[:, 0:nzc]

            for q, v in enumerate(coarse_plane(tile)):
                c_g[q, e, :, 0:nzc] = v

        def plane(q, J):
            if J == 0:
                return c_g[q, 0]
            if J == cy + 1:
                return c_g[q, 1]
            return c_all[q, J - 1]

        lower = sub < 4

        def joined(a, b, by):
            return jnp.where(lower, roll_sub(a, by), roll_sub(b, by + 4))

        lane = iota(1)
        edges = {1: lane == 0, -1: lane == nzc - 1}
        none = jnp.zeros((8, LANES), I32)
        center = [joined(plane(q, 1), plane(q, cy), 0) for q in range(Q)]
        pulled = []
        for q in range(Q):
            ex, ey, ez = STEP[q]
            if (ex, ey, ez) == (0, 0, 0):
                pulled.append(center[q])
                continue
            v = roll_lane(joined(plane(q, 1 - ey), plane(q, cy - ey), ex), ez)
            m = None
            if ey != 0:
                walls = (wall, none) if ey < 0 else (none, wall)
                m = roll_lane(joined(*walls, ex), ez) == 1
            if ez != 0:
                m = edges[ez] if m is None else m | edges[ez]
            pulled.append(v if m is None else jnp.where(m, center[26 - q], v))
        new = collide(pulled, coef)
        for q0, n in OCTETS:
            tile = jnp.swapaxes(jnp.stack(new[q0 : q0 + n]), 0, 1)
            for e in range(2):
                for X in range(cx):
                    c_buf[X, e, q0 : q0 + n] = tile[1 + X + 4 * e][:, 0:nzc]
        for e in range(2):
            coarse_copy(e).start()

    for e in range(2):
        edge_copy(e).wait()
        coarse_copy(e).wait()


def cost(flops, nbytes):
    return pl.CostEstimate(flops=flops, bytes_accessed=nbytes, transcendentals=0)


def in_hbm(x):
    return pltpu.with_memory_space_constraint(x, pltpu.HBM)


def local(fine_pops, coarse_pops, obstacle, block_level, relax_rates):
    fine = jnp.transpose(fine_pops, (1, 2, 0, 3))
    coarse = jnp.transpose(coarse_pops, (1, 2, 0, 3))
    sx, sy, _, nz = fine.shape
    cx, cy, _, nzc = coarse.shape

    x_message = struct((8 * ((X_FINE + 9 * sy + 7) // 8), LANES))
    up, down = pl.pallas_call(
        pack_x_kernel,
        out_shape=(x_message, x_message),
        in_specs=[ANY] * 3,
        out_specs=(VMEM, VMEM),
        scratch_shapes=[
            pltpu.VMEM((sy, 16, nz), F32),
            pltpu.VMEM((sy, Q - 16, nz), F32),
            pltpu.VMEM((cy, Q, nzc), F32),
            pltpu.VMEM((cy, Q, nzc), F32),
            pltpu.VMEM((2, 16, LANES), F32),
            pltpu.SMEM(block_level.shape, I32),
            pltpu.SemaphoreType.DMA((5,)),
        ],
        compiler_params=params(),
        name="pack_x",
    )(in_hbm(fine), in_hbm(coarse), in_hbm(block_level))
    from_low = lax.ppermute(up, "stream", ring("stream", 1))
    from_high = lax.ppermute(down, "stream", ring("stream", -1))

    levels, coef, flags, c_wall, c_wide, refine, thin = pl.pallas_call(
        tables_kernel,
        out_shape=(
            struct((9, 8, LANES), I32),
            struct((Q + len(EVEN), 8, LANES)),
            struct((2, 8, LANES), I32),
            struct((8, LANES), I32),
            struct((cy, cx, QPAD, nz)),
            struct((2 * nzc, 2 * nz), BF16),
            struct((nz, nz), BF16),
        ),
        in_specs=[VMEM] * 2 + [SMEM] * 2,
        out_specs=(VMEM,) * 7,
        compiler_params=params(),
        cost_estimate=cost(10_000_000, 1_000_000),
        name="tables",
    )(coarse, obstacle, block_level, relax_rates)

    y_message = struct((Y_ROWS, LANES))
    second, first, w_edge = pl.pallas_call(
        pack_y_kernel,
        out_shape=(y_message, y_message, struct((Q, 2, 8, LANES))),
        in_specs=[VMEM] * 5,
        out_specs=(VMEM,) * 3,
        scratch_shapes=[pltpu.VMEM(y_message.shape, F32)] * 2,
        compiler_params=params(),
        name="pack_y",
    )(fine, coarse, from_low, from_high, levels)
    if lax.axis_size("span") % 2 == 0:
        second = lax.ppermute(second, "span", pairs("span", 1))
        first = lax.ppermute(first, "span", pairs("span", 0))
    else:
        second, first = (lax.ppermute(first, "span", ring("span", 1)),
                         lax.ppermute(second, "span", ring("span", -1)))

    fine_shape, coarse_shape = struct(fine.shape), struct(coarse.shape)
    out, c_out, w_in, ex_side, c_all, f_in, aux = pl.pallas_call(
        inner_kernel,
        out_shape=(
            fine_shape,
            coarse_shape,
            struct((Q, sy - 2, 8, LANES)),
            struct((2, sx + 2, QPAD, nz)),
            struct((Q, cy, 8, LANES)),
            struct((sx, sy - 2, Q, nz)),
            struct((Q, 2, 8, LANES)),
        ),
        in_specs=[VMEM] * 12,
        out_specs=(ANY, ANY) + (VMEM,) * 5,
        scratch_shapes=[
            pltpu.VMEM((2, cy, QPAD, nz), F32),
            pltpu.VMEM((sx + 2, QPAD, nz), F32),
            pltpu.VMEM((cx, 1, Q, nzc), F32),
            pltpu.SemaphoreType.DMA((2,)),
        ],
        compiler_params=params(),
        cost_estimate=cost(20_000_000, 1_000_000),
        name="inner",
    )(fine, coarse, from_low, from_high, w_edge, levels, coef, flags, c_wall, c_wide, refine, thin)

    out, c_out = pl.pallas_call(
        outer_kernel,
        out_shape=(fine_shape, coarse_shape),
        in_specs=[VMEM] * 13 + [ANY, ANY],
        out_specs=(ANY, ANY),
        scratch_shapes=[
            pltpu.VMEM((2 * Y_ROWS, LANES), F32),
            pltpu.VMEM((5, QPAD, nz), F32),
            pltpu.VMEM((2, sx + 2, QPAD, nz), F32),
            pltpu.VMEM((9, 8, LANES), F32),
            pltpu.VMEM((Q, 8, LANES), F32),
            pltpu.VMEM((Q, 2, 8, LANES), F32),
            pltpu.VMEM((sx, 2, Q, nz), F32),
            pltpu.VMEM((2, 2, Q, nz), F32),
            pltpu.VMEM((2 * QPAD * cx, nz), F32),
            pltpu.VMEM((cx, 2, Q, nzc), F32),
            pltpu.SemaphoreType.DMA((10,)),
        ],
        input_output_aliases={13: 0, 14: 1},
        compiler_params=params(),
        name="outer",
    )(second, first, w_edge, w_in, c_all, ex_side, f_in, aux, levels, coef, c_wall, refine, thin,
      out, c_out)
    return jnp.transpose(out, (2, 0, 1, 3)), jnp.transpose(c_out, (2, 0, 1, 3))


def solution(mesh):
    placed = (
        P(None, "stream", "span", None),
        P(None, "stream", "span", None),
        P("stream", "span", None),
        P(),
        P(),
    )
    return jax.shard_map(
        local,
        mesh=mesh,
        in_specs=placed,
        out_specs=(P(None, "stream", "span", None), P(None, "stream", "span", None)),
        check_vma=False,
    )
```

```python
import jax
import jax.numpy as jnp
from jax import lax
from jax.experimental import pallas as pl
from jax.experimental.pallas import tpu as pltpu
from jax.sharding import PartitionSpec as P

F32 = jnp.float32
I32 = jnp.int32
BF16 = jnp.bfloat16
Q = 27
QPAD = 32
LANES = 128
OCTETS = [(8 * o, min(8, Q - 8 * o)) for o in range(4)]
STEP = [(q // 9 - 1, q // 3 % 3 - 1, q % 3 - 1) for q in range(Q)]
HIGH_X = [q for q in range(Q) if STEP[q][0] == 1]
LOW_X = [q for q in range(Q) if STEP[q][0] == -1]
HIGH_Y = [q for q in range(Q) if STEP[q][1] == 1]
LOW_Y = [q for q in range(Q) if STEP[q][1] == -1]
EVEN = [9 * a + 3 * b + c for a in (0, 2) for b in (0, 2) for c in (0, 2)]

VMEM = pl.BlockSpec(memory_space=pltpu.VMEM)
SMEM = pl.BlockSpec(memory_space=pltpu.SMEM)
ANY = pl.BlockSpec(memory_space=pl.ANY)
LIMIT = 16 << 20

LEV_BELOW, LEV_ROW, LEV_ABOVE = 0, 1, 2
LEV_X_LOW, LEV_X_HIGH, LEV_OWN, LEV_Y_LOW, LEV_Y_HIGH, EVEN_SPAN = 3, 4, 5, 6, 7, 8

X_FINE, X_MIDDLE = Q, Q + 9
Y_SECOND, Y_THIRD, Y_CORNER = Q, 2 * Q, 2 * Q + 16
Y_ROWS = 80


def fine_slot(k):
    ex = k // 3 - 1
    if ex == 0:
        return 6 * (k % 3), 6, 1
    return 36 + 7 * (k % 3 if ex < 0 else 3 + k % 3), 7, (1 if ex < 0 else 0)


def params(**more):
    return pltpu.CompilerParams(vmem_limit_bytes=LIMIT, **more)


def struct(shape, dtype=F32):
    return jax.ShapeDtypeStruct(shape, dtype)


def ring(axis, by):
    peers = lax.axis_size(axis)
    return [(i, (i + by) % peers) for i in range(peers)]


def pairs(axis, odd):
    peers = lax.axis_size(axis)
    return [(i, (i + (1 if i % 2 == odd else -1)) % peers) for i in range(peers)]


def roll_lane(v, by):
    return v if by == 0 else pltpu.roll(v, by % v.shape[1], 1)


def roll_sub(v, by):
    return v if by == 0 else pltpu.roll(v, by % v.shape[0], 0)


def iota(axis, shape=(8, LANES)):
    return lax.broadcasted_iota(I32, shape, axis)


def row8(ref, at):
    return jnp.broadcast_to(ref[at : at + 1], (8, LANES))


def dot_parts(x, m, count):
    parts = []
    for _ in range(count):
        parts.append(x.astype(BF16))
        x = x - parts[-1].astype(F32)
    return sum(jnp.dot(p, m, preferred_element_type=F32) for p in reversed(parts))


def dot_exact(x, m):
    return dot_parts(x, m, 3)


def pair_of(i):
    a = (i + 1) >> 1
    return a, a + (1 if (i + 1) & 1 else -1)


def blend(a, b):
    return 0.75 * a + 0.25 * b


def pack_x_kernel(fine, coarse, level, up, down, f_low, f_high, c_low, c_high, middle, lev, sems):
    sx, sy, cx = fine.shape[0], fine.shape[1], coarse.shape[0]
    fetch_level = pltpu.make_async_copy(level, lev, sems.at[4])
    copies = [
        pltpu.make_async_copy(fine.at[sx - 1, :, pl.ds(16, Q - 16)], f_high, sems.at[0]),
        pltpu.make_async_copy(coarse.at[cx - 1], c_high, sems.at[1]),
        pltpu.make_async_copy(fine.at[0, :, pl.ds(0, 16)], f_low, sems.at[2]),
        pltpu.make_async_copy(coarse.at[0], c_low, sems.at[3]),
    ]
    fetch_level.start()
    for c in copies:
        c.start()
    for c in copies:
        c.wait()
    cy, nzc = c_low.shape[0], c_low.shape[2]
    for k, (out, f, c, q0) in enumerate(((up, f_high, c_high, HIGH_X[0] - 16), (down, f_low, c_low, LOW_X[0]))):
        middle[k, :, 0:nzc] = c[1, 0:16]
        middle[k, 0 : Q - 16, nzc : 2 * nzc] = c[1, 16:Q]
        out[0:Q, 0:nzc] = c[0]
        out[0:Q, nzc : 2 * nzc] = c[cy - 1]
        for y in range(sy):
            out[X_FINE + 9 * y : X_FINE + 9 * y + 9] = f[y, q0 : q0 + 9]
    fetch_level.wait()
    n_row = lev.shape[0]
    row, col = lax.axis_index("stream"), lax.axis_index("span")
    for k, (out, to) in enumerate(((up, row + 1), (down, row + n_row - 1))):
        both = lev[row, col] * lev[lax.rem(to, n_row), col]
        at = slice(X_MIDDLE, X_MIDDLE + 16)
        out[at] = jnp.where(jnp.full((16, LANES), both, I32) == 1, out[at], middle[k])


def gain_of(q):
    return (1.0 if q // 9 == 0 else 1.0 / 3.0) * (1.0 if q // 3 % 3 == 0 else 1.0 / 3.0) * (
        1.0 if q % 3 == 0 else 1.0 / 3.0)


def tables_kernel(fine_far, coarse_far, obstacle_far, level, rates,
                  levels, coef, flags, c_wall, c_wide, refine, thin, fine, coarse, obstacle, sems):
    arrive = [pltpu.make_async_copy(a, b, sems.at[k]) for k, (a, b) in enumerate(
        ((obstacle_far, obstacle), (coarse_far, coarse), (fine_far, fine)))]
    for c in arrive:
        c.start()
    cx, cy, nzc = coarse.shape[0], coarse.shape[1], coarse.shape[3]
    sx, sy, nz = obstacle.shape
    row, col = lax.axis_index("stream"), lax.axis_index("span")
    n_row, n_col = level.shape
    at_row = [lax.rem(row + n_row - 1, n_row), row, lax.rem(row + 1, n_row)]
    at_col = [lax.rem(col + n_col - 1, n_col), col, lax.rem(col + 1, n_col)]
    lane, sub = iota(1), iota(0)
    for k in range(3):
        levels[k] = jnp.where(sub == 0, level[at_row[0], at_col[k]],
                              jnp.where(sub == sx + 1, level[at_row[2], at_col[k]], level[at_row[1], at_col[k]]))
    for k, (r, c) in ((LEV_X_LOW, (0, 1)), (LEV_X_HIGH, (2, 1)), (LEV_OWN, (1, 1)), (LEV_Y_LOW, (1, 0)),
                      (LEV_Y_HIGH, (1, 2))):
        levels[k] = jnp.full((8, LANES), level[at_row[r], at_col[c]], I32)
    even = lax.rem(col, 2) == 0 if n_col % 2 == 0 else True
    levels[EVEN_SPAN] = jnp.full((8, LANES), jnp.where(even, 1, 0), I32)
    refined = levels[LEV_OWN] == 1
    for q in range(Q):
        s = jnp.full((8, LANES), rates[q], F32)
        s = jnp.where(refined, s, 1.0 / (2.0 / s - 0.5))
        coef[q] = 0.125 - 0.125 * s
        if q in EVEN:
            coef[Q + EVEN.index(q)] = (0.125 * gain_of(q)) * s
    shape = (2 * nzc, 2 * nz)
    i, l = iota(0, shape), iota(1, shape)
    half, l = l // nz, l % nz
    za = (l >> 1) + half * nzc
    zb = jnp.clip((l >> 1) + jnp.where((l & 1) == 1, 1, -1), 0, nzc - 1) + half * nzc
    refine[...] = (jnp.where(i == za, 0.75, 0.0) + jnp.where(i == zb, 0.25, 0.0)).astype(BF16)
    shape = (nz, nz)
    thin[...] = jnp.where((iota(0, shape) >> 1) == iota(1, shape), 0.125, 0.0).astype(BF16)
    arrive[0].wait()
    planes = []
    for k, y in enumerate((sy // 2 - 1, sy // 2)):
        v = jnp.zeros((8, LANES), I32)
        for x in (sx // 2 - 1, sx // 2):
            v = jnp.where(sub == x + 1, jnp.broadcast_to(obstacle[x, y : y + 1, :], (8, LANES)), v)
        flags[k] = v
        planes.append(v)
    both = jnp.maximum(planes[0], planes[1])
    both = jnp.maximum(both, roll_sub(both, -1))
    both = jnp.maximum(both, roll_lane(both, -1))
    both = jnp.take_along_axis(both, (2 * lane) & (LANES - 1), axis=1)
    both = jnp.broadcast_to(both[sx // 2 : sx // 2 + 1], (8, LANES))
    c_wall[...] = jnp.where((sub == 1 + cx // 2) & (lane < nzc), both, 0)
    arrive[1].wait()
    for Y in range(cy):
        for X in range(cx):
            c_wide[Y, X, 0:Q] = dot_exact(coarse[X, Y], refine[0:nzc, 0:nz])
    arrive[2].wait()


def fine_plane(fine, from_low, from_high, y, mixed=None):
    sx = fine.shape[0]
    base = X_FINE + 9 * y
    rows = [None] * Q
    for q0, n in OCTETS:
        cells = [fine[x, y, q0 : q0 + n] for x in range(sx)]
        low = high = cells[0]
        if q0 == 16:
            low = from_low[base - 2 : base + 6]
        if q0 == 24:
            low = from_low[base + 6 : base + 9]
        if q0 == 0:
            high = from_high[base : base + 8]
        if q0 == 8:
            high = row8(from_high, base + 8)
        if mixed is not None:
            if q0 >= 16:
                low = mixed(0, q0, n, low)
            else:
                high = mixed(1, q0, n, high)
        tile = jnp.swapaxes(jnp.stack([low, *cells, high]), 0, 1)
        for k in range(n):
            rows[q0 + k] = tile[k]
    return rows


def coarse_plane(tile_of):
    rows = [None] * Q
    for q0, n in OCTETS:
        tiles = [tile_of(I, q0, n) for I in range(5)]
        tile = jnp.swapaxes(jnp.stack(tiles + tiles[:3]), 0, 1)
        for k in range(n):
            rows[q0 + k] = tile[k]
    return rows


def pack_y_kernel(fine, coarse, from_low, from_high, levels, second, first, w_edge, up, down):
    sy, cy, nzc = fine.shape[1], coarse.shape[1], coarse.shape[3]
    low_half = iota(1, (Q, LANES)) < nzc
    own = levels[LEV_OWN] == 1
    for out, e, y, Y, qs, to in ((up, 1, sy - 1, cy - 1, HIGH_Y, LEV_Y_HIGH), (down, 0, 0, 0, LOW_Y, LEV_Y_LOW)):
        both = own & (levels[to] == 1)
        g_low, g_high = from_low[0:Q], from_high[0:Q]
        if e == 0:
            g_high = roll_lane(g_high, nzc)
        else:
            g_low = roll_lane(g_low, nzc)
        out[0:Q] = g_low
        out[0:Q, nzc : 2 * nzc] = coarse[0, Y]
        out[Y_SECOND : Y_SECOND + Q] = g_high
        out[Y_SECOND : Y_SECOND + Q, 0:nzc] = coarse[2, Y]
        out[Y_THIRD : Y_THIRD + 16, 0:nzc] = coarse[1, Y, 0:16]
        out[Y_THIRD : Y_THIRD + Q - 16, nzc : 2 * nzc] = coarse[1, Y, 16:Q]
        rows = fine_plane(fine, from_low, from_high, y)
        for q in range(Q):
            w_edge[q, e] = rows[q]
        for k in range(3):
            out[Y_CORNER + k : Y_CORNER + k + 1] = rows[qs[6 + k]][0:1]
            out[Y_CORNER + 3 + k : Y_CORNER + 4 + k] = rows[qs[k]][7:8]
        for k, q in enumerate(qs):
            at, n, s = fine_slot(k)
            out[at : at + n] = jnp.where(both[0:n], rows[q][s : s + n], out[at : at + n])
    even = levels[EVEN_SPAN] == 1
    for at in range(0, Y_ROWS, 8):
        a, b = up[at : at + 8], down[at : at + 8]
        first[at : at + 8] = jnp.where(even, a, b)
        second[at : at + 8] = jnp.where(even, b, a)


def forward(m0, m1, m2):
    pair = m0 + m2
    return pair + 4.0 * m1, m2 - m0, pair


ALONG_Y = [(9 * a + c, 3) for a in range(3) for c in range(3)]
ALONG_Z = [(9 * a + 3 * b, 1) for a in range(3) for b in range(3)]
ALONG_X = [(r, 9) for r in range(9)]


def collide(g, coef):
    t = [None] * Q
    for r in range(9):
        t[r], t[9 + r], t[18 + r] = forward(g[r], g[9 + r], g[18 + r])
    cols = [(t[c] + t[6 + c]) + 4.0 * t[3 + c] for c in range(3)]
    density = (cols[0] + cols[2]) + 4.0 * cols[1]
    inv = 1.0 / density
    rows = [(t[3 * b] + t[3 * b + 2]) + 4.0 * t[3 * b + 1] for b in (0, 2)]
    uy = (rows[1] - rows[0]) * inv
    uz = (cols[2] - cols[0]) * inv
    dcols = [(t[9 + c] + t[15 + c]) + 4.0 * t[12 + c] for c in range(3)]
    ux = ((dcols[0] + dcols[2]) + 4.0 * dcols[1]) * inv
    for r in range(9):
        t0, d, pair = t[r], t[9 + r], t[18 + r]
        t1 = d - ux * t0
        t[9 + r], t[18 + r] = t1, pair - ux * (d + t1)
    for u, lines in ((uy, ALONG_Y), (uz, ALONG_Z)):
        for at, by in lines:
            t0, d, pair = forward(t[at], t[at + by], t[at + 2 * by])
            t1 = d - u * t0
            t[at], t[at + by], t[at + 2 * by] = t0, t1, pair - u * (d + t1)
    for q in range(Q):
        t[q] = coef[q] * t[q]
        if q in EVEN:
            t[q] = t[q] + coef[Q + EVEN.index(q)] * density
    for u, lines in ((uz, ALONG_Z), (uy, ALONG_Y), (ux, ALONG_X)):
        for at, by in lines:
            t0, t1, t2 = t[at], t[at + by], t[at + 2 * by]
            d = t1 + u * t0
            s = t2 + u * (t1 + d)
            t[at], t[at + by], t[at + 2 * by] = s - d, 0.5 * (t0 - s), s + d
    return t


def pull(source, center, step_mask):
    out = []
    for q in range(Q):
        ex, ey, ez = STEP[q]
        v = roll_lane(roll_sub(source(q), ex), ez)
        mask = step_mask(ex, ey, ez)
        if mask is not None:
            v = jnp.where(mask, center(26 - q), v)
        out.append(v)
    return out


def bounce_mask(height, wall_of):
    lane = iota(1)
    edges = {1: lane == 0, -1: lane == height - 1}

    def mask_of(ex, ey, ez):
        m = None
        if (ex, ey, ez) == (0, 0, 0):
            return None
        wall = wall_of(ey)
        if wall is not None:
            m = roll_lane(roll_sub(wall, ex), ez) == 1
        if ez != 0:
            m = edges[ez] if m is None else m | edges[ez]
        return m

    return mask_of


def wall_plane(flags, y, first):
    def wall_of(ey):
        k = y - ey - first
        return flags[k] if k in (0, 1) else None

    return wall_of


def store_rows(rows, out, t, xs, width):
    for q0, n in OCTETS:
        tile = jnp.swapaxes(jnp.stack(rows[q0 : q0 + n]), 0, 1)
        for k, x in enumerate(xs):
            out[k, t, q0 : q0 + n] = tile[x][:, 0:width]


def coalesce(planes, out, at, thin):
    nzc = out.shape[3]
    for X in range(out.shape[0]):
        s = sum(p[2 * X] + p[2 * X + 1] for p in planes)
        out[X, at] = dot_exact(s, thin[...])[:, 0:nzc]


def coarse_step(plane, J, wall, coef, buf, at, nzc, cx, wall_row):
    mask_of = bounce_mask(nzc, lambda ey: wall if J - ey == wall_row else None)
    new = collide(pull(lambda q: plane(q, J - STEP[q][1]), lambda q: plane(q, J), mask_of), coef)
    if J == wall_row:
        stay = wall == 1
        new = [jnp.where(stay, plane(q, J), new[q]) for q in range(Q)]
    store_rows(new, buf, at, range(1, cx + 1), nzc)


def inner_kernel(fine, coarse, from_low, from_high, w_edge, levels, coef, flags, c_wall, c_wide, refine, thin,
                 out, c_out, w_in, ex_side, c_all, f_in, aux, ghost, ex_mid, c_buf, sems):
    sx, sy, nz = fine.shape[0], fine.shape[1], fine.shape[3]
    cx, cy, nzc = coarse.shape[0], coarse.shape[1], coarse.shape[3]
    mid = sy // 2
    own = jnp.max(levels[LEV_OWN])
    n = 8 * ((X_MIDDLE + 16 + 7) // 8)
    both = dot_exact(jnp.concatenate([from_low[0:n], from_high[0:n]], axis=0), refine[...])
    for side in range(2):
        v = both[side * n : side * n + n]
        ghost[side, 0, 0:Q] = v[0:Q, 0:nz]
        ghost[side, cy - 1, 0:Q] = v[0:Q, nz : 2 * nz]
        ghost[side, 1, 0:16] = v[X_MIDDLE : X_MIDDLE + 16, 0:nz]
        ghost[side, 1, 16:Q] = v[X_MIDDLE : X_MIDDLE + Q - 16, nz : 2 * nz]

    def wide(J, I):
        if I == 0:
            return ghost[0, J - 1]
        if I == cx + 1:
            return ghost[1, J - 1]
        return c_wide[J - 1, I - 1]

    for J in range(1, cy + 1):
        for i in range(sx + 2):
            a, b = pair_of(i)
            v = blend(wide(J, a), wide(J, b))
            if J == 2:
                ex_mid[i] = v
            else:
                ex_side[J // 2, i] = v

    def exploded(J, i):
        return ex_mid.at[i] if J == 2 else ex_side.at[J // 2, i]

    copies = [pltpu.make_async_copy(f_in.at[:, pl.ds(mid - 2, 2)], out.at[:, pl.ds(mid - 1, 2)], sems.at[0]),
              pltpu.make_async_copy(c_buf, c_out.at[:, pl.ds(cy // 2, 1)], sems.at[1]),
              pltpu.make_async_copy(f_in, out.at[:, pl.ds(1, sy - 2)], sems.at[0])]

    @pl.when(own == 1)
    def _():
        refined = (levels[LEV_X_LOW] == 1, levels[LEV_X_HIGH] == 1)
        sub = iota(0)
        for y in range(1, sy - 1):
            a, b = pair_of(y + 1)

            def mixed(side, q0, n, tile):
                i = 0 if side == 0 else sx + 1
                e = blend(exploded(a, i)[q0 : q0 + n], exploded(b, i)[q0 : q0 + n])
                return jnp.where(refined[side][0:n], tile, e)

            rows = fine_plane(fine, from_low, from_high, y, mixed)
            for q in range(Q):
                w_in[q, y - 1] = rows[q]

        def plane(q, y):
            if y in (0, sy - 1):
                return w_edge[q, 0 if y == 0 else 1]
            return w_in[q, y - 1]

        for y in (mid - 1, mid, 1, sy - 2):
            pulled = pull(lambda q: plane(q, y - STEP[q][1]), lambda q: plane(q, y),
                          bounce_mask(nz, wall_plane(flags, y, mid - 1)))
            if y in (1, sy - 2):
                for q in range(Q):
                    aux[q, 0 if y == 1 else 1] = jnp.where(sub == 0, roll_sub(pulled[q], -1), roll_sub(pulled[q], 1))
            new = collide(pulled, coef)
            if y in (mid - 1, mid):
                stay = flags[y - mid + 1] == 1
                new = [jnp.where(stay, w_in[q, y - 1], new[q]) for q in range(Q)]
            store_rows(new, f_in, y - 1, range(1, sx + 1), nz)
            if y == mid:
                copies[0].start()
                coalesce([f_in.at[:, mid - 2], f_in.at[:, mid - 1]], c_buf, 0, thin)
                copies[1].start()
        copies[0].wait()

    @pl.when(own != 1)
    def _():
        for y in range(1, sy - 1):
            a, b = pair_of(y + 1)
            for x in range(sx):
                f_in[x, y - 1] = blend(exploded(a, x + 1)[0:Q], exploded(b, x + 1)[0:Q])
        copies[2].start()

        def tile_of(Y):
            def tile(I, q0, n):
                if 1 <= I <= cx:
                    return coarse[I - 1, Y, q0 : q0 + n]
                msg = from_low if I == 0 else from_high
                if Y != 1:
                    v = msg[q0 : q0 + n]
                    return (v if Y == 0 else roll_lane(v, nzc))[:, 0:nzc]
                if q0 < 16:
                    return msg[X_MIDDLE + q0 : X_MIDDLE + q0 + n, 0:nzc]
                return roll_lane(msg[X_MIDDLE + q0 - 16 : X_MIDDLE + q0 - 16 + n], nzc)[:, 0:nzc]

            return tile

        for Y in range(cy):
            for q, v in enumerate(coarse_plane(tile_of(Y))):
                c_all[q, Y, :, 0:nzc] = v
        coarse_step(lambda q, J: c_all[q, J - 1], 2, c_wall[...], coef, c_buf, 0, nzc, cx, 2)
        copies[1].start()
        copies[2].wait()

    copies[1].wait()


def outer_kernel(second, first, w_edge, w_in, c_all, ex_side, f_in, aux, levels, coef, c_wall, refine, thin,
                 _out_in, _c_in, out, c_out, msgs, wide, ex_g, w_g, w_e, c_g, f_buf, f_fix, s_buf, c_buf, sems):
    sx, sy, nz = out.shape[0], out.shape[1], out.shape[3]
    cx, cy, nzc = c_out.shape[0], c_out.shape[1], c_out.shape[3]
    own = jnp.max(levels[LEV_OWN])
    sub = iota(0)
    even = levels[EVEN_SPAN] == 1
    for at in range(0, Y_ROWS, 8):
        a, b = first[at : at + 8], second[at : at + 8]
        msgs[at : at + 8] = jnp.where(even, b, a)
        msgs[Y_ROWS + at : Y_ROWS + at + 8] = jnp.where(even, a, b)
    v = dot_exact(msgs[...], refine[...])
    for e in range(2):
        at = Y_ROWS * e
        wide[0, 0:Q] = v[at : at + Q, 0:nz]
        wide[1, 0:Q] = v[at : at + Q, nz : 2 * nz]
        wide[3, 0:Q] = v[at + Y_SECOND : at + Y_SECOND + Q, 0:nz]
        wide[4, 0:Q] = v[at + Y_SECOND : at + Y_SECOND + Q, nz : 2 * nz]
        wide[2, 0:16] = v[at + Y_THIRD : at + Y_THIRD + 16, 0:nz]
        wide[2, 16:Q] = v[at + Y_THIRD : at + Y_THIRD + Q - 16, nz : 2 * nz]
        for i in range(sx + 2):
            a, b = pair_of(i)
            ex_g[e, i] = blend(wide[a], wide[b])

    def edge_copy(e):
        y = (sy - 1) * e
        return pltpu.make_async_copy(f_buf.at[:, pl.ds(e, 1)], out.at[:, pl.ds(y, 1)], sems.at[e])

    def coarse_copy(e):
        return pltpu.make_async_copy(c_buf.at[:, pl.ds(e, 1)], c_out.at[:, pl.ds((cy - 1) * e, 1)], sems.at[2 + e])

    @pl.when(own == 1)
    def _():
        ready = [pltpu.make_async_copy(f_in.at[pl.ds(1, sx - 2), pl.ds((sy - 3) * e, 1)],
                                       out.at[pl.ds(1, sx - 2), pl.ds(1 + (sy - 3) * e, 1)], sems.at[4 + e])
                 for e in range(2)]
        fixed = [[pltpu.make_async_copy(f_fix.at[pl.ds(side, 1), pl.ds(e, 1)],
                                        out.at[pl.ds((sx - 1) * side, 1), pl.ds(1 + (sy - 3) * e, 1)],
                                        sems.at[6 + 2 * e + side]) for side in range(2)] for e in range(2)]
        for c in ready:
            c.start()
        lane = iota(1)
        inside = {0: None, 1: lane != 0, -1: lane != nz - 1}
        for e in range(2):
            msg = msgs.at[pl.ds(Y_ROWS * e, Y_ROWS)]
            qs = HIGH_Y if e == 0 else LOW_Y
            far = levels[LEV_BELOW if e == 0 else LEV_ABOVE] == 1
            near = levels[LEV_Y_LOW if e == 0 else LEV_Y_HIGH] == 1
            for q0, n in OCTETS:
                tiles = [blend(ex_g[e, i, q0 : q0 + n], ex_side[e, i, q0 : q0 + n]) for i in range(sx + 2)]
                tile = jnp.swapaxes(jnp.stack(tiles), 0, 1)
                for k, q in enumerate(qs):
                    if q0 <= q < q0 + n:
                        at, _, s = fine_slot(k)
                        v = roll_sub(msg[at : at + 8], s)
                        if STEP[q][0] != 0:
                            corner = Y_CORNER + k % 3 + (0 if STEP[q][0] > 0 else 3)
                            v = jnp.where(near, v, row8(msg, corner))
                        w_g[k] = jnp.where(far, v, tile[q - q0])
            coarse_low = (levels[LEV_X_LOW] != 1) & (sub == 0)
            coarse_high = (levels[LEV_X_HIGH] != 1) & (sub == sx + 1)
            v_low = blend(ex_side[e, 0], ex_g[e, 0])
            v_high = blend(ex_side[e, sx + 1], ex_g[e, sx + 1])
            for q in range(Q):
                v = w_edge[q, e]
                if STEP[q][0] > 0:
                    v = jnp.where(coarse_low, jnp.broadcast_to(v_low[q : q + 1], (8, LANES)), v)
                if STEP[q][0] < 0:
                    v = jnp.where(coarse_high, jnp.broadcast_to(v_high[q : q + 1], (8, LANES)), v)
                w_e[q] = v

            def source(q):
                return (w_g[qs.index(q)] if q in qs else
                        w_e[q] if STEP[q][1] == 0 else w_in[q, (sy - 3) * e])

            pulled = pull(source, lambda q: w_e[q], bounce_mask(nz, lambda ey: None))
            spare = (sub == 0) | (sub == sx + 1)
            for q in range(Q):
                ex, _, ez = STEP[q]
                v = aux[q, e]
                if q in qs and ex != 0:
                    m = sub == (0 if ex > 0 else sx + 1)
                    if ez != 0:
                        m = m & inside[ez]
                    v = jnp.where(m, roll_lane(w_e[q], ez), v)
                pulled[q] = jnp.where(spare, v, pulled[q])
            new = collide(pulled, coef)
            for q0, n in OCTETS:
                tile = jnp.swapaxes(jnp.stack(new[q0 : q0 + n]), 0, 1)
                for x in range(sx):
                    f_buf[x, e, q0 : q0 + n] = tile[x + 1]
                f_fix[0, e, q0 : q0 + n] = tile[0]
                f_fix[1, e, q0 : q0 + n] = tile[sx + 1]
            edge_copy(e).start()
            for c in fixed[e]:
                c.start()

            def beside(x):
                if x in (0, sx - 1):
                    return f_fix[0 if x == 0 else 1, e]
                return f_in[x, (sy - 3) * e]

            for X in range(cx):
                at = QPAD * (cx * e + X)
                s_buf[at : at + Q] = ((f_buf[2 * X, e] + f_buf[2 * X + 1, e])
                                      + (beside(2 * X) + beside(2 * X + 1)))
        mean = dot_parts(s_buf[...], thin[...], 2)
        for e in range(2):
            for X in range(cx):
                at = QPAD * (cx * e + X)
                c_buf[X, e] = mean[at : at + Q, 0:nzc]
            coarse_copy(e).start()
        for c in ready + fixed[0] + fixed[1]:
            c.wait()

    @pl.when(own != 1)
    def _():
        wall = c_wall[...]

        for e in range(2):
            msg = msgs.at[pl.ds(Y_ROWS * e, Y_ROWS)]
            for x in range(sx):
                f_buf[x, e] = blend(ex_side[e, x + 1, 0:Q], ex_g[e, x + 1, 0:Q])
            edge_copy(e).start()

            def tile(I, q0, n):
                at = Y_SECOND if I >= 3 else 0
                if I == 2:
                    at = Y_THIRD - (16 if q0 >= 16 else 0)
                v = msg[at + q0 : at + q0 + n]
                if I in (1, 4) or (I == 2 and q0 >= 16):
                    v = roll_lane(v, nzc)
                return v[:, 0:nzc]

            for q, v in enumerate(coarse_plane(tile)):
                c_g[q, e, :, 0:nzc] = v

        def plane(q, J):
            if J == 0:
                return c_g[q, 0]
            if J == cy + 1:
                return c_g[q, 1]
            return c_all[q, J - 1]

        lower = sub < 4

        def joined(a, b, by):
            return jnp.where(lower, roll_sub(a, by), roll_sub(b, by + 4))

        lane = iota(1)
        edges = {1: lane == 0, -1: lane == nzc - 1}
        none = jnp.zeros((8, LANES), I32)
        center = [joined(plane(q, 1), plane(q, cy), 0) for q in range(Q)]
        pulled = []
        for q in range(Q):
            ex, ey, ez = STEP[q]
            if (ex, ey, ez) == (0, 0, 0):
                pulled.append(center[q])
                continue
            v = roll_lane(joined(plane(q, 1 - ey), plane(q, cy - ey), ex), ez)
            m = None
            if ey != 0:
                walls = (wall, none) if ey < 0 else (none, wall)
                m = roll_lane(joined(*walls, ex), ez) == 1
            if ez != 0:
                m = edges[ez] if m is None else m | edges[ez]
            pulled.append(v if m is None else jnp.where(m, center[26 - q], v))
        new = collide(pulled, coef)
        for q0, n in OCTETS:
            tile = jnp.swapaxes(jnp.stack(new[q0 : q0 + n]), 0, 1)
            for e in range(2):
                for X in range(cx):
                    c_buf[X, e, q0 : q0 + n] = tile[1 + X + 4 * e][:, 0:nzc]
        for e in range(2):
            coarse_copy(e).start()

    for e in range(2):
        edge_copy(e).wait()
        coarse_copy(e).wait()


def cost(flops, nbytes):
    return pl.CostEstimate(flops=flops, bytes_accessed=nbytes, transcendentals=0)


def in_hbm(x):
    return pltpu.with_memory_space_constraint(x, pltpu.HBM)


def local(fine_pops, coarse_pops, obstacle, block_level, relax_rates):
    fine = jnp.transpose(fine_pops, (1, 2, 0, 3))
    coarse = jnp.transpose(coarse_pops, (1, 2, 0, 3))
    sx, sy, _, nz = fine.shape
    cx, cy, _, nzc = coarse.shape

    x_message = struct((8 * ((X_FINE + 9 * sy + 7) // 8), LANES))
    up, down = pl.pallas_call(
        pack_x_kernel,
        out_shape=(x_message, x_message),
        in_specs=[ANY] * 3,
        out_specs=(VMEM, VMEM),
        scratch_shapes=[
            pltpu.VMEM((sy, 16, nz), F32),
            pltpu.VMEM((sy, Q - 16, nz), F32),
            pltpu.VMEM((cy, Q, nzc), F32),
            pltpu.VMEM((cy, Q, nzc), F32),
            pltpu.VMEM((2, 16, LANES), F32),
            pltpu.SMEM(block_level.shape, I32),
            pltpu.SemaphoreType.DMA((5,)),
        ],
        compiler_params=params(),
        name="pack_x",
    )(in_hbm(fine), in_hbm(coarse), in_hbm(block_level))
    from_low = lax.ppermute(up, "stream", ring("stream", 1))
    from_high = lax.ppermute(down, "stream", ring("stream", -1))

    fine_shape, coarse_shape = struct(fine.shape), struct(coarse.shape)
    levels, coef, flags, c_wall, c_wide, refine, thin, fine, coarse = pl.pallas_call(
        tables_kernel,
        out_shape=(
            struct((9, 8, LANES), I32),
            struct((Q + len(EVEN), 8, LANES)),
            struct((2, 8, LANES), I32),
            struct((8, LANES), I32),
            struct((cy, cx, QPAD, nz)),
            struct((2 * nzc, 2 * nz), BF16),
            struct((nz, nz), BF16),
            fine_shape,
            coarse_shape,
        ),
        in_specs=[ANY] * 3 + [SMEM] * 2,
        out_specs=(VMEM,) * 9,
        scratch_shapes=[pltpu.VMEM(obstacle.shape, I32), pltpu.SemaphoreType.DMA((3,))],
        compiler_params=params(),
        cost_estimate=cost(10_000_000, 1_000_000),
        name="tables",
    )(in_hbm(fine), in_hbm(coarse), in_hbm(obstacle), block_level, relax_rates)

    y_message = struct((Y_ROWS, LANES))
    second, first, w_edge = pl.pallas_call(
        pack_y_kernel,
        out_shape=(y_message, y_message, struct((Q, 2, 8, LANES))),
        in_specs=[VMEM] * 5,
        out_specs=(VMEM,) * 3,
        scratch_shapes=[pltpu.VMEM(y_message.shape, F32)] * 2,
        compiler_params=params(),
        name="pack_y",
    )(fine, coarse, from_low, from_high, levels)
    if lax.axis_size("span") % 2 == 0:
        second = lax.ppermute(second, "span", pairs("span", 1))
        first = lax.ppermute(first, "span", pairs("span", 0))
    else:
        second, first = (lax.ppermute(first, "span", ring("span", 1)),
                         lax.ppermute(second, "span", ring("span", -1)))

    out, c_out, w_in, ex_side, c_all, f_in, aux = pl.pallas_call(
        inner_kernel,
        out_shape=(
            fine_shape,
            coarse_shape,
            struct((Q, sy - 2, 8, LANES)),
            struct((2, sx + 2, QPAD, nz)),
            struct((Q, cy, 8, LANES)),
            struct((sx, sy - 2, Q, nz)),
            struct((Q, 2, 8, LANES)),
        ),
        in_specs=[VMEM] * 12,
        out_specs=(ANY, ANY) + (VMEM,) * 5,
        scratch_shapes=[
            pltpu.VMEM((2, cy, QPAD, nz), F32),
            pltpu.VMEM((sx + 2, QPAD, nz), F32),
            pltpu.VMEM((cx, 1, Q, nzc), F32),
            pltpu.SemaphoreType.DMA((2,)),
        ],
        compiler_params=params(),
        cost_estimate=cost(20_000_000, 1_000_000),
        name="inner",
    )(fine, coarse, from_low, from_high, w_edge, levels, coef, flags, c_wall, c_wide, refine, thin)

    out, c_out = pl.pallas_call(
        outer_kernel,
        out_shape=(fine_shape, coarse_shape),
        in_specs=[VMEM] * 13 + [ANY, ANY],
        out_specs=(ANY, ANY),
        scratch_shapes=[
            pltpu.VMEM((2 * Y_ROWS, LANES), F32),
            pltpu.VMEM((5, QPAD, nz), F32),
            pltpu.VMEM((2, sx + 2, QPAD, nz), F32),
            pltpu.VMEM((9, 8, LANES), F32),
            pltpu.VMEM((Q, 8, LANES), F32),
            pltpu.VMEM((Q, 2, 8, LANES), F32),
            pltpu.VMEM((sx, 2, Q, nz), F32),
            pltpu.VMEM((2, 2, Q, nz), F32),
            pltpu.VMEM((2 * QPAD * cx, nz), F32),
            pltpu.VMEM((cx, 2, Q, nzc), F32),
            pltpu.SemaphoreType.DMA((10,)),
        ],
        input_output_aliases={13: 0, 14: 1},
        compiler_params=params(),
        name="outer",
    )(second, first, w_edge, w_in, c_all, ex_side, f_in, aux, levels, coef, c_wall, refine, thin,
      out, c_out)
    return jnp.transpose(out, (2, 0, 1, 3)), jnp.transpose(c_out, (2, 0, 1, 3))


def solution(mesh):
    placed = (
        P(None, "stream", "span", None),
        P(None, "stream", "span", None),
        P("stream", "span", None),
        P(),
        P(),
    )
    return jax.shard_map(
        local,
        mesh=mesh,
        in_specs=placed,
        out_specs=(P(None, "stream", "span", None), P(None, "stream", "span", None)),
        check_vma=False,
    )
```

```python
import jax
import jax.numpy as jnp
from jax import lax
from jax.experimental import pallas as pl
from jax.experimental.pallas import tpu as pltpu
from jax.sharding import PartitionSpec as P

F32 = jnp.float32
I32 = jnp.int32
BF16 = jnp.bfloat16
Q = 27
QPAD = 32
LANES = 128
OCTETS = [(8 * o, min(8, Q - 8 * o)) for o in range(4)]
STEP = [(q // 9 - 1, q // 3 % 3 - 1, q % 3 - 1) for q in range(Q)]
HIGH_X = [q for q in range(Q) if STEP[q][0] == 1]
LOW_X = [q for q in range(Q) if STEP[q][0] == -1]
HIGH_Y = [q for q in range(Q) if STEP[q][1] == 1]
LOW_Y = [q for q in range(Q) if STEP[q][1] == -1]
EVEN = [9 * a + 3 * b + c for a in (0, 2) for b in (0, 2) for c in (0, 2)]

VMEM = pl.BlockSpec(memory_space=pltpu.VMEM)
SMEM = pl.BlockSpec(memory_space=pltpu.SMEM)
ANY = pl.BlockSpec(memory_space=pl.ANY)
LIMIT = 16 << 20

LEV_BELOW, LEV_ROW, LEV_ABOVE = 0, 1, 2
LEV_X_LOW, LEV_X_HIGH, LEV_OWN, LEV_Y_LOW, LEV_Y_HIGH, EVEN_SPAN = 3, 4, 5, 6, 7, 8

X_FINE, X_MIDDLE = Q, Q + 9
SPARE = (3, 24)
Y_SECOND, Y_THIRD, Y_CORNER = Q, 2 * Q, 2 * Q + 16
Y_ROWS = 80


def fine_slot(k):
    ex = k // 3 - 1
    if ex == 0:
        return 6 * (k % 3), 6, 1
    return 36 + 7 * (k % 3 if ex < 0 else 3 + k % 3), 7, (1 if ex < 0 else 0)


def params(**more):
    return pltpu.CompilerParams(vmem_limit_bytes=LIMIT, **more)


def struct(shape, dtype=F32):
    return jax.ShapeDtypeStruct(shape, dtype)


def ring(axis, by):
    peers = lax.axis_size(axis)
    return [(i, (i + by) % peers) for i in range(peers)]


def pairs(axis, odd):
    peers = lax.axis_size(axis)
    return [(i, (i + (1 if i % 2 == odd else -1)) % peers) for i in range(peers)]


def roll_lane(v, by):
    return v if by == 0 else pltpu.roll(v, by % v.shape[1], 1)


def roll_sub(v, by):
    return v if by == 0 else pltpu.roll(v, by % v.shape[0], 0)


def iota(axis, shape=(8, LANES)):
    return lax.broadcasted_iota(I32, shape, axis)


def row8(ref, at):
    return jnp.broadcast_to(ref[at : at + 1], (8, LANES))


def dot_parts(x, m, count):
    parts = []
    for _ in range(count):
        parts.append(x.astype(BF16))
        x = x - parts[-1].astype(F32)
    return sum(jnp.dot(p, m, preferred_element_type=F32) for p in reversed(parts))


def dot_exact(x, m):
    return dot_parts(x, m, 3)


def pair_of(i):
    a = (i + 1) >> 1
    return a, a + (1 if (i + 1) & 1 else -1)


def blend(a, b):
    return 0.75 * a + 0.25 * b


def pack_x_kernel(fine, coarse, level, up, down, f_low, f_high, c_low, c_high, middle, lev, sems):
    sx, sy, cx = fine.shape[0], fine.shape[1], coarse.shape[0]
    fetch_level = pltpu.make_async_copy(level, lev, sems.at[4])
    copies = [
        pltpu.make_async_copy(fine.at[sx - 1, :, pl.ds(16, Q - 16)], f_high, sems.at[0]),
        pltpu.make_async_copy(coarse.at[cx - 1], c_high, sems.at[1]),
        pltpu.make_async_copy(fine.at[0, :, pl.ds(0, 16)], f_low, sems.at[2]),
        pltpu.make_async_copy(coarse.at[0], c_low, sems.at[3]),
    ]
    fetch_level.start()
    for c in copies:
        c.start()
    for c in copies:
        c.wait()
    cy, nzc = c_low.shape[0], c_low.shape[2]
    for k, (out, f, c, q0) in enumerate(((up, f_high, c_high, HIGH_X[0] - 16), (down, f_low, c_low, LOW_X[0]))):
        middle[k, 0:16, 0:nzc] = c[1, 0:16]
        middle[k, 0 : Q - 16, nzc : 2 * nzc] = c[1, 16:Q]
        out[0:Q, 0:nzc] = c[0]
        out[0:Q, nzc : 2 * nzc] = c[cy - 1]
        middle[k, 16:17] = f[sy - 1, q0 + 8 : q0 + 9]
        for y in range(sy):
            n = 9 if y < sy - 1 else 8
            out[X_FINE + 9 * y : X_FINE + 9 * y + n] = f[y, q0 : q0 + n]
    fetch_level.wait()
    n_row, n_col = lev.shape
    row, col = lax.axis_index("stream"), lax.axis_index("span")
    high_half = iota(1, (2, LANES)) >= nzc
    for k, (out, to) in enumerate(((up, row + 1), (down, row + n_row - 1))):
        both = lev[row, col] * lev[lax.rem(to, n_row), col]
        on = both * lev[lax.rem(to, n_row), lax.rem(col + 1, n_col)]
        at = slice(X_MIDDLE, X_MIDDLE + 17)
        out[at] = jnp.where(jnp.full((17, LANES), both, I32) == 1, out[at], middle[k])
        last = middle[k, 16:17]
        at = slice(SPARE[k], SPARE[k] + 2)
        spare = jnp.concatenate([roll_lane(last, nzc), last], axis=0)
        out[at] = jnp.where(high_half & (jnp.full((2, LANES), on, I32) == 1), spare, out[at])


def gain_of(q):
    return (1.0 if q // 9 == 0 else 1.0 / 3.0) * (1.0 if q // 3 % 3 == 0 else 1.0 / 3.0) * (
        1.0 if q % 3 == 0 else 1.0 / 3.0)


def tables_kernel(fine_far, coarse_far, obstacle_far, level, rates,
                  levels, coef, flags, c_wall, c_wide, refine, thin, fine, coarse, obstacle, sems):
    arrive = [pltpu.make_async_copy(a, b, sems.at[k]) for k, (a, b) in enumerate(
        ((obstacle_far, obstacle), (coarse_far, coarse), (fine_far, fine)))]
    for c in arrive:
        c.start()
    cx, cy, nzc = coarse.shape[0], coarse.shape[1], coarse.shape[3]
    sx, sy, nz = obstacle.shape
    row, col = lax.axis_index("stream"), lax.axis_index("span")
    n_row, n_col = level.shape
    at_row = [lax.rem(row + n_row - 1, n_row), row, lax.rem(row + 1, n_row)]
    at_col = [lax.rem(col + n_col - 1, n_col), col, lax.rem(col + 1, n_col)]
    lane, sub = iota(1), iota(0)
    for k in range(3):
        levels[k] = jnp.where(sub == 0, level[at_row[0], at_col[k]],
                              jnp.where(sub == sx + 1, level[at_row[2], at_col[k]], level[at_row[1], at_col[k]]))
    for k, (r, c) in ((LEV_X_LOW, (0, 1)), (LEV_X_HIGH, (2, 1)), (LEV_OWN, (1, 1)), (LEV_Y_LOW, (1, 0)),
                      (LEV_Y_HIGH, (1, 2))):
        levels[k] = jnp.full((8, LANES), level[at_row[r], at_col[c]], I32)
    even = lax.rem(col, 2) == 0 if n_col % 2 == 0 else True
    levels[EVEN_SPAN] = jnp.full((8, LANES), jnp.where(even, 1, 0), I32)
    refined = levels[LEV_OWN] == 1
    for q in range(Q):
        s = jnp.full((8, LANES), rates[q], F32)
        s = jnp.where(refined, s, 1.0 / (2.0 / s - 0.5))
        coef[q] = 0.125 - 0.125 * s
        if q in EVEN:
            coef[Q + EVEN.index(q)] = (0.125 * gain_of(q)) * s
    shape = (2 * nzc, 2 * nz)
    i, l = iota(0, shape), iota(1, shape)
    half, l = l // nz, l % nz
    za = (l >> 1) + half * nzc
    zb = jnp.clip((l >> 1) + jnp.where((l & 1) == 1, 1, -1), 0, nzc - 1) + half * nzc
    refine[...] = (jnp.where(i == za, 0.75, 0.0) + jnp.where(i == zb, 0.25, 0.0)).astype(BF16)
    shape = (nz, nz)
    thin[...] = jnp.where((iota(0, shape) >> 1) == iota(1, shape), 0.125, 0.0).astype(BF16)
    arrive[0].wait()
    planes = []
    for k, y in enumerate((sy // 2 - 1, sy // 2)):
        v = jnp.zeros((8, LANES), I32)
        for x in (sx // 2 - 1, sx // 2):
            v = jnp.where(sub == x + 1, jnp.broadcast_to(obstacle[x, y : y + 1, :], (8, LANES)), v)
        flags[k] = v
        planes.append(v)
    both = jnp.maximum(planes[0], planes[1])
    both = jnp.maximum(both, roll_sub(both, -1))
    both = jnp.maximum(both, roll_lane(both, -1))
    both = jnp.take_along_axis(both, (2 * lane) & (LANES - 1), axis=1)
    both = jnp.broadcast_to(both[sx // 2 : sx // 2 + 1], (8, LANES))
    c_wall[...] = jnp.where((sub == 1 + cx // 2) & (lane < nzc), both, 0)
    arrive[1].wait()
    for Y in range(cy):
        for X in range(cx):
            c_wide[Y, X, 0:Q] = dot_exact(coarse[X, Y], refine[0:nzc, 0:nz])
    arrive[2].wait()


def fine_plane(fine, from_low, from_high, y, mixed=None, last=None):
    sx = fine.shape[0]
    base = X_FINE + 9 * y
    rows = [None] * Q
    for q0, n in OCTETS:
        cells = [fine[x, y, q0 : q0 + n] for x in range(sx)]
        low = high = cells[0]
        if q0 == 16:
            low = from_low[base - 2 : base + 6]
        if q0 == 24:
            low = from_low[base + 6 : base + 9] if last is None else jnp.concatenate([from_low[base + 6 : base + 8], last[0]], axis=0)
        if q0 == 0:
            high = from_high[base : base + 8]
        if q0 == 8:
            high = row8(from_high, base + 8) if last is None else jnp.broadcast_to(last[1], (8, LANES))
        if mixed is not None:
            if q0 >= 16:
                low = mixed(0, q0, n, low)
            else:
                high = mixed(1, q0, n, high)
        tile = jnp.swapaxes(jnp.stack([low, *cells, high]), 0, 1)
        for k in range(n):
            rows[q0 + k] = tile[k]
    return rows


def coarse_plane(tile_of):
    rows = [None] * Q
    for q0, n in OCTETS:
        tiles = [tile_of(I, q0, n) for I in range(5)]
        tile = jnp.swapaxes(jnp.stack(tiles + tiles[:3]), 0, 1)
        for k in range(n):
            rows[q0 + k] = tile[k]
    return rows


def pack_y_kernel(fine, coarse, from_low, from_high, levels, second, first, w_edge, up, down):
    sy, cy, nzc = fine.shape[1], coarse.shape[1], coarse.shape[3]
    low_half = iota(1, (Q, LANES)) < nzc
    own = levels[LEV_OWN] == 1
    for out, e, y, Y, qs, to in ((up, 1, sy - 1, cy - 1, HIGH_Y, LEV_Y_HIGH), (down, 0, 0, 0, LOW_Y, LEV_Y_LOW)):
        both = own & (levels[to] == 1)
        g_low, g_high = from_low[0:Q], from_high[0:Q]
        if e == 0:
            g_high = roll_lane(g_high, nzc)
        else:
            g_low = roll_lane(g_low, nzc)
        out[0:Q] = g_low
        out[0:Q, nzc : 2 * nzc] = coarse[0, Y]
        out[Y_SECOND : Y_SECOND + Q] = g_high
        out[Y_SECOND : Y_SECOND + Q, 0:nzc] = coarse[2, Y]
        out[Y_THIRD : Y_THIRD + 16, 0:nzc] = coarse[1, Y, 0:16]
        out[Y_THIRD : Y_THIRD + Q - 16, nzc : 2 * nzc] = coarse[1, Y, 16:Q]
        last = None
        if e == 1:
            last = []
            for side, msg, near in ((0, from_low, LEV_X_LOW), (1, from_high, LEV_X_HIGH)):
                at = SPARE[side]
                halves = jnp.where(low_half[0:1], roll_lane(msg[at : at + 1], nzc), msg[at + 1 : at + 2])
                packed = (levels[LEV_OWN] * levels[near])[0:1] == 1
                last.append(jnp.where(packed, halves, msg[X_MIDDLE + 16 : X_MIDDLE + 17]))
        rows = fine_plane(fine, from_low, from_high, y, last=last)
        for q in range(Q):
            w_edge[q, e] = rows[q]
        for k in range(3):
            out[Y_CORNER + k : Y_CORNER + k + 1] = rows[qs[6 + k]][0:1]
            out[Y_CORNER + 3 + k : Y_CORNER + 4 + k] = rows[qs[k]][7:8]
        for k, q in enumerate(qs):
            at, n, s = fine_slot(k)
            out[at : at + n] = jnp.where(both[0:n], rows[q][s : s + n], out[at : at + n])
    even = levels[EVEN_SPAN] == 1
    for at in range(0, Y_ROWS, 8):
        a, b = up[at : at + 8], down[at : at + 8]
        first[at : at + 8] = jnp.where(even, a, b)
        second[at : at + 8] = jnp.where(even, b, a)


def forward(m0, m1, m2):
    pair = m0 + m2
    return pair + 4.0 * m1, m2 - m0, pair


ALONG_Y = [(9 * a + c, 3) for a in range(3) for c in range(3)]
ALONG_Z = [(9 * a + 3 * b, 1) for a in range(3) for b in range(3)]
ALONG_X = [(r, 9) for r in range(9)]


def collide(g, coef):
    t = [None] * Q
    for r in range(9):
        t[r], t[9 + r], t[18 + r] = forward(g[r], g[9 + r], g[18 + r])
    cols = [(t[c] + t[6 + c]) + 4.0 * t[3 + c] for c in range(3)]
    density = (cols[0] + cols[2]) + 4.0 * cols[1]
    inv = 1.0 / density
    rows = [(t[3 * b] + t[3 * b + 2]) + 4.0 * t[3 * b + 1] for b in (0, 2)]
    uy = (rows[1] - rows[0]) * inv
    uz = (cols[2] - cols[0]) * inv
    dcols = [(t[9 + c] + t[15 + c]) + 4.0 * t[12 + c] for c in range(3)]
    ux = ((dcols[0] + dcols[2]) + 4.0 * dcols[1]) * inv
    for r in range(9):
        t0, d, pair = t[r], t[9 + r], t[18 + r]
        t1 = d - ux * t0
        t[9 + r], t[18 + r] = t1, pair - ux * (d + t1)
    for u, lines in ((uy, ALONG_Y), (uz, ALONG_Z)):
        for at, by in lines:
            t0, d, pair = forward(t[at], t[at + by], t[at + 2 * by])
            t1 = d - u * t0
            t[at], t[at + by], t[at + 2 * by] = t0, t1, pair - u * (d + t1)
    for q in range(Q):
        t[q] = coef[q] * t[q]
        if q in EVEN:
            t[q] = t[q] + coef[Q + EVEN.index(q)] * density
    for u, lines in ((uz, ALONG_Z), (uy, ALONG_Y), (ux, ALONG_X)):
        for at, by in lines:
            t0, t1, t2 = t[at], t[at + by], t[at + 2 * by]
            d = t1 + u * t0
            s = t2 + u * (t1 + d)
            t[at], t[at + by], t[at + 2 * by] = s - d, 0.5 * (t0 - s), s + d
    return t


def pull(source, center, step_mask):
    out = []
    for q in range(Q):
        ex, ey, ez = STEP[q]
        v = roll_lane(roll_sub(source(q), ex), ez)
        mask = step_mask(ex, ey, ez)
        if mask is not None:
            v = jnp.where(mask, center(26 - q), v)
        out.append(v)
    return out


def bounce_mask(height, wall_of):
    lane = iota(1)
    edges = {1: lane == 0, -1: lane == height - 1}

    def mask_of(ex, ey, ez):
        m = None
        if (ex, ey, ez) == (0, 0, 0):
            return None
        wall = wall_of(ey)
        if wall is not None:
            m = roll_lane(roll_sub(wall, ex), ez) == 1
        if ez != 0:
            m = edges[ez] if m is None else m | edges[ez]
        return m

    return mask_of


def wall_plane(flags, y, first):
    def wall_of(ey):
        k = y - ey - first
        return flags[k] if k in (0, 1) else None

    return wall_of


def store_rows(rows, out, t, xs, width):
    for q0, n in OCTETS:
        tile = jnp.swapaxes(jnp.stack(rows[q0 : q0 + n]), 0, 1)
        for k, x in enumerate(xs):
            out[k, t, q0 : q0 + n] = tile[x][:, 0:width]


def coalesce(planes, out, at, thin):
    nzc = out.shape[3]
    for X in range(out.shape[0]):
        s = sum(p[2 * X] + p[2 * X + 1] for p in planes)
        out[X, at] = dot_exact(s, thin[...])[:, 0:nzc]


def coarse_step(plane, J, wall, coef, buf, at, nzc, cx, wall_row):
    mask_of = bounce_mask(nzc, lambda ey: wall if J - ey == wall_row else None)
    new = collide(pull(lambda q: plane(q, J - STEP[q][1]), lambda q: plane(q, J), mask_of), coef)
    if J == wall_row:
        stay = wall == 1
        new = [jnp.where(stay, plane(q, J), new[q]) for q in range(Q)]
    store_rows(new, buf, at, range(1, cx + 1), nzc)


def inner_kernel(fine, coarse, from_low, from_high, w_edge, levels, coef, flags, c_wall, c_wide, refine, thin,
                 out, c_out, w_in, ex_side, c_all, f_in, aux, ghost, ex_mid, c_buf, sems):
    sx, sy, nz = fine.shape[0], fine.shape[1], fine.shape[3]
    cx, cy, nzc = coarse.shape[0], coarse.shape[1], coarse.shape[3]
    mid = sy // 2
    own = jnp.max(levels[LEV_OWN])
    n = 8 * ((X_MIDDLE + 16 + 7) // 8)
    both = dot_exact(jnp.concatenate([from_low[0:n], from_high[0:n]], axis=0), refine[...])
    for side in range(2):
        v = both[side * n : side * n + n]
        ghost[side, 0, 0:Q] = v[0:Q, 0:nz]
        ghost[side, cy - 1, 0:Q] = v[0:Q, nz : 2 * nz]
        ghost[side, 1, 0:16] = v[X_MIDDLE : X_MIDDLE + 16, 0:nz]
        ghost[side, 1, 16:Q] = v[X_MIDDLE : X_MIDDLE + Q - 16, nz : 2 * nz]

    def wide(J, I):
        if I == 0:
            return ghost[0, J - 1]
        if I == cx + 1:
            return ghost[1, J - 1]
        return c_wide[J - 1, I - 1]

    for J in range(1, cy + 1):
        for i in range(sx + 2):
            a, b = pair_of(i)
            v = blend(wide(J, a), wide(J, b))
            if J == 2:
                ex_mid[i] = v
            else:
                ex_side[J // 2, i] = v

    def exploded(J, i):
        return ex_mid.at[i] if J == 2 else ex_side.at[J // 2, i]

    copies = [pltpu.make_async_copy(f_in.at[:, pl.ds(mid - 2, 2)], out.at[:, pl.ds(mid - 1, 2)], sems.at[0]),
              pltpu.make_async_copy(c_buf, c_out.at[:, pl.ds(cy // 2, 1)], sems.at[1]),
              pltpu.make_async_copy(f_in, out.at[:, pl.ds(1, sy - 2)], sems.at[0])]

    @pl.when(own == 1)
    def _():
        refined = (levels[LEV_X_LOW] == 1, levels[LEV_X_HIGH] == 1)
        sub = iota(0)
        for y in range(1, sy - 1):
            a, b = pair_of(y + 1)

            def mixed(side, q0, n, tile):
                i = 0 if side == 0 else sx + 1
                e = blend(exploded(a, i)[q0 : q0 + n], exploded(b, i)[q0 : q0 + n])
                return jnp.where(refined[side][0:n], tile, e)

            rows = fine_plane(fine, from_low, from_high, y, mixed)
            for q in range(Q):
                w_in[q, y - 1] = rows[q]

        def plane(q, y):
            if y in (0, sy - 1):
                return w_edge[q, 0 if y == 0 else 1]
            return w_in[q, y - 1]

        for y in (mid - 1, mid, 1, sy - 2):
            pulled = pull(lambda q: plane(q, y - STEP[q][1]), lambda q: plane(q, y),
                          bounce_mask(nz, wall_plane(flags, y, mid - 1)))
            if y in (1, sy - 2):
                for q in range(Q):
                    aux[q, 0 if y == 1 else 1] = jnp.where(sub == 0, roll_sub(pulled[q], -1), roll_sub(pulled[q], 1))
            new = collide(pulled, coef)
            if y in (mid - 1, mid):
                stay = flags[y - mid + 1] == 1
                new = [jnp.where(stay, w_in[q, y - 1], new[q]) for q in range(Q)]
            store_rows(new, f_in, y - 1, range(1, sx + 1), nz)
            if y == mid:
                copies[0].start()
                coalesce([f_in.at[:, mid - 2], f_in.at[:, mid - 1]], c_buf, 0, thin)
                copies[1].start()
        copies[0].wait()

    @pl.when(own != 1)
    def _():
        for y in range(1, sy - 1):
            a, b = pair_of(y + 1)
            for x in range(sx):
                f_in[x, y - 1] = blend(exploded(a, x + 1)[0:Q], exploded(b, x + 1)[0:Q])
        copies[2].start()

        def tile_of(Y):
            def tile(I, q0, n):
                if 1 <= I <= cx:
                    return coarse[I - 1, Y, q0 : q0 + n]
                msg = from_low if I == 0 else from_high
                if Y != 1:
                    v = msg[q0 : q0 + n]
                    return (v if Y == 0 else roll_lane(v, nzc))[:, 0:nzc]
                if q0 < 16:
                    return msg[X_MIDDLE + q0 : X_MIDDLE + q0 + n, 0:nzc]
                return roll_lane(msg[X_MIDDLE + q0 - 16 : X_MIDDLE + q0 - 16 + n], nzc)[:, 0:nzc]

            return tile

        for Y in range(cy):
            for q, v in enumerate(coarse_plane(tile_of(Y))):
                c_all[q, Y, :, 0:nzc] = v
        coarse_step(lambda q, J: c_all[q, J - 1], 2, c_wall[...], coef, c_buf, 0, nzc, cx, 2)
        copies[1].start()
        copies[2].wait()

    copies[1].wait()


def outer_kernel(second, first, w_edge, w_in, c_all, ex_side, f_in, aux, levels, coef, c_wall, refine, thin,
                 _out_in, _c_in, out, c_out, msgs, wide, ex_g, w_g, w_e, c_g, f_buf, f_fix, s_buf, c_buf, sems):
    sx, sy, nz = out.shape[0], out.shape[1], out.shape[3]
    cx, cy, nzc = c_out.shape[0], c_out.shape[1], c_out.shape[3]
    own = jnp.max(levels[LEV_OWN])
    sub = iota(0)
    even = levels[EVEN_SPAN] == 1
    for at in range(0, Y_ROWS, 8):
        a, b = first[at : at + 8], second[at : at + 8]
        msgs[at : at + 8] = jnp.where(even, b, a)
        msgs[Y_ROWS + at : Y_ROWS + at + 8] = jnp.where(even, a, b)
    v = dot_exact(msgs[...], refine[...])
    for e in range(2):
        at = Y_ROWS * e
        wide[0, 0:Q] = v[at : at + Q, 0:nz]
        wide[1, 0:Q] = v[at : at + Q, nz : 2 * nz]
        wide[3, 0:Q] = v[at + Y_SECOND : at + Y_SECOND + Q, 0:nz]
        wide[4, 0:Q] = v[at + Y_SECOND : at + Y_SECOND + Q, nz : 2 * nz]
        wide[2, 0:16] = v[at + Y_THIRD : at + Y_THIRD + 16, 0:nz]
        wide[2, 16:Q] = v[at + Y_THIRD : at + Y_THIRD + Q - 16, nz : 2 * nz]
        for i in range(sx + 2):
            a, b = pair_of(i)
            ex_g[e, i] = blend(wide[a], wide[b])

    def edge_copy(e):
        y = (sy - 1) * e
        return pltpu.make_async_copy(f_buf.at[:, pl.ds(e, 1)], out.at[:, pl.ds(y, 1)], sems.at[e])

    def coarse_copy(e):
        return pltpu.make_async_copy(c_buf.at[:, pl.ds(e, 1)], c_out.at[:, pl.ds((cy - 1) * e, 1)], sems.at[2 + e])

    @pl.when(own == 1)
    def _():
        ready = [pltpu.make_async_copy(f_in.at[pl.ds(1, sx - 2), pl.ds((sy - 3) * e, 1)],
                                       out.at[pl.ds(1, sx - 2), pl.ds(1 + (sy - 3) * e, 1)], sems.at[4 + e])
                 for e in range(2)]
        fixed = [[pltpu.make_async_copy(f_fix.at[pl.ds(side, 1), pl.ds(e, 1)],
                                        out.at[pl.ds((sx - 1) * side, 1), pl.ds(1 + (sy - 3) * e, 1)],
                                        sems.at[6 + 2 * e + side]) for side in range(2)] for e in range(2)]
        for c in ready:
            c.start()
        lane = iota(1)
        inside = {0: None, 1: lane != 0, -1: lane != nz - 1}
        for e in range(2):
            msg = msgs.at[pl.ds(Y_ROWS * e, Y_ROWS)]
            qs = HIGH_Y if e == 0 else LOW_Y
            far = levels[LEV_BELOW if e == 0 else LEV_ABOVE] == 1
            near = levels[LEV_Y_LOW if e == 0 else LEV_Y_HIGH] == 1
            for q0, n in OCTETS:
                tiles = [blend(ex_g[e, i, q0 : q0 + n], ex_side[e, i, q0 : q0 + n]) for i in range(sx + 2)]
                tile = jnp.swapaxes(jnp.stack(tiles), 0, 1)
                for k, q in enumerate(qs):
                    if q0 <= q < q0 + n:
                        at, _, s = fine_slot(k)
                        v = roll_sub(msg[at : at + 8], s)
                        if STEP[q][0] != 0:
                            corner = Y_CORNER + k % 3 + (0 if STEP[q][0] > 0 else 3)
                            v = jnp.where(near, v, row8(msg, corner))
                        w_g[k] = jnp.where(far, v, tile[q - q0])
            coarse_low = (levels[LEV_X_LOW] != 1) & (sub == 0)
            coarse_high = (levels[LEV_X_HIGH] != 1) & (sub == sx + 1)
            v_low = blend(ex_side[e, 0], ex_g[e, 0])
            v_high = blend(ex_side[e, sx + 1], ex_g[e, sx + 1])
            for q in range(Q):
                v = w_edge[q, e]
                if STEP[q][0] > 0:
                    v = jnp.where(coarse_low, jnp.broadcast_to(v_low[q : q + 1], (8, LANES)), v)
                if STEP[q][0] < 0:
                    v = jnp.where(coarse_high, jnp.broadcast_to(v_high[q : q + 1], (8, LANES)), v)
                w_e[q] = v

            def source(q):
                return (w_g[qs.index(q)] if q in qs else
                        w_e[q] if STEP[q][1] == 0 else w_in[q, (sy - 3) * e])

            pulled = pull(source, lambda q: w_e[q], bounce_mask(nz, lambda ey: None))
            spare = (sub == 0) | (sub == sx + 1)
            for q in range(Q):
                ex, _, ez = STEP[q]
                v = aux[q, e]
                if q in qs and ex != 0:
                    m = sub == (0 if ex > 0 else sx + 1)
                    if ez != 0:
                        m = m & inside[ez]
                    v = jnp.where(m, roll_lane(w_e[q], ez), v)
                pulled[q] = jnp.where(spare, v, pulled[q])
            new = collide(pulled, coef)
            for q0, n in OCTETS:
                tile = jnp.swapaxes(jnp.stack(new[q0 : q0 + n]), 0, 1)
                for x in range(sx):
                    f_buf[x, e, q0 : q0 + n] = tile[x + 1]
                f_fix[0, e, q0 : q0 + n] = tile[0]
                f_fix[1, e, q0 : q0 + n] = tile[sx + 1]
            edge_copy(e).start()
            for c in fixed[e]:
                c.start()

            def beside(x):
                if x in (0, sx - 1):
                    return f_fix[0 if x == 0 else 1, e]
                return f_in[x, (sy - 3) * e]

            for X in range(cx):
                at = QPAD * (cx * e + X)
                s_buf[at : at + Q] = ((f_buf[2 * X, e] + f_buf[2 * X + 1, e])
                                      + (beside(2 * X) + beside(2 * X + 1)))
        mean = dot_parts(s_buf[...], thin[...], 2)
        for e in range(2):
            for X in range(cx):
                at = QPAD * (cx * e + X)
                c_buf[X, e] = mean[at : at + Q, 0:nzc]
            coarse_copy(e).start()
        for c in ready + fixed[0] + fixed[1]:
            c.wait()

    @pl.when(own != 1)
    def _():
        wall = c_wall[...]

        for e in range(2):
            msg = msgs.at[pl.ds(Y_ROWS * e, Y_ROWS)]
            for x in range(sx):
                f_buf[x, e] = blend(ex_side[e, x + 1, 0:Q], ex_g[e, x + 1, 0:Q])
            edge_copy(e).start()

            def tile(I, q0, n):
                at = Y_SECOND if I >= 3 else 0
                if I == 2:
                    at = Y_THIRD - (16 if q0 >= 16 else 0)
                v = msg[at + q0 : at + q0 + n]
                if I in (1, 4) or (I == 2 and q0 >= 16):
                    v = roll_lane(v, nzc)
                return v[:, 0:nzc]

            for q, v in enumerate(coarse_plane(tile)):
                c_g[q, e, :, 0:nzc] = v

        def plane(q, J):
            if J == 0:
                return c_g[q, 0]
            if J == cy + 1:
                return c_g[q, 1]
            return c_all[q, J - 1]

        lower = sub < 4

        def joined(a, b, by):
            return jnp.where(lower, roll_sub(a, by), roll_sub(b, by + 4))

        lane = iota(1)
        edges = {1: lane == 0, -1: lane == nzc - 1}
        none = jnp.zeros((8, LANES), I32)
        center = [joined(plane(q, 1), plane(q, cy), 0) for q in range(Q)]
        pulled = []
        for q in range(Q):
            ex, ey, ez = STEP[q]
            if (ex, ey, ez) == (0, 0, 0):
                pulled.append(center[q])
                continue
            v = roll_lane(joined(plane(q, 1 - ey), plane(q, cy - ey), ex), ez)
            m = None
            if ey != 0:
                walls = (wall, none) if ey < 0 else (none, wall)
                m = roll_lane(joined(*walls, ex), ez) == 1
            if ez != 0:
                m = edges[ez] if m is None else m | edges[ez]
            pulled.append(v if m is None else jnp.where(m, center[26 - q], v))
        new = collide(pulled, coef)
        for q0, n in OCTETS:
            tile = jnp.swapaxes(jnp.stack(new[q0 : q0 + n]), 0, 1)
            for e in range(2):
                for X in range(cx):
                    c_buf[X, e, q0 : q0 + n] = tile[1 + X + 4 * e][:, 0:nzc]
        for e in range(2):
            coarse_copy(e).start()

    for e in range(2):
        edge_copy(e).wait()
        coarse_copy(e).wait()


def cost(flops, nbytes):
    return pl.CostEstimate(flops=flops, bytes_accessed=nbytes, transcendentals=0)


def in_hbm(x):
    return pltpu.with_memory_space_constraint(x, pltpu.HBM)


def local(fine_pops, coarse_pops, obstacle, block_level, relax_rates):
    fine = jnp.transpose(fine_pops, (1, 2, 0, 3))
    coarse = jnp.transpose(coarse_pops, (1, 2, 0, 3))
    sx, sy, _, nz = fine.shape
    cx, cy, _, nzc = coarse.shape

    x_message = struct((X_FINE + 9 * sy - 1, LANES))
    up, down = pl.pallas_call(
        pack_x_kernel,
        out_shape=(x_message, x_message),
        in_specs=[ANY] * 3,
        out_specs=(VMEM, VMEM),
        scratch_shapes=[
            pltpu.VMEM((sy, 16, nz), F32),
            pltpu.VMEM((sy, Q - 16, nz), F32),
            pltpu.VMEM((cy, Q, nzc), F32),
            pltpu.VMEM((cy, Q, nzc), F32),
            pltpu.VMEM((2, 17, LANES), F32),
            pltpu.SMEM(block_level.shape, I32),
            pltpu.SemaphoreType.DMA((5,)),
        ],
        compiler_params=params(),
        name="pack_x",
    )(in_hbm(fine), in_hbm(coarse), in_hbm(block_level))
    from_low = lax.ppermute(up, "stream", ring("stream", 1))
    from_high = lax.ppermute(down, "stream", ring("stream", -1))

    fine_shape, coarse_shape = struct(fine.shape), struct(coarse.shape)
    levels, coef, flags, c_wall, c_wide, refine, thin, fine, coarse = pl.pallas_call(
        tables_kernel,
        out_shape=(
            struct((9, 8, LANES), I32),
            struct((Q + len(EVEN), 8, LANES)),
            struct((2, 8, LANES), I32),
            struct((8, LANES), I32),
            struct((cy, cx, QPAD, nz)),
            struct((2 * nzc, 2 * nz), BF16),
            struct((nz, nz), BF16),
            fine_shape,
            coarse_shape,
        ),
        in_specs=[ANY] * 3 + [SMEM] * 2,
        out_specs=(VMEM,) * 9,
        scratch_shapes=[pltpu.VMEM(obstacle.shape, I32), pltpu.SemaphoreType.DMA((3,))],
        compiler_params=params(),
        cost_estimate=cost(10_000_000, 1_000_000),
        name="tables",
    )(in_hbm(fine), in_hbm(coarse), in_hbm(obstacle), block_level, relax_rates)

    y_message = struct((Y_ROWS, LANES))
    second, first, w_edge = pl.pallas_call(
        pack_y_kernel,
        out_shape=(y_message, y_message, struct((Q, 2, 8, LANES))),
        in_specs=[VMEM] * 5,
        out_specs=(VMEM,) * 3,
        scratch_shapes=[pltpu.VMEM(y_message.shape, F32)] * 2,
        compiler_params=params(),
        name="pack_y",
    )(fine, coarse, from_low, from_high, levels)
    if lax.axis_size("span") % 2 == 0:
        second = lax.ppermute(second, "span", pairs("span", 1))
        first = lax.ppermute(first, "span", pairs("span", 0))
    else:
        second, first = (lax.ppermute(first, "span", ring("span", 1)),
                         lax.ppermute(second, "span", ring("span", -1)))

    out, c_out, w_in, ex_side, c_all, f_in, aux = pl.pallas_call(
        inner_kernel,
        out_shape=(
            fine_shape,
            coarse_shape,
            struct((Q, sy - 2, 8, LANES)),
            struct((2, sx + 2, QPAD, nz)),
            struct((Q, cy, 8, LANES)),
            struct((sx, sy - 2, Q, nz)),
            struct((Q, 2, 8, LANES)),
        ),
        in_specs=[VMEM] * 12,
        out_specs=(ANY, ANY) + (VMEM,) * 5,
        scratch_shapes=[
            pltpu.VMEM((2, cy, QPAD, nz), F32),
            pltpu.VMEM((sx + 2, QPAD, nz), F32),
            pltpu.VMEM((cx, 1, Q, nzc), F32),
            pltpu.SemaphoreType.DMA((2,)),
        ],
        compiler_params=params(),
        cost_estimate=cost(20_000_000, 1_000_000),
        name="inner",
    )(fine, coarse, from_low, from_high, w_edge, levels, coef, flags, c_wall, c_wide, refine, thin)

    out, c_out = pl.pallas_call(
        outer_kernel,
        out_shape=(fine_shape, coarse_shape),
        in_specs=[VMEM] * 13 + [ANY, ANY],
        out_specs=(ANY, ANY),
        scratch_shapes=[
            pltpu.VMEM((2 * Y_ROWS, LANES), F32),
            pltpu.VMEM((5, QPAD, nz), F32),
            pltpu.VMEM((2, sx + 2, QPAD, nz), F32),
            pltpu.VMEM((9, 8, LANES), F32),
            pltpu.VMEM((Q, 8, LANES), F32),
            pltpu.VMEM((Q, 2, 8, LANES), F32),
            pltpu.VMEM((sx, 2, Q, nz), F32),
            pltpu.VMEM((2, 2, Q, nz), F32),
            pltpu.VMEM((2 * QPAD * cx, nz), F32),
            pltpu.VMEM((cx, 2, Q, nzc), F32),
            pltpu.SemaphoreType.DMA((10,)),
        ],
        input_output_aliases={13: 0, 14: 1},
        compiler_params=params(),
        name="outer",
    )(second, first, w_edge, w_in, c_all, ex_side, f_in, aux, levels, coef, c_wall, refine, thin,
      out, c_out)
    return jnp.transpose(out, (2, 0, 1, 3)), jnp.transpose(c_out, (2, 0, 1, 3))


def solution(mesh):
    placed = (
        P(None, "stream", "span", None),
        P(None, "stream", "span", None),
        P("stream", "span", None),
        P(),
        P(),
    )
    return jax.shard_map(
        local,
        mesh=mesh,
        in_specs=placed,
        out_specs=(P(None, "stream", "span", None), P(None, "stream", "span", None)),
        check_vma=False,
    )
```

```python
import jax
import jax.numpy as jnp
from jax import lax
from jax.experimental import pallas as pl
from jax.experimental.pallas import tpu as pltpu
from jax.sharding import PartitionSpec as P

F32 = jnp.float32
I32 = jnp.int32
BF16 = jnp.bfloat16
Q = 27
QPAD = 32
LANES = 128
OCTETS = [(8 * o, min(8, Q - 8 * o)) for o in range(4)]
STEP = [(q // 9 - 1, q // 3 % 3 - 1, q % 3 - 1) for q in range(Q)]
HIGH_X = [q for q in range(Q) if STEP[q][0] == 1]
LOW_X = [q for q in range(Q) if STEP[q][0] == -1]
HIGH_Y = [q for q in range(Q) if STEP[q][1] == 1]
LOW_Y = [q for q in range(Q) if STEP[q][1] == -1]
EVEN = [9 * a + 3 * b + c for a in (0, 2) for b in (0, 2) for c in (0, 2)]

VMEM = pl.BlockSpec(memory_space=pltpu.VMEM)
SMEM = pl.BlockSpec(memory_space=pltpu.SMEM)
ANY = pl.BlockSpec(memory_space=pl.ANY)
LIMIT = 16 << 20

LEV_BELOW, LEV_ROW, LEV_ABOVE = 0, 1, 2
LEV_X_LOW, LEV_X_HIGH, LEV_OWN, LEV_Y_LOW, LEV_Y_HIGH, EVEN_SPAN = 3, 4, 5, 6, 7, 8

X_FINE, X_MIDDLE = Q, Q + 9
Y_SECOND, Y_THIRD, Y_CORNER = Q, 2 * Q, 2 * Q + 16
Y_ROWS = 80


def fine_slot(k):
    ex = k // 3 - 1
    if ex == 0:
        return 6 * (k % 3), 6, 1
    return 36 + 7 * (k % 3 if ex < 0 else 3 + k % 3), 7, (1 if ex < 0 else 0)


def params(**more):
    return pltpu.CompilerParams(vmem_limit_bytes=LIMIT, **more)


def struct(shape, dtype=F32):
    return jax.ShapeDtypeStruct(shape, dtype)


def ring(axis, by):
    peers = lax.axis_size(axis)
    return [(i, (i + by) % peers) for i in range(peers)]


def pairs(axis, odd):
    peers = lax.axis_size(axis)
    return [(i, (i + (1 if i % 2 == odd else -1)) % peers) for i in range(peers)]


def roll_lane(v, by):
    return v if by == 0 else pltpu.roll(v, by % v.shape[1], 1)


def roll_sub(v, by):
    return v if by == 0 else pltpu.roll(v, by % v.shape[0], 0)


def iota(axis, shape=(8, LANES)):
    return lax.broadcasted_iota(I32, shape, axis)


def row8(ref, at):
    return jnp.broadcast_to(ref[at : at + 1], (8, LANES))


def dot_parts(x, m, count):
    parts = []
    for _ in range(count):
        parts.append(x.astype(BF16))
        x = x - parts[-1].astype(F32)
    return sum(jnp.dot(p, m, preferred_element_type=F32) for p in reversed(parts))


def dot_exact(x, m):
    return dot_parts(x, m, 3)


def pair_of(i):
    a = (i + 1) >> 1
    return a, a + (1 if (i + 1) & 1 else -1)


def blend(a, b):
    return 0.75 * a + 0.25 * b


def pack_x_kernel(fine, coarse, level, up, down, f_low, f_high, c_low, c_high, middle, lev, sems):
    sx, sy, cx = fine.shape[0], fine.shape[1], coarse.shape[0]
    fetch_level = pltpu.make_async_copy(level, lev, sems.at[4])
    copies = [
        pltpu.make_async_copy(fine.at[sx - 1, :, pl.ds(16, Q - 16)], f_high, sems.at[0]),
        pltpu.make_async_copy(coarse.at[cx - 1], c_high, sems.at[1]),
        pltpu.make_async_copy(fine.at[0, :, pl.ds(0, 16)], f_low, sems.at[2]),
        pltpu.make_async_copy(coarse.at[0], c_low, sems.at[3]),
    ]
    fetch_level.start()
    for c in copies:
        c.start()
    for c in copies:
        c.wait()
    cy, nzc = c_low.shape[0], c_low.shape[2]
    for k, (out, f, c, q0) in enumerate(((up, f_high, c_high, HIGH_X[0] - 16), (down, f_low, c_low, LOW_X[0]))):
        middle[k, :, 0:nzc] = c[1, 0:16]
        middle[k, 0 : Q - 16, nzc : 2 * nzc] = c[1, 16:Q]
        out[0:Q, 0:nzc] = c[0]
        out[0:Q, nzc : 2 * nzc] = c[cy - 1]
        for y in range(sy):
            out[X_FINE + 9 * y : X_FINE + 9 * y + 9] = f[y, q0 : q0 + 9]
    fetch_level.wait()
    n_row = lev.shape[0]
    row, col = lax.axis_index("stream"), lax.axis_index("span")
    for k, (out, to) in enumerate(((up, row + 1), (down, row + n_row - 1))):
        both = lev[row, col] * lev[lax.rem(to, n_row), col]
        at = slice(X_MIDDLE, X_MIDDLE + 16)
        out[at] = jnp.where(jnp.full((16, LANES), both, I32) == 1, out[at], middle[k])


def gain_of(q):
    return (1.0 if q // 9 == 0 else 1.0 / 3.0) * (1.0 if q // 3 % 3 == 0 else 1.0 / 3.0) * (
        1.0 if q % 3 == 0 else 1.0 / 3.0)


def tables_kernel(fine_far, coarse_far, obstacle_far, level, rates,
                  levels, coef, flags, c_wall, c_wide, refine, thin, fine, coarse, obstacle, sems):
    arrive = [pltpu.make_async_copy(a, b, sems.at[k]) for k, (a, b) in enumerate(
        ((obstacle_far, obstacle), (coarse_far, coarse), (fine_far, fine)))]
    for c in arrive:
        c.start()
    cx, cy, nzc = coarse.shape[0], coarse.shape[1], coarse.shape[3]
    sx, sy, nz = obstacle.shape
    row, col = lax.axis_index("stream"), lax.axis_index("span")
    n_row, n_col = level.shape
    at_row = [lax.rem(row + n_row - 1, n_row), row, lax.rem(row + 1, n_row)]
    at_col = [lax.rem(col + n_col - 1, n_col), col, lax.rem(col + 1, n_col)]
    lane, sub = iota(1), iota(0)
    for k in range(3):
        levels[k] = jnp.where(sub == 0, level[at_row[0], at_col[k]],
                              jnp.where(sub == sx + 1, level[at_row[2], at_col[k]], level[at_row[1], at_col[k]]))
    for k, (r, c) in ((LEV_X_LOW, (0, 1)), (LEV_X_HIGH, (2, 1)), (LEV_OWN, (1, 1)), (LEV_Y_LOW, (1, 0)),
                      (LEV_Y_HIGH, (1, 2))):
        levels[k] = jnp.full((8, LANES), level[at_row[r], at_col[c]], I32)
    even = lax.rem(col, 2) == 0 if n_col % 2 == 0 else True
    levels[EVEN_SPAN] = jnp.full((8, LANES), jnp.where(even, 1, 0), I32)
    refined = levels[LEV_OWN] == 1
    for q in range(Q):
        s = jnp.full((8, LANES), rates[q], F32)
        s = jnp.where(refined, s, 1.0 / (2.0 / s - 0.5))
        coef[q] = 0.125 - 0.125 * s
        if q in EVEN:
            coef[Q + EVEN.index(q)] = (0.125 * gain_of(q)) * s
    shape = (2 * nzc, 2 * nz)
    i, l = iota(0, shape), iota(1, shape)
    half, l = l // nz, l % nz
    za = (l >> 1) + half * nzc
    zb = jnp.clip((l >> 1) + jnp.where((l & 1) == 1, 1, -1), 0, nzc - 1) + half * nzc
    refine[...] = (jnp.where(i == za, 0.75, 0.0) + jnp.where(i == zb, 0.25, 0.0)).astype(BF16)
    shape = (nz, nz)
    thin[...] = jnp.where((iota(0, shape) >> 1) == iota(1, shape), 0.125, 0.0).astype(BF16)
    arrive[0].wait()
    planes = []
    for k, y in enumerate((sy // 2 - 1, sy // 2)):
        v = jnp.zeros((8, LANES), I32)
        for x in (sx // 2 - 1, sx // 2):
            v = jnp.where(sub == x + 1, jnp.broadcast_to(obstacle[x, y : y + 1, :], (8, LANES)), v)
        flags[k] = v
        planes.append(v)
    both = jnp.maximum(planes[0], planes[1])
    both = jnp.maximum(both, roll_sub(both, -1))
    both = jnp.maximum(both, roll_lane(both, -1))
    both = jnp.take_along_axis(both, (2 * lane) & (LANES - 1), axis=1)
    both = jnp.broadcast_to(both[sx // 2 : sx // 2 + 1], (8, LANES))
    c_wall[...] = jnp.where((sub == 1 + cx // 2) & (lane < nzc), both, 0)
    arrive[1].wait()
    for Y in range(cy):
        for X in range(cx):
            c_wide[Y, X, 0:Q] = dot_exact(coarse[X, Y], refine[0:nzc, 0:nz])
    arrive[2].wait()


def fine_plane(fine, from_low, from_high, y, mixed=None):
    sx = fine.shape[0]
    base = X_FINE + 9 * y
    rows = [None] * Q
    for q0, n in OCTETS:
        cells = [fine[x, y, q0 : q0 + n] for x in range(sx)]
        low = high = cells[0]
        if q0 == 16:
            low = from_low[base - 2 : base + 6]
        if q0 == 24:
            low = from_low[base + 6 : base + 9]
        if q0 == 0:
            high = from_high[base : base + 8]
        if q0 == 8:
            high = row8(from_high, base + 8)
        if mixed is not None:
            if q0 >= 16:
                low = mixed(0, q0, n, low)
            else:
                high = mixed(1, q0, n, high)
        tile = jnp.swapaxes(jnp.stack([low, *cells, high]), 0, 1)
        for k in range(n):
            rows[q0 + k] = tile[k]
    return rows


def coarse_plane(tile_of):
    rows = [None] * Q
    for q0, n in OCTETS:
        tiles = [tile_of(I, q0, n) for I in range(5)]
        tile = jnp.swapaxes(jnp.stack(tiles + tiles[:3]), 0, 1)
        for k in range(n):
            rows[q0 + k] = tile[k]
    return rows


def pack_y_kernel(fine, coarse, from_low, from_high, levels, second, first, w_edge, up, down):
    sy, cy, nzc = fine.shape[1], coarse.shape[1], coarse.shape[3]
    low_half = iota(1, (Q, LANES)) < nzc
    own = levels[LEV_OWN] == 1
    for out, e, y, Y, qs, to in ((up, 1, sy - 1, cy - 1, HIGH_Y, LEV_Y_HIGH), (down, 0, 0, 0, LOW_Y, LEV_Y_LOW)):
        both = own & (levels[to] == 1)
        g_low, g_high = from_low[0:Q], from_high[0:Q]
        if e == 0:
            g_high = roll_lane(g_high, nzc)
        else:
            g_low = roll_lane(g_low, nzc)
        out[0:Q] = g_low
        out[0:Q, nzc : 2 * nzc] = coarse[0, Y]
        out[Y_SECOND : Y_SECOND + Q] = g_high
        out[Y_SECOND : Y_SECOND + Q, 0:nzc] = coarse[2, Y]
        out[Y_THIRD : Y_THIRD + 16, 0:nzc] = coarse[1, Y, 0:16]
        out[Y_THIRD : Y_THIRD + Q - 16, nzc : 2 * nzc] = coarse[1, Y, 16:Q]
        rows = fine_plane(fine, from_low, from_high, y)
        for q in range(Q):
            w_edge[q, e] = rows[q]
        for k in range(3):
            out[Y_CORNER + k : Y_CORNER + k + 1] = rows[qs[6 + k]][0:1]
            out[Y_CORNER + 3 + k : Y_CORNER + 4 + k] = rows[qs[k]][7:8]
        for k, q in enumerate(qs):
            at, n, s = fine_slot(k)
            out[at : at + n] = jnp.where(both[0:n], rows[q][s : s + n], out[at : at + n])
    even = levels[EVEN_SPAN] == 1
    for at in range(0, Y_ROWS, 8):
        a, b = up[at : at + 8], down[at : at + 8]
        first[at : at + 8] = jnp.where(even, a, b)
        second[at : at + 8] = jnp.where(even, b, a)


def forward(m0, m1, m2):
    pair = m0 + m2
    return pair + 4.0 * m1, m2 - m0, pair


ALONG_Y = [(9 * a + c, 3) for a in range(3) for c in range(3)]
ALONG_Z = [(9 * a + 3 * b, 1) for a in range(3) for b in range(3)]
ALONG_X = [(r, 9) for r in range(9)]


def collide(g, coef):
    t = [None] * Q
    for r in range(9):
        t[r], t[9 + r], t[18 + r] = forward(g[r], g[9 + r], g[18 + r])
    cols = [(t[c] + t[6 + c]) + 4.0 * t[3 + c] for c in range(3)]
    density = (cols[0] + cols[2]) + 4.0 * cols[1]
    inv = 1.0 / density
    rows = [(t[3 * b] + t[3 * b + 2]) + 4.0 * t[3 * b + 1] for b in (0, 2)]
    uy = (rows[1] - rows[0]) * inv
    uz = (cols[2] - cols[0]) * inv
    dcols = [(t[9 + c] + t[15 + c]) + 4.0 * t[12 + c] for c in range(3)]
    ux = ((dcols[0] + dcols[2]) + 4.0 * dcols[1]) * inv
    for r in range(9):
        t0, d, pair = t[r], t[9 + r], t[18 + r]
        t1 = d - ux * t0
        t[9 + r], t[18 + r] = t1, pair - ux * (d + t1)
    for u, lines in ((uy, ALONG_Y), (uz, ALONG_Z)):
        for at, by in lines:
            t0, d, pair = forward(t[at], t[at + by], t[at + 2 * by])
            t1 = d - u * t0
            t[at], t[at + by], t[at + 2 * by] = t0, t1, pair - u * (d + t1)
    for q in range(Q):
        t[q] = coef[q] * t[q]
        if q in EVEN:
            t[q] = t[q] + coef[Q + EVEN.index(q)] * density
    for u, lines in ((uz, ALONG_Z), (uy, ALONG_Y), (ux, ALONG_X)):
        for at, by in lines:
            t0, t1, t2 = t[at], t[at + by], t[at + 2 * by]
            d = t1 + u * t0
            s = t2 + u * (t1 + d)
            t[at], t[at + by], t[at + 2 * by] = s - d, 0.5 * (t0 - s), s + d
    return t


def pull(source, center, step_mask):
    out = []
    for q in range(Q):
        ex, ey, ez = STEP[q]
        v = roll_lane(roll_sub(source(q), ex), ez)
        mask = step_mask(ex, ey, ez)
        if mask is not None:
            v = jnp.where(mask, center(26 - q), v)
        out.append(v)
    return out


def bounce_mask(height, wall_of):
    lane = iota(1)
    edges = {1: lane == 0, -1: lane == height - 1}

    def mask_of(ex, ey, ez):
        m = None
        if (ex, ey, ez) == (0, 0, 0):
            return None
        wall = wall_of(ey)
        if wall is not None:
            m = roll_lane(roll_sub(wall, ex), ez) == 1
        if ez != 0:
            m = edges[ez] if m is None else m | edges[ez]
        return m

    return mask_of


def wall_plane(flags, y, first):
    def wall_of(ey):
        k = y - ey - first
        return flags[k] if k in (0, 1) else None

    return wall_of


def store_rows(rows, out, t, xs, width):
    for q0, n in OCTETS:
        tile = jnp.swapaxes(jnp.stack(rows[q0 : q0 + n]), 0, 1)
        for k, x in enumerate(xs):
            out[k, t, q0 : q0 + n] = tile[x][:, 0:width]


def coalesce(planes, out, at, thin):
    nzc = out.shape[3]
    for X in range(out.shape[0]):
        s = sum(p[2 * X] + p[2 * X + 1] for p in planes)
        out[X, at] = dot_exact(s, thin[...])[:, 0:nzc]


def coarse_step(plane, J, wall, coef, buf, at, nzc, cx, wall_row):
    mask_of = bounce_mask(nzc, lambda ey: wall if J - ey == wall_row else None)
    new = collide(pull(lambda q: plane(q, J - STEP[q][1]), lambda q: plane(q, J), mask_of), coef)
    if J == wall_row:
        stay = wall == 1
        new = [jnp.where(stay, plane(q, J), new[q]) for q in range(Q)]
    store_rows(new, buf, at, range(1, cx + 1), nzc)


def inner_kernel(fine, coarse, from_low, from_high, w_edge, levels, coef, flags, c_wall, c_wide, refine, thin,
                 out, c_out, w_in, ex_side, c_all, f_in, aux, ghost, ex_mid, c_buf, sems):
    sx, sy, nz = fine.shape[0], fine.shape[1], fine.shape[3]
    cx, cy, nzc = coarse.shape[0], coarse.shape[1], coarse.shape[3]
    mid = sy // 2
    own = jnp.max(levels[LEV_OWN])
    n = 8 * ((X_MIDDLE + 16 + 7) // 8)
    both = dot_exact(jnp.concatenate([from_low[0:n], from_high[0:n]], axis=0), refine[...])
    for side in range(2):
        v = both[side * n : side * n + n]
        ghost[side, 0, 0:Q] = v[0:Q, 0:nz]
        ghost[side, cy - 1, 0:Q] = v[0:Q, nz : 2 * nz]
        ghost[side, 1, 0:16] = v[X_MIDDLE : X_MIDDLE + 16, 0:nz]
        ghost[side, 1, 16:Q] = v[X_MIDDLE : X_MIDDLE + Q - 16, nz : 2 * nz]

    def wide(J, I):
        if I == 0:
            return ghost[0, J - 1]
        if I == cx + 1:
            return ghost[1, J - 1]
        return c_wide[J - 1, I - 1]

    for J in range(1, cy + 1):
        for i in range(sx + 2):
            a, b = pair_of(i)
            v = blend(wide(J, a), wide(J, b))
            if J == 2:
                ex_mid[i] = v
            else:
                ex_side[J // 2, i] = v

    def exploded(J, i):
        return ex_mid.at[i] if J == 2 else ex_side.at[J // 2, i]

    copies = [pltpu.make_async_copy(f_in.at[:, pl.ds(mid - 2, 2)], out.at[:, pl.ds(mid - 1, 2)], sems.at[0]),
              pltpu.make_async_copy(c_buf, c_out.at[:, pl.ds(cy // 2, 1)], sems.at[1]),
              pltpu.make_async_copy(f_in, out.at[:, pl.ds(1, sy - 2)], sems.at[0])]

    @pl.when(own == 1)
    def _():
        refined = (levels[LEV_X_LOW] == 1, levels[LEV_X_HIGH] == 1)
        sub = iota(0)
        for y in range(1, sy - 1):
            a, b = pair_of(y + 1)

            def mixed(side, q0, n, tile):
                i = 0 if side == 0 else sx + 1
                e = blend(exploded(a, i)[q0 : q0 + n], exploded(b, i)[q0 : q0 + n])
                return jnp.where(refined[side][0:n], tile, e)

            rows = fine_plane(fine, from_low, from_high, y, mixed)
            for q in range(Q):
                w_in[q, y - 1] = rows[q]

        def plane(q, y):
            if y in (0, sy - 1):
                return w_edge[q, 0 if y == 0 else 1]
            return w_in[q, y - 1]

        for y in (mid - 1, mid, 1, sy - 2):
            pulled = pull(lambda q: plane(q, y - STEP[q][1]), lambda q: plane(q, y),
                          bounce_mask(nz, wall_plane(flags, y, mid - 1)))
            if y in (1, sy - 2):
                for q in range(Q):
                    aux[q, 0 if y == 1 else 1] = jnp.where(sub == 0, roll_sub(pulled[q], -1), roll_sub(pulled[q], 1))
            new = collide(pulled, coef)
            if y in (mid - 1, mid):
                stay = flags[y - mid + 1] == 1
                new = [jnp.where(stay, w_in[q, y - 1], new[q]) for q in range(Q)]
            store_rows(new, f_in, y - 1, range(1, sx + 1), nz)
            if y == mid:
                copies[0].start()
                coalesce([f_in.at[:, mid - 2], f_in.at[:, mid - 1]], c_buf, 0, thin)
                copies[1].start()
        copies[0].wait()

    @pl.when(own != 1)
    def _():
        for y in range(1, sy - 1):
            a, b = pair_of(y + 1)
            for x in range(sx):
                f_in[x, y - 1] = blend(exploded(a, x + 1)[0:Q], exploded(b, x + 1)[0:Q])
        copies[2].start()

        def tile_of(Y):
            def tile(I, q0, n):
                if 1 <= I <= cx:
                    return coarse[I - 1, Y, q0 : q0 + n]
                msg = from_low if I == 0 else from_high
                if Y != 1:
                    v = msg[q0 : q0 + n]
                    return (v if Y == 0 else roll_lane(v, nzc))[:, 0:nzc]
                if q0 < 16:
                    return msg[X_MIDDLE + q0 : X_MIDDLE + q0 + n, 0:nzc]
                return roll_lane(msg[X_MIDDLE + q0 - 16 : X_MIDDLE + q0 - 16 + n], nzc)[:, 0:nzc]

            return tile

        for Y in range(cy):
            for q, v in enumerate(coarse_plane(tile_of(Y))):
                c_all[q, Y, :, 0:nzc] = v
        coarse_step(lambda q, J: c_all[q, J - 1], 2, c_wall[...], coef, c_buf, 0, nzc, cx, 2)
        copies[1].start()
        copies[2].wait()

    copies[1].wait()


def outer_kernel(second, first, w_edge, w_in, c_all, ex_side, f_in, aux, levels, coef, c_wall, refine, thin,
                 _out_in, _c_in, out, c_out, msgs, wide, ex_g, w_g, w_e, c_g, f_buf, f_fix, s_buf, c_buf, sems):
    sx, sy, nz = out.shape[0], out.shape[1], out.shape[3]
    cx, cy, nzc = c_out.shape[0], c_out.shape[1], c_out.shape[3]
    own = jnp.max(levels[LEV_OWN])
    sub = iota(0)
    even = levels[EVEN_SPAN] == 1
    for at in range(0, Y_ROWS, 8):
        a, b = first[at : at + 8], second[at : at + 8]
        msgs[at : at + 8] = jnp.where(even, b, a)
        msgs[Y_ROWS + at : Y_ROWS + at + 8] = jnp.where(even, a, b)
    v = dot_parts(msgs[...], refine[...], 2)
    for e in range(2):
        at = Y_ROWS * e
        wide[0, 0:Q] = v[at : at + Q, 0:nz]
        wide[1, 0:Q] = v[at : at + Q, nz : 2 * nz]
        wide[3, 0:Q] = v[at + Y_SECOND : at + Y_SECOND + Q, 0:nz]
        wide[4, 0:Q] = v[at + Y_SECOND : at + Y_SECOND + Q, nz : 2 * nz]
        wide[2, 0:16] = v[at + Y_THIRD : at + Y_THIRD + 16, 0:nz]
        wide[2, 16:Q] = v[at + Y_THIRD : at + Y_THIRD + Q - 16, nz : 2 * nz]
        for i in range(sx + 2):
            a, b = pair_of(i)
            ex_g[e, i] = blend(wide[a], wide[b])

    def edge_copy(e):
        y = (sy - 1) * e
        return pltpu.make_async_copy(f_buf.at[:, pl.ds(e, 1)], out.at[:, pl.ds(y, 1)], sems.at[e])

    def coarse_copy(e):
        return pltpu.make_async_copy(c_buf.at[:, pl.ds(e, 1)], c_out.at[:, pl.ds((cy - 1) * e, 1)], sems.at[2 + e])

    @pl.when(own == 1)
    def _():
        ready = [pltpu.make_async_copy(f_in.at[pl.ds(1, sx - 2), pl.ds((sy - 3) * e, 1)],
                                       out.at[pl.ds(1, sx - 2), pl.ds(1 + (sy - 3) * e, 1)], sems.at[4 + e])
                 for e in range(2)]
        fixed = [[pltpu.make_async_copy(f_fix.at[pl.ds(side, 1), pl.ds(e, 1)],
                                        out.at[pl.ds((sx - 1) * side, 1), pl.ds(1 + (sy - 3) * e, 1)],
                                        sems.at[6 + 2 * e + side]) for side in range(2)] for e in range(2)]
        for c in ready:
            c.start()
        lane = iota(1)
        inside = {0: None, 1: lane != 0, -1: lane != nz - 1}
        for e in range(2):
            msg = msgs.at[pl.ds(Y_ROWS * e, Y_ROWS)]
            qs = HIGH_Y if e == 0 else LOW_Y
            far = levels[LEV_BELOW if e == 0 else LEV_ABOVE] == 1
            near = levels[LEV_Y_LOW if e == 0 else LEV_Y_HIGH] == 1
            for q0, n in OCTETS:
                tiles = [blend(ex_g[e, i, q0 : q0 + n], ex_side[e, i, q0 : q0 + n]) for i in range(sx + 2)]
                tile = jnp.swapaxes(jnp.stack(tiles), 0, 1)
                for k, q in enumerate(qs):
                    if q0 <= q < q0 + n:
                        at, _, s = fine_slot(k)
                        v = roll_sub(msg[at : at + 8], s)
                        if STEP[q][0] != 0:
                            corner = Y_CORNER + k % 3 + (0 if STEP[q][0] > 0 else 3)
                            v = jnp.where(near, v, row8(msg, corner))
                        w_g[k] = jnp.where(far, v, tile[q - q0])
            coarse_low = (levels[LEV_X_LOW] != 1) & (sub == 0)
            coarse_high = (levels[LEV_X_HIGH] != 1) & (sub == sx + 1)
            v_low = blend(ex_side[e, 0], ex_g[e, 0])
            v_high = blend(ex_side[e, sx + 1], ex_g[e, sx + 1])
            for q in range(Q):
                v = w_edge[q, e]
                if STEP[q][0] > 0:
                    v = jnp.where(coarse_low, jnp.broadcast_to(v_low[q : q + 1], (8, LANES)), v)
                if STEP[q][0] < 0:
                    v = jnp.where(coarse_high, jnp.broadcast_to(v_high[q : q + 1], (8, LANES)), v)
                w_e[q] = v

            def source(q):
                return (w_g[qs.index(q)] if q in qs else
                        w_e[q] if STEP[q][1] == 0 else w_in[q, (sy - 3) * e])

            pulled = pull(source, lambda q: w_e[q], bounce_mask(nz, lambda ey: None))
            spare = (sub == 0) | (sub == sx + 1)
            for q in range(Q):
                ex, _, ez = STEP[q]
                v = aux[q, e]
                if q in qs and ex != 0:
                    m = sub == (0 if ex > 0 else sx + 1)
                    if ez != 0:
                        m = m & inside[ez]
                    v = jnp.where(m, roll_lane(w_e[q], ez), v)
                pulled[q] = jnp.where(spare, v, pulled[q])
            new = collide(pulled, coef)
            for q0, n in OCTETS:
                tile = jnp.swapaxes(jnp.stack(new[q0 : q0 + n]), 0, 1)
                for x in range(sx):
                    f_buf[x, e, q0 : q0 + n] = tile[x + 1]
                f_fix[0, e, q0 : q0 + n] = tile[0]
                f_fix[1, e, q0 : q0 + n] = tile[sx + 1]
            edge_copy(e).start()
            for c in fixed[e]:
                c.start()

            def beside(x):
                if x in (0, sx - 1):
                    return f_fix[0 if x == 0 else 1, e]
                return f_in[x, (sy - 3) * e]

            for X in range(cx):
                at = QPAD * (cx * e + X)
                s_buf[at : at + Q] = ((f_buf[2 * X, e] + f_buf[2 * X + 1, e])
                                      + (beside(2 * X) + beside(2 * X + 1)))
        mean = dot_parts(s_buf[...], thin[...], 2)
        for e in range(2):
            for X in range(cx):
                at = QPAD * (cx * e + X)
                c_buf[X, e] = mean[at : at + Q, 0:nzc]
            coarse_copy(e).start()
        for c in ready + fixed[0] + fixed[1]:
            c.wait()

    @pl.when(own != 1)
    def _():
        wall = c_wall[...]

        for e in range(2):
            msg = msgs.at[pl.ds(Y_ROWS * e, Y_ROWS)]
            for x in range(sx):
                f_buf[x, e] = blend(ex_side[e, x + 1, 0:Q], ex_g[e, x + 1, 0:Q])
            edge_copy(e).start()

            def tile(I, q0, n):
                at = Y_SECOND if I >= 3 else 0
                if I == 2:
                    at = Y_THIRD - (16 if q0 >= 16 else 0)
                v = msg[at + q0 : at + q0 + n]
                if I in (1, 4) or (I == 2 and q0 >= 16):
                    v = roll_lane(v, nzc)
                return v[:, 0:nzc]

            for q, v in enumerate(coarse_plane(tile)):
                c_g[q, e, :, 0:nzc] = v

        def plane(q, J):
            if J == 0:
                return c_g[q, 0]
            if J == cy + 1:
                return c_g[q, 1]
            return c_all[q, J - 1]

        lower = sub < 4

        def joined(a, b, by):
            return jnp.where(lower, roll_sub(a, by), roll_sub(b, by + 4))

        lane = iota(1)
        edges = {1: lane == 0, -1: lane == nzc - 1}
        none = jnp.zeros((8, LANES), I32)
        center = [joined(plane(q, 1), plane(q, cy), 0) for q in range(Q)]
        pulled = []
        for q in range(Q):
            ex, ey, ez = STEP[q]
            if (ex, ey, ez) == (0, 0, 0):
                pulled.append(center[q])
                continue
            v = roll_lane(joined(plane(q, 1 - ey), plane(q, cy - ey), ex), ez)
            m = None
            if ey != 0:
                walls = (wall, none) if ey < 0 else (none, wall)
                m = roll_lane(joined(*walls, ex), ez) == 1
            if ez != 0:
                m = edges[ez] if m is None else m | edges[ez]
            pulled.append(v if m is None else jnp.where(m, center[26 - q], v))
        new = collide(pulled, coef)
        for q0, n in OCTETS:
            tile = jnp.swapaxes(jnp.stack(new[q0 : q0 + n]), 0, 1)
            for e in range(2):
                for X in range(cx):
                    c_buf[X, e, q0 : q0 + n] = tile[1 + X + 4 * e][:, 0:nzc]
        for e in range(2):
            coarse_copy(e).start()

    for e in range(2):
        edge_copy(e).wait()
        coarse_copy(e).wait()


def cost(flops, nbytes):
    return pl.CostEstimate(flops=flops, bytes_accessed=nbytes, transcendentals=0)


def in_hbm(x):
    return pltpu.with_memory_space_constraint(x, pltpu.HBM)


def local(fine_pops, coarse_pops, obstacle, block_level, relax_rates):
    fine = jnp.transpose(fine_pops, (1, 2, 0, 3))
    coarse = jnp.transpose(coarse_pops, (1, 2, 0, 3))
    sx, sy, _, nz = fine.shape
    cx, cy, _, nzc = coarse.shape

    x_message = struct((8 * ((X_FINE + 9 * sy + 7) // 8), LANES))
    up, down = pl.pallas_call(
        pack_x_kernel,
        out_shape=(x_message, x_message),
        in_specs=[ANY] * 3,
        out_specs=(VMEM, VMEM),
        scratch_shapes=[
            pltpu.VMEM((sy, 16, nz), F32),
            pltpu.VMEM((sy, Q - 16, nz), F32),
            pltpu.VMEM((cy, Q, nzc), F32),
            pltpu.VMEM((cy, Q, nzc), F32),
            pltpu.VMEM((2, 16, LANES), F32),
            pltpu.SMEM(block_level.shape, I32),
            pltpu.SemaphoreType.DMA((5,)),
        ],
        compiler_params=params(),
        name="pack_x",
    )(in_hbm(fine), in_hbm(coarse), in_hbm(block_level))
    from_low = lax.ppermute(up, "stream", ring("stream", 1))
    from_high = lax.ppermute(down, "stream", ring("stream", -1))

    fine_shape, coarse_shape = struct(fine.shape), struct(coarse.shape)
    levels, coef, flags, c_wall, c_wide, refine, thin, fine, coarse = pl.pallas_call(
        tables_kernel,
        out_shape=(
            struct((9, 8, LANES), I32),
            struct((Q + len(EVEN), 8, LANES)),
            struct((2, 8, LANES), I32),
            struct((8, LANES), I32),
            struct((cy, cx, QPAD, nz)),
            struct((2 * nzc, 2 * nz), BF16),
            struct((nz, nz), BF16),
            fine_shape,
            coarse_shape,
        ),
        in_specs=[ANY] * 3 + [SMEM] * 2,
        out_specs=(VMEM,) * 9,
        scratch_shapes=[pltpu.VMEM(obstacle.shape, I32), pltpu.SemaphoreType.DMA((3,))],
        compiler_params=params(),
        cost_estimate=cost(10_000_000, 1_000_000),
        name="tables",
    )(in_hbm(fine), in_hbm(coarse), in_hbm(obstacle), block_level, relax_rates)

    y_message = struct((Y_ROWS, LANES))
    second, first, w_edge = pl.pallas_call(
        pack_y_kernel,
        out_shape=(y_message, y_message, struct((Q, 2, 8, LANES))),
        in_specs=[VMEM] * 5,
        out_specs=(VMEM,) * 3,
        scratch_shapes=[pltpu.VMEM(y_message.shape, F32)] * 2,
        compiler_params=params(),
        name="pack_y",
    )(fine, coarse, from_low, from_high, levels)
    if lax.axis_size("span") % 2 == 0:
        second = lax.ppermute(second, "span", pairs("span", 1))
        first = lax.ppermute(first, "span", pairs("span", 0))
    else:
        second, first = (lax.ppermute(first, "span", ring("span", 1)),
                         lax.ppermute(second, "span", ring("span", -1)))

    out, c_out, w_in, ex_side, c_all, f_in, aux = pl.pallas_call(
        inner_kernel,
        out_shape=(
            fine_shape,
            coarse_shape,
            struct((Q, sy - 2, 8, LANES)),
            struct((2, sx + 2, QPAD, nz)),
            struct((Q, cy, 8, LANES)),
            struct((sx, sy - 2, Q, nz)),
            struct((Q, 2, 8, LANES)),
        ),
        in_specs=[VMEM] * 12,
        out_specs=(ANY, ANY) + (VMEM,) * 5,
        scratch_shapes=[
            pltpu.VMEM((2, cy, QPAD, nz), F32),
            pltpu.VMEM((sx + 2, QPAD, nz), F32),
            pltpu.VMEM((cx, 1, Q, nzc), F32),
            pltpu.SemaphoreType.DMA((2,)),
        ],
        compiler_params=params(),
        cost_estimate=cost(20_000_000, 1_000_000),
        name="inner",
    )(fine, coarse, from_low, from_high, w_edge, levels, coef, flags, c_wall, c_wide, refine, thin)

    out, c_out = pl.pallas_call(
        outer_kernel,
        out_shape=(fine_shape, coarse_shape),
        in_specs=[VMEM] * 13 + [ANY, ANY],
        out_specs=(ANY, ANY),
        scratch_shapes=[
            pltpu.VMEM((2 * Y_ROWS, LANES), F32),
            pltpu.VMEM((5, QPAD, nz), F32),
            pltpu.VMEM((2, sx + 2, QPAD, nz), F32),
            pltpu.VMEM((9, 8, LANES), F32),
            pltpu.VMEM((Q, 8, LANES), F32),
            pltpu.VMEM((Q, 2, 8, LANES), F32),
            pltpu.VMEM((sx, 2, Q, nz), F32),
            pltpu.VMEM((2, 2, Q, nz), F32),
            pltpu.VMEM((2 * QPAD * cx, nz), F32),
            pltpu.VMEM((cx, 2, Q, nzc), F32),
            pltpu.SemaphoreType.DMA((10,)),
        ],
        input_output_aliases={13: 0, 14: 1},
        compiler_params=params(),
        name="outer",
    )(second, first, w_edge, w_in, c_all, ex_side, f_in, aux, levels, coef, c_wall, refine, thin,
      out, c_out)
    return jnp.transpose(out, (2, 0, 1, 3)), jnp.transpose(c_out, (2, 0, 1, 3))


def solution(mesh):
    placed = (
        P(None, "stream", "span", None),
        P(None, "stream", "span", None),
        P("stream", "span", None),
        P(),
        P(),
    )
    return jax.shard_map(
        local,
        mesh=mesh,
        in_specs=placed,
        out_specs=(P(None, "stream", "span", None), P(None, "stream", "span", None)),
        check_vma=False,
    )
```
